32 devices in a mesh: dp: 4 (over z), row: 4 (over y, x), col: 2 (over core).
Axes of the slice: x: 2, y: 2, z: 4, core: 2. Of those that a mesh axis runs over, the one named last changes fastest.
Arguments:
- block_input: bfloat16 [1536, 2048], P('dp', 'row'), may hold values from -6 to 6
- segments: int32 [4, 384], P('dp'), may hold values from 0 to 5, never falling along the last dimension, each value on 1 to 192 neighbouring positions
- attention_norm: float32 [2048], P('row'), may hold values from 0.5 to 1.5
- query_weight: bfloat16 [2048, 2048], P('row', 'col'), may hold values from -0.125 to 0.125
- key_weight: bfloat16 [2048, 1024], P('row', 'col'), may hold values from -0.125 to 0.125
- value_weight: bfloat16 [2048, 1024], P('row', 'col'), may hold values from -0.125 to 0.125
- query_norm: float32 [128], replicated, may hold values from 0.5 to 1.5
- key_norm: float32 [128], replicated, may hold values from 0.5 to 1.5
- output_weight: bfloat16 [2048, 2048], P('col', 'row'), may hold values from -0.5 to 0.5
- feedforward_norm: float32 [2048], P('row'), may hold values from 0.5 to 1.5
- gate_weight: bfloat16 [2048, 6144], P('row', 'col'), may hold values from -0.125 to 0.125
- up_weight: bfloat16 [2048, 6144], P('row', 'col'), may hold values from -0.125 to 0.125
- down_weight: bfloat16 [6144, 2048], P('col', 'row'), may hold values from -0.15625 to 0.15625
- cotangent: bfloat16 [1536, 2048], P('dp', 'row'), may hold values from -6 to 6
Outputs:
- block_output: bfloat16 [1536, 2048], P('dp', 'row')
- input_gradient: float32 [1536, 2048], P('dp', 'row')
- attention_norm_gradient: float32 [2048], P('row')
- query_gradient: float32 [2048, 2048], P('row', 'col')
- key_gradient: float32 [2048, 1024], P('row', 'col')
- value_gradient: float32 [2048, 1024], P('row', 'col')
- query_norm_gradient: float32 [128], replicated
- key_norm_gradient: float32 [128], replicated
- output_gradient: float32 [2048, 2048], P('col', 'row')
- feedforward_norm_gradient: float32 [2048], P('row')
- gate_gradient: float32 [2048, 6144], P('row', 'col')
- up_gradient: float32 [2048, 6144], P('row', 'col')
- down_gradient: float32 [6144, 2048], P('col', 'row')
The draws below stay inside these ranges and needn't reach their ends.
Inputs may be any that keep to these rules, and one draw needn't show every extreme that they name: `segments`: along each row sequence numbers never fall; each of the 6 sequences of a batch spans 1 to 192 tokens, and one spans exactly 192.
All inputs are finite; a program needn't handle non-finite values.
Results may differ from the reference program's by a relative error of at most 0.018.
Values may be sent and summed in bfloat16 or wider, within the bound.
A program may use at most 192 MiB of HBM per device.

```python
import math
from functools import partial
import jax
import jax.numpy as jnp
import numpy as np
from jax import lax

D = 2048
QH = 16
KVH = 8
HD = 128
FF = 6144
TOK_DEV = 384
SEGS = 6
LONGEST = 192
TOKENS = 1536
N_DP = 4


def block_levels(rng, shape, pieces, smallest, largest):
    def one(axis_at, shards_of):
        steps = jax.random.uniform(jax.random.fold_in(jax.random.fold_in(rng, 6), axis_at), (shards_of,), jnp.float32, smallest / len(pieces), largest / len(pieces))
        return jnp.repeat(jnp.exp(steps), shape[axis_at] // shards_of).reshape((-1,) + (1,) * (len(shape) - axis_at - 1))

    level = one(*pieces[0])
    for cut in pieces[1:]:
        level = level * one(*cut)
    return level


def length_profile(number_of, total, bound, slope):
    loads = [(1 << 20) // math.isqrt(grade ** slope) + 1 for grade in range(2, number_of + 1)]
    rest, holding = total - bound - (number_of - 1), [1] * (number_of - 1)
    while rest > 0:
        candidates = [i for i in range(number_of - 1) if holding[i] < bound]
        pool, remaining = sum([loads[i] for i in candidates]), rest
        for i in candidates:
            addition = min(bound - holding[i], max(1, remaining * loads[i] // pool), rest)
            holding[i] = holding[i] + addition
            rest = rest - addition
    return np.array([bound] + holding)


def ragged(stream_key, count, total, limit, slope):
    if count == 2:
        one = jax.random.randint(stream_key, (), max(1, total - limit), min(limit, total - 1) + 1)
        return jnp.stack([one, total - one])
    tallies = jnp.asarray(length_profile(count, total, limit, slope), jnp.int32)
    couples = (count - 1) // 2
    source_of, taker = tallies[1:1 + 2 * couples:2], tallies[2:2 + 2 * couples:2]
    room = jnp.minimum(source_of - 1, limit - taker)
    passed = jax.random.randint(jax.random.fold_in(stream_key, 1), (couples,), 0, 1 << 20) % (room + 1)
    tallies = tallies.at[1:1 + 2 * couples:2].set(source_of - passed).at[2:2 + 2 * couples:2].set(taker + passed)
    return tallies[jax.random.permutation(jax.random.fold_in(stream_key, 2), count)]


def centred(own_key, shape, spread, most, cuts=(), kind=jnp.bfloat16):
    entries = jax.random.normal(own_key, shape, jnp.float32) * spread
    if len(cuts) > 0:
        entries = block_levels(own_key, shape, cuts, -0.22, 0.18) * entries
    return jnp.clip(entries, min=-most, max=most).astype(kind)


def setup_inputs(seed: int = 0) -> dict:
    streams_of = jax.random.split(jax.random.key(seed), 15)
    return {
        "block_input": centred(streams_of[0], (TOKENS, D), 1.0, 6.0, ((0, 4), (1, 4))),
        "segments": jax.vmap(lambda own: jnp.searchsorted(jnp.cumsum(ragged(own, SEGS, TOK_DEV, LONGEST, 2)), jnp.arange(TOK_DEV), side="right"))(jax.random.split(streams_of[1], N_DP)).reshape((N_DP, TOK_DEV)).astype(jnp.int32),
        "attention_norm": jnp.clip(1.0 + 0.1 * jax.random.normal(streams_of[2], (D,), jnp.float32), 0.5, 1.5),
        "query_weight": centred(streams_of[3], (D, QH * HD), D ** -0.5, 0.125, ((0, 4), (1, 2))),
        "key_weight": centred(streams_of[4], (D, KVH * HD), D ** -0.5, 0.125, ((0, 4), (1, 2))),
        "value_weight": centred(streams_of[5], (D, KVH * HD), D ** -0.5, 0.125, ((0, 4), (1, 2))),
        "query_norm": jnp.clip(1.0 + 0.1 * jax.random.normal(streams_of[6], (HD,), jnp.float32), 0.5, 1.5),
        "key_norm": jnp.clip(1.0 + 0.1 * jax.random.normal(streams_of[7], (HD,), jnp.float32), 0.5, 1.5),
        "output_weight": centred(streams_of[8], (QH * HD, D), (QH * HD // 16) ** -0.5, 0.5, ((0, 2), (1, 4))),
        "feedforward_norm": jnp.clip(1.0 + 0.1 * jax.random.normal(streams_of[9], (D,), jnp.float32), 0.5, 1.5),
        "gate_weight": centred(streams_of[10], (D, FF), D ** -0.5, 0.125, ((0, 4), (1, 2))),
        "up_weight": centred(streams_of[11], (D, FF), D ** -0.5, 0.125, ((0, 4), (1, 2))),
        "down_weight": centred(streams_of[12], (FF, D), (FF // 4) ** -0.5, 0.15625, ((0, 2), (1, 4))),
        "cotangent": centred(streams_of[13], (TOKENS, D), 1.0, 6.0, ((0, 4), (1, 4))),
    }


epsilon = 1e-06
rope_base = 1000000.0

def rotate_half(values):
    half = values.shape[-1] // 2
    return jnp.concatenate([-values[..., half:], values[..., :half]], axis=-1)

def positions_of(segment_row):
    length = segment_row.shape[0]
    index = jnp.arange(length, dtype=jnp.int32)
    starts = jnp.concatenate([jnp.ones((1,), jnp.bool_), segment_row[1:] != segment_row[:-1]])
    first = lax.cummax(jnp.where(starts, index, jnp.zeros_like(index)), axis=0)
    return index - first

def rotary_tables(positions, head_size):
    half = head_size // 2
    inverse = rope_base ** (-2.0 * jnp.arange(half, dtype=jnp.float32) / head_size)
    angles = positions.astype(jnp.float32)[:, None] * inverse[None, :]
    angles = jnp.concatenate([angles, angles], axis=-1)
    return (jnp.cos(angles)[:, None, :], jnp.sin(angles)[:, None, :])

def head_forward(raw, gain, cosine, sine):
    scale = lax.rsqrt(lax.optimization_barrier(jnp.mean(raw * raw, axis=-1, keepdims=True)) + epsilon)
    normed = raw * scale * gain
    return normed * cosine + rotate_half(normed) * sine

def reference(block_input, segments, attention_norm, query_weight, key_weight, value_weight, query_norm, key_norm, output_weight, feedforward_norm, gate_weight, up_weight, down_weight, cotangent):
    group = QH // KVH
    scale = HD ** (-0.5)
    index = jnp.arange(TOK_DEV, dtype=jnp.int32)
    causal = index[None, :] <= index[:, None]

    def batch_pass(sums, inputs):
        rows_in, segment_row, rows_incoming = inputs
        cosine, sine = rotary_tables(positions_of(segment_row), HD)
        rotary = partial(head_forward, cosine=cosine, sine=sine)
        allowed = (segment_row[:, None] == segment_row[None, :]) & causal
        residual = rows_in.astype(jnp.float32)
        first_scale = lax.rsqrt(lax.optimization_barrier(jnp.mean(residual * residual, axis=-1, keepdims=True)) + epsilon)
        first_unit = residual * first_scale
        first_normed = (first_unit * attention_norm).astype(jnp.bfloat16)
        query_raw = jnp.dot(first_normed, query_weight, preferred_element_type=jnp.float32).reshape(TOK_DEV, QH, HD)
        key_raw = jnp.dot(first_normed, key_weight, preferred_element_type=jnp.float32).reshape(TOK_DEV, KVH, HD)
        value_raw = jnp.dot(first_normed, value_weight, preferred_element_type=jnp.float32).reshape(TOK_DEV, KVH, HD)
        query_rot, query_pull = jax.vjp(rotary, query_raw, query_norm)
        key_rot, key_pull = jax.vjp(rotary, key_raw, key_norm)
        query_low = query_rot.astype(jnp.bfloat16).reshape(TOK_DEV, KVH, group, HD)
        key_low = key_rot.astype(jnp.bfloat16)
        value_low = value_raw.astype(jnp.bfloat16)
        scores = jnp.einsum('qhgd,khd->hgqk', query_low.astype(jnp.float32), key_low.astype(jnp.float32)) * scale
        numerators = jnp.where(allowed, jnp.exp(scores), 0.0)
        totals = lax.optimization_barrier(jnp.sum(numerators, axis=-1, keepdims=True))
        shares = numerators / totals
        shares_low = shares.astype(jnp.bfloat16)
        mixed_low = jnp.einsum('hgqk,khd->qhgd', shares_low.astype(jnp.float32), value_low.astype(jnp.float32)).astype(jnp.bfloat16)
        mixed_flat = mixed_low.reshape(TOK_DEV, QH * HD)
        middle = residual + jnp.dot(mixed_flat, output_weight, preferred_element_type=jnp.float32)
        second_scale = lax.rsqrt(lax.optimization_barrier(jnp.mean(middle * middle, axis=-1, keepdims=True)) + epsilon)
        second_unit = middle * second_scale
        second_normed = (second_unit * feedforward_norm).astype(jnp.bfloat16)
        gate = jnp.dot(second_normed, gate_weight, preferred_element_type=jnp.float32)
        upward = jnp.dot(second_normed, up_weight, preferred_element_type=jnp.float32)
        gate_sigmoid = jax.nn.sigmoid(gate)
        gate_silu = gate * gate_sigmoid
        hidden = (gate_silu * upward).astype(jnp.bfloat16)
        rows_out = (middle + jnp.dot(hidden, down_weight, preferred_element_type=jnp.float32)).astype(jnp.bfloat16)
        hidden_back = jnp.dot(rows_incoming, down_weight.T, preferred_element_type=jnp.float32)
        down_sum = jnp.dot(hidden.T, rows_incoming, preferred_element_type=jnp.float32)
        gate_back = (hidden_back * upward * gate_sigmoid * (1.0 + gate * (1.0 - gate_sigmoid))).astype(jnp.bfloat16)
        up_back = (hidden_back * gate_silu).astype(jnp.bfloat16)
        gate_sum = jnp.dot(second_normed.T, gate_back, preferred_element_type=jnp.float32)
        up_sum = jnp.dot(second_normed.T, up_back, preferred_element_type=jnp.float32)
        second_back = jnp.dot(gate_back, gate_weight.T, preferred_element_type=jnp.float32) + jnp.dot(up_back, up_weight.T, preferred_element_type=jnp.float32)
        feed_sum = lax.optimization_barrier(jnp.sum(second_back * second_unit, axis=0))
        unit_back = second_back * feedforward_norm
        middle_back = rows_incoming.astype(jnp.float32) + second_scale * (unit_back - second_unit * lax.optimization_barrier(jnp.mean(unit_back * second_unit, axis=-1, keepdims=True)))
        middle_low = middle_back.astype(jnp.bfloat16)
        output_sum = jnp.dot(mixed_flat.T, middle_low, preferred_element_type=jnp.float32)
        mixed_back = jnp.dot(middle_low, output_weight.T, preferred_element_type=jnp.float32).astype(jnp.bfloat16).reshape(TOK_DEV, KVH, group, HD)
        delta = jnp.transpose(lax.optimization_barrier(jnp.sum(mixed_back.astype(jnp.float32) * mixed_low.astype(jnp.float32), axis=-1)), (1, 2, 0))
        share_back = jnp.einsum('qhgd,khd->hgqk', mixed_back.astype(jnp.float32), value_low.astype(jnp.float32))
        score_back = (shares * (share_back - delta[..., None])).astype(jnp.bfloat16)
        value_back = jnp.einsum('hgqk,qhgd->khd', shares_low.astype(jnp.float32), mixed_back.astype(jnp.float32))
        query_back = scale * jnp.einsum('hgqk,khd->qhgd', score_back.astype(jnp.float32), key_low.astype(jnp.float32))
        key_back = scale * jnp.einsum('hgqk,qhgd->khd', score_back.astype(jnp.float32), query_low.astype(jnp.float32))
        query_raw_back, query_gain_back = query_pull(query_back.reshape(TOK_DEV, QH, HD))
        key_raw_back, key_gain_back = key_pull(key_back)
        query_low_back = query_raw_back.reshape(TOK_DEV, QH * HD).astype(jnp.bfloat16)
        key_low_back = key_raw_back.reshape(TOK_DEV, KVH * HD).astype(jnp.bfloat16)
        value_low_back = value_back.reshape(TOK_DEV, KVH * HD).astype(jnp.bfloat16)
        query_sum = jnp.dot(first_normed.T, query_low_back, preferred_element_type=jnp.float32)
        key_sum = jnp.dot(first_normed.T, key_low_back, preferred_element_type=jnp.float32)
        value_sum = jnp.dot(first_normed.T, value_low_back, preferred_element_type=jnp.float32)
        first_back = jnp.dot(query_low_back, query_weight.T, preferred_element_type=jnp.float32)
        first_back = first_back + jnp.dot(key_low_back, key_weight.T, preferred_element_type=jnp.float32)
        first_back = first_back + jnp.dot(value_low_back, value_weight.T, preferred_element_type=jnp.float32)
        attention_sum = lax.optimization_barrier(jnp.sum(first_back * first_unit, axis=0))
        first_unit_back = first_back * attention_norm
        input_back = middle_back + first_scale * (first_unit_back - first_unit * lax.optimization_barrier(jnp.mean(first_unit_back * first_unit, axis=-1, keepdims=True)))
        terms = (attention_sum, query_sum, key_sum, value_sum, query_gain_back, key_gain_back, output_sum, feed_sum, gate_sum, up_sum, down_sum)
        sums = tuple((total + term for total, term in zip(sums, terms)))
        return (sums, (rows_out, input_back))
    shapes = [(D,), (D, QH * HD), (D, KVH * HD), (D, KVH * HD), (HD,), (HD,), (QH * HD, D), (D,), (D, FF), (D, FF), (FF, D)]
    initial = tuple((jnp.zeros(shape, jnp.float32) for shape in shapes))
    inputs = (block_input.reshape(N_DP, TOK_DEV, D), segments, cotangent.reshape(N_DP, TOK_DEV, D))
    sums, (outputs, input_grads) = lax.scan(batch_pass, initial, inputs)
    return (outputs.reshape(N_DP * TOK_DEV, D), input_grads.reshape(N_DP * TOK_DEV, D), sums[0], sums[1], sums[2], sums[3], sums[4], sums[5], sums[6], sums[7], sums[8], sums[9], sums[10])
```

```python
from functools import partial

import jax
import jax.numpy as jnp
from jax import lax
from jax.experimental import pallas as pl
from jax.experimental.pallas import tpu as pltpu
from jax.sharding import PartitionSpec as P

epsilon = 1e-06
rope_base = 1000000.0
lanes = 128
full_vmem = 67043328
chunk_limit = 262144
low = jnp.bfloat16
wide = jnp.float32


def dot(a, b, contract=((1,), (0,))):
    return lax.dot_general(a, b, (contract, ((), ())), preferred_element_type=wide)


def dot_t(a, b):
    return dot(a, b, ((1,), (1,)))


def t_dot(a, b):
    return dot(a, b, ((0,), (0,)))


def window(index, size):
    return pl.ds(pl.multiple_of(index * size, lanes), size)


def remote(source, target, send, receive, axis, index):
    return pltpu.make_async_remote_copy(
        src_ref=source,
        dst_ref=target,
        send_sem=send,
        recv_sem=receive,
        device_id={axis: index},
        device_id_type=pl.DeviceIdType.MESH,
    )


def greet(groups):
    barrier = pltpu.get_barrier_semaphore()
    total = 0
    for axis, size in groups:
        me = lax.axis_index(axis)
        for shift in range(1, size):
            pl.semaphore_signal(
                barrier,
                inc=1,
                device_id={axis: lax.rem(me + shift, size)},
                device_id_type=pl.DeviceIdType.MESH,
            )
            total += 1
    if total:
        pl.semaphore_wait(barrier, total)


def half_turn(values):
    size = values.shape[-1]
    turned = pltpu.roll(values, size // 2, axis=1)
    lane = lax.broadcasted_iota(jnp.int32, values.shape, 1)
    return jnp.where(lane < size // 2, -turned, turned)


class Exchange:
    def __init__(self, axis, size, send, receive, send_sem, receive_sem):
        self.axis, self.size = axis, size
        self.send, self.receive = send, receive
        self.send_sem, self.receive_sem = send_sem, receive_sem
        self.me = lax.axis_index(axis)

    def target(self, shift):
        return lax.rem(self.me + shift, self.size)

    def source(self, shift):
        return lax.rem(self.me + self.size - shift, self.size)

    def copy(self, shift):
        sent = self.send(shift)
        return remote(
            sent,
            self.receive.at[shift - 1],
            self.send_sem.at[shift - 1],
            self.receive_sem.at[shift - 1],
            self.axis,
            self.target(shift),
        )

    def start(self, shift):
        self.copy(shift).start()

    def arrive(self, shift):
        self.copy(shift).wait_recv()

    def finish(self):
        for shift in range(1, self.size):
            self.copy(shift).wait_send()


class Ranked(Exchange):
    def copy(self, shift):
        return remote(
            self.send(shift),
            self.receive.at[self.me],
            self.send_sem.at[shift - 1],
            self.receive_sem.at[shift - 1],
            self.axis,
            self.target(shift),
        )

    def total(self, rows):
        result = self.receive[0, rows]
        for member in range(1, self.size):
            result = result + self.receive[member, rows]
        return result


def each_tile(rows, body):
    tile = lanes if rows % lanes == 0 else rows

    def step(index, carry):
        body(pl.ds(pl.multiple_of(index * tile, tile), tile), index * tile, tile)
        return carry

    lax.fori_loop(0, rows // tile, step, 0)


def forward_kernel(
    rows_of,
    cols_of,
    x,
    seg_row,
    seg_col,
    inverse,
    gain1,
    wq,
    wk,
    wv,
    qn,
    kn,
    wo,
    gain2,
    wg,
    wu,
    wd,
    ct,
    n1,
    fs,
    raw,
    lows,
    shares,
    trig,
    mixed,
    mid,
    ss,
    n2,
    hid,
    gub,
    unit,
    pq_own,
    pq_s,
    pq_r,
    ph_own,
    ph_s,
    ph_r,
    pg_own,
    pg_s,
    pg_r,
    mixed_r,
    stat_s,
    stat_r,
    ox_s,
    ox_r,
    row_send,
    row_recv,
    stat_send,
    stat_recv,
    col_send,
    col_recv,
):
    tokens, depth = x.shape
    width = depth * rows_of
    qw, kw, fw = wq.shape[1] // rows_of, wk.shape[1] // rows_of, wg.shape[1] // rows_of
    size = qn.shape[1]
    heads, key_heads = qw // size, kw // size
    group = heads // key_heads
    scale = size ** (-0.5)
    me = lax.axis_index("row")
    greet((("row", rows_of), ("col", cols_of)))

    def row_exchange(kind, send, receive):
        return Exchange("row", rows_of, send, receive, row_send.at[kind], row_recv.at[kind])

    def stat_exchange(kind):
        return Ranked(
            "row",
            rows_of,
            lambda shift: stat_s.at[kind],
            stat_r.at[kind],
            stat_send.at[kind],
            stat_recv.at[kind],
        )

    stat1 = stat_exchange(0)

    def prepare(rows, start, tile):
        value = x[rows, :].astype(wide)
        square = jnp.broadcast_to(jnp.sum(value * value, axis=1, keepdims=True), (tile, lanes))
        stat_s[0, rows] = square
        stat_r[0, me, rows] = square
        unit[rows, :] = (value * gain1[...]).astype(low)

    each_tile(tokens, prepare)
    for shift in range(1, rows_of):
        stat1.start(shift)

    def project(index, target, slot):
        u = unit[...]
        q = dot(u, wq[:, window(index, qw)])
        k = dot(u, wk[:, window(index, kw)])
        v = dot(u, wv[:, window(index, kw)])
        kind = target.dtype
        if slot is None:
            target[:, :qw] = q.astype(kind)
            target[:, qw : qw + kw] = k.astype(kind)
            target[:, qw + kw :] = v.astype(kind)
        else:
            target[slot, :, :qw] = q.astype(kind)
            target[slot, :, qw : qw + kw] = k.astype(kind)
            target[slot, :, qw + kw :] = v.astype(kind)

    qkv = row_exchange(0, lambda shift: pq_s.at[shift - 1], pq_r)
    for shift in range(1, rows_of):
        project(qkv.target(shift), pq_s, shift - 1)
        qkv.start(shift)
    project(me, pq_own, None)

    back = row_exchange(1, lambda shift: ph_s.at[shift - 1], ph_r)
    for shift in range(1, rows_of):
        ph_s[shift - 1] = dot_t(ct[...], wd[window(back.target(shift), fw), :]).astype(low)
        back.start(shift)
    ph_own[...] = dot_t(ct[...], wd[window(me, fw), :])

    def tables(rows, start, tile):
        key = lax.broadcasted_iota(jnp.int32, (tile, tokens), 1)
        query = lax.broadcasted_iota(jnp.int32, (tile, tokens), 0) + start
        allowed = (seg_col[rows, :] == seg_row[...]) & (key <= query)
        count = jnp.sum(jnp.where(allowed, 1.0, 0.0), axis=1, keepdims=True) - 1.0
        angle = count * inverse[...]
        trig[0, rows, :] = jnp.cos(angle)
        trig[1, rows, :] = jnp.sin(angle)

    each_tile(tokens, tables)

    for shift in range(1, rows_of):
        stat1.arrive(shift)
        qkv.arrive(shift)

    def heads_in(rows, start, tile):
        first = lax.rsqrt(stat1.total(rows) / width + epsilon)
        fs[rows, :] = first
        first = first[:, :1]
        n1[rows, :] = (x[rows, :].astype(wide) * first * gain1[...]).astype(low)
        value = pq_own[rows, :]
        for shift in range(1, rows_of):
            value = value + pq_r[shift - 1, rows, :].astype(wide)
        value = value * first
        raw[rows, :] = value[:, : qw + kw]
        cosine, sine = trig[0, rows, :], trig[1, rows, :]
        for head in range(heads + key_heads):
            piece = value[:, head * size : (head + 1) * size]
            gain = qn[...] if head < heads else kn[...]
            norm = lax.rsqrt(jnp.mean(piece * piece, axis=1, keepdims=True) + epsilon)
            normed = piece * norm * gain
            rotated = normed * cosine + half_turn(normed) * sine
            lows[rows, head * size : (head + 1) * size] = rotated.astype(low)
        lows[rows, qw + kw :] = value[:, qw + kw :].astype(low)

    each_tile(tokens, heads_in)

    def attend(rows, start, tile):
        key = lax.broadcasted_iota(jnp.int32, (tile, tokens), 1)
        query = lax.broadcasted_iota(jnp.int32, (tile, tokens), 0) + start
        allowed = (seg_col[rows, :] == seg_row[...]) & (key <= query)
        for head in range(heads):
            pair = head // group
            keys = lows[:, qw + pair * size : qw + (pair + 1) * size]
            values = lows[:, qw + kw + pair * size : qw + kw + (pair + 1) * size]
            scores = dot_t(lows[rows, head * size : (head + 1) * size], keys) * scale
            numerators = jnp.where(allowed, jnp.exp(scores), 0.0)
            share = numerators / jnp.sum(numerators, axis=1, keepdims=True)
            shares[head, rows, :] = share
            mixed[0, rows, head * size : (head + 1) * size] = dot(
                share.astype(low), values
            ).astype(low)

    each_tile(tokens, attend)

    gather = row_exchange(2, lambda shift: mixed.at[0], mixed_r)
    for shift in range(1, rows_of):
        gather.start(shift)
    ox_s[...] = dot(mixed[0], wo[window(me, qw), :])
    for shift in range(1, rows_of):
        gather.arrive(shift)
        mixed[shift] = mixed_r[shift - 1]
        ox_s[...] += dot(mixed_r[shift - 1], wo[window(gather.source(shift), qw), :])
    column = Exchange("col", cols_of, lambda shift: ox_s, ox_r, col_send, col_recv)
    for shift in range(1, cols_of):
        column.start(shift)
    for shift in range(1, cols_of):
        column.arrive(shift)

    stat2 = stat_exchange(1)

    def middle(rows, start, tile):
        value = ox_s[rows, :]
        for shift in range(1, cols_of):
            value = value + ox_r[shift - 1, rows, :]
        value = x[rows, :].astype(wide) + value
        mid[rows, :] = value
        square = jnp.broadcast_to(jnp.sum(value * value, axis=1, keepdims=True), (tile, lanes))
        stat_s[1, rows] = square
        stat_r[1, me, rows] = square
        unit[rows, :] = (value * gain2[...]).astype(low)

    each_tile(tokens, middle)
    for shift in range(1, rows_of):
        stat2.start(shift)

    feed = row_exchange(3, lambda shift: pg_s.at[shift - 1], pg_r)
    for shift in range(1, rows_of):
        columns = window(feed.target(shift), fw)
        pg_s[shift - 1, :, :fw] = dot(unit[...], wg[:, columns]).astype(low)
        pg_s[shift - 1, :, fw:] = dot(unit[...], wu[:, columns]).astype(low)
        feed.start(shift)
    pg_own[:, :fw] = dot(unit[...], wg[:, window(me, fw)])
    pg_own[:, fw:] = dot(unit[...], wu[:, window(me, fw)])
    for shift in range(1, rows_of):
        stat2.arrive(shift)
        back.arrive(shift)

    def scale_rows(rows, start, tile):
        second = lax.rsqrt(stat2.total(rows) / width + epsilon)
        ss[rows, :] = second
        n2[rows, :] = (mid[rows, :] * second[:, :1] * gain2[...]).astype(low)

    each_tile(tokens, scale_rows)
    for shift in range(1, rows_of):
        feed.arrive(shift)

    def activate(rows, start, tile):
        second = ss[rows, :1]
        gate = pg_own[rows, :fw]
        upward = pg_own[rows, fw:]
        for shift in range(1, rows_of):
            gate = gate + pg_r[shift - 1, rows, :fw].astype(wide)
            upward = upward + pg_r[shift - 1, rows, fw:].astype(wide)
        gate = gate * second
        upward = upward * second
        behind = ph_own[rows, :]
        for shift in range(1, rows_of):
            behind = behind + ph_r[shift - 1, rows, :].astype(wide)
        sigmoid = jax.nn.sigmoid(gate)
        silu = gate * sigmoid
        hid[rows, :] = (silu * upward).astype(low)
        gub[rows, :fw] = (behind * upward * sigmoid * (1.0 + gate * (1.0 - sigmoid))).astype(low)
        gub[rows, fw:] = (behind * silu).astype(low)

    each_tile(tokens, activate)
    for exchange in (stat1, qkv, back, gather, column, stat2, feed):
        exchange.finish()


def backward_kernel(
    rows_of,
    cols_of,
    x,
    ct,
    n1,
    fs,
    raw,
    lows,
    shares,
    trig,
    mixed,
    mid,
    ss,
    n2,
    hid,
    gub,
    gain1,
    gain2,
    qn,
    kn,
    wq,
    wk,
    wv,
    wo,
    wg,
    wu,
    wd,
    bo,
    ig,
    small,
    gq,
    gk,
    gv,
    go,
    gg,
    gu,
    gd,
    hid_r,
    gub_r,
    n_t,
    mb,
    ml,
    pm_own,
    pm_s,
    pm_r,
    sl,
    sb,
    dqkv,
    dqkv_r,
    gains,
    stat_s,
    stat_r,
    ox_s,
    ox_r,
    row_send,
    row_recv,
    stat_send,
    stat_recv,
    col_send,
    col_recv,
):
    tokens, depth = x.shape
    width = depth * rows_of
    qw, kw, fw = wq.shape[1] // rows_of, wk.shape[1] // rows_of, wg.shape[1] // rows_of
    size = qn.shape[1]
    heads, key_heads = qw // size, kw // size
    group = heads // key_heads
    scale = size ** (-0.5)
    me = lax.axis_index("row")
    greet((("row", rows_of), ("col", cols_of)))

    def row_exchange(kind, send, receive):
        return Exchange("row", rows_of, send, receive, row_send.at[kind], row_recv.at[kind])

    def stat_exchange(kind):
        return Ranked(
            "row",
            rows_of,
            lambda shift: stat_s.at[kind],
            stat_r.at[kind],
            stat_send.at[kind],
            stat_recv.at[kind],
        )

    def column_exchange(kind):
        return Exchange(
            "col",
            cols_of,
            lambda shift: ox_s.at[kind],
            ox_r.at[kind],
            col_send.at[kind],
            col_recv.at[kind],
        )

    def column_sum(kind, rows):
        value = ox_s[kind, rows, :]
        for shift in range(1, cols_of):
            value = value + ox_r[kind, shift - 1, rows, :]
        return value

    hide = row_exchange(0, lambda shift: hid, hid_r)
    gates = row_exchange(1, lambda shift: gub, gub_r)
    for shift in range(1, rows_of):
        hide.start(shift)
    for shift in range(1, rows_of):
        gates.start(shift)
    body = pl.ds(0, tokens)
    cut = ct[...]
    for shift in range(rows_of):
        if shift:
            hide.arrive(shift)
        piece = hid[...] if shift == 0 else hid_r[shift - 1]
        index = window(hide.source(shift), fw)
        part = dot(piece, wd[index, :])
        if shift == 0:
            ox_s[0, body, :] = part
        else:
            ox_s[0, body, :] += part
        gd[index, :] = t_dot(piece, cut).astype(low)
    column0 = column_exchange(0)
    for shift in range(1, cols_of):
        column0.start(shift)
    n_t[...] = n2[...].T
    for shift in range(rows_of):
        if shift:
            gates.arrive(shift)
        piece = gub if shift == 0 else gub_r.at[shift - 1]
        index = window(gates.source(shift), fw)
        part = dot_t(piece[:, :fw], wg[:, index]) + dot_t(piece[:, fw:], wu[:, index])
        if shift == 0:
            ox_s[1, body, :] = part
        else:
            ox_s[1, body, :] += part
    column1 = column_exchange(1)
    for shift in range(1, cols_of):
        column1.start(shift)
    for shift in range(1, cols_of):
        column0.arrive(shift)

    def result(rows, start, tile):
        bo[rows, :] = (mid[rows, :] + column_sum(0, rows)).astype(low)

    each_tile(tokens, result)
    for shift in range(1, cols_of):
        column1.arrive(shift)

    stat2 = stat_exchange(0)
    small[...] = jnp.zeros_like(small)
    gains[...] = jnp.zeros_like(gains)

    def feed_stat(rows, start, tile):
        back = column_sum(1, rows)
        unit = mid[rows, :] * ss[rows, :1]
        small[1:2, :] += jnp.sum(back * unit, axis=0, keepdims=True)
        inner = jnp.sum(back * gain2[...] * unit, axis=1, keepdims=True)
        inner = jnp.broadcast_to(inner, (tile, lanes))
        stat_s[0, rows] = inner
        stat_r[0, me, rows] = inner

    each_tile(tokens, feed_stat)
    pad = pl.ds(tokens, 8)
    stat_s[0, pad] = jnp.zeros((8, lanes), wide)
    for shift in range(1, rows_of):
        stat2.start(shift)
    for shift in range(rows_of):
        piece = gub if shift == 0 else gub_r.at[shift - 1]
        index = window(gates.source(shift), fw)
        gg[:, index] = dot(n_t[...], piece[:, :fw]).astype(low)
    for shift in range(1, rows_of):
        stat2.arrive(shift)

    def middle_back(rows, start, tile):
        second = ss[rows, :1]
        unit = mid[rows, :] * second
        inner = stat2.total(rows)[:, :1] / width
        value = ct[rows, :].astype(wide) + second * (
            column_sum(1, rows) * gain2[...] - unit * inner
        )
        mb[rows, :] = value
        ml[rows, :] = value.astype(low)

    each_tile(tokens, middle_back)
    blend = row_exchange(2, lambda shift: pm_s.at[shift - 1], pm_r)
    for shift in range(1, rows_of):
        pm_s[shift - 1] = dot_t(ml[...], wo[window(blend.target(shift), qw), :]).astype(low)
        blend.start(shift)
    pm_own[...] = dot_t(ml[...], wo[window(me, qw), :])
    for shift in range(rows_of):
        index = window(blend.source(shift), qw)
        go[index, :] = t_dot(mixed[shift], ml[...]).astype(low)
    for shift in range(1, rows_of):
        blend.arrive(shift)

    def share_back(rows, start, tile):
        value = pm_own[rows, :]
        for shift in range(1, rows_of):
            value = value + pm_r[shift - 1, rows, :].astype(wide)
        incoming = value.astype(low)
        pm_s[0, rows, :] = incoming
        product = incoming.astype(wide) * mixed[0, rows, :].astype(wide)
        for head in range(heads):
            pair = head // group
            part = slice(head * size, (head + 1) * size)
            values = lows[:, qw + kw + pair * size : qw + kw + (pair + 1) * size]
            delta = jnp.sum(product[:, part], axis=1, keepdims=True)
            share = shares[head, rows, :]
            sl[head, rows, :] = share.astype(low)
            sb[head, rows, :] = (share * (dot_t(incoming[:, part], values) - delta)).astype(low)

    blend.finish()
    each_tile(tokens, share_back)
    n_t[...] = n1[...].T

    def pull(head, back, gain, row):
        raw_piece = raw[:, head * size : (head + 1) * size]
        norm = lax.rsqrt(jnp.mean(raw_piece * raw_piece, axis=1, keepdims=True) + epsilon)
        unit = raw_piece * norm
        normed_back = back * trig[0] - half_turn(back * trig[1])
        gains[row : row + 1, :] += jnp.sum(normed_back * unit, axis=0, keepdims=True)
        unit_back = normed_back * gain
        return norm * (unit_back - unit * jnp.mean(unit_back * unit, axis=1, keepdims=True))

    for pair in range(key_heads):
        keys = lows[:, qw + pair * size : qw + (pair + 1) * size]
        key_back = jnp.zeros((tokens, size), wide)
        value_back = jnp.zeros((tokens, size), wide)
        for head in range(pair * group, (pair + 1) * group):
            part = slice(head * size, (head + 1) * size)
            value_back = value_back + t_dot(sl[head], pm_s[0, :, part])
            key_back = key_back + scale * t_dot(sb[head], lows[:, part])
            query_back = scale * dot(sb[head], keys)
            dqkv[:, part] = pull(head, query_back, qn[...], 0).astype(low)
        spot = qw + pair * size
        dqkv[:, spot : spot + size] = pull(heads + pair, key_back, kn[...], 1).astype(low)
        spot = qw + kw + pair * size
        dqkv[:, spot : spot + size] = value_back.astype(low)

    deliver = row_exchange(3, lambda shift: dqkv, dqkv_r)
    for shift in range(1, rows_of):
        deliver.start(shift)
    for shift in range(rows_of):
        if shift:
            deliver.arrive(shift)
        piece = dqkv if shift == 0 else dqkv_r.at[shift - 1]
        source = deliver.source(shift)
        part = dot_t(piece[:, :qw], wq[:, window(source, qw)])
        part = part + dot_t(piece[:, qw : qw + kw], wk[:, window(source, kw)])
        part = part + dot_t(piece[:, qw + kw :], wv[:, window(source, kw)])
        if shift == 0:
            ox_s[2, body, :] = part
        else:
            ox_s[2, body, :] += part
    ox_s[2, pad, :] = jnp.zeros((8, depth), wide)
    ox_s[2, pad, :lanes] = gains[...]
    column2 = column_exchange(2)
    for shift in range(1, cols_of):
        column2.start(shift)
    for shift in range(rows_of):
        piece = dqkv if shift == 0 else dqkv_r.at[shift - 1]
        source = deliver.source(shift)
        gq[:, window(source, qw)] = dot(n_t[...], piece[:, :qw]).astype(low)
        gk[:, window(source, kw)] = dot(n_t[...], piece[:, qw : qw + kw]).astype(low)
        gv[:, window(source, kw)] = dot(n_t[...], piece[:, qw + kw :]).astype(low)
    for shift in range(1, cols_of):
        column2.arrive(shift)

    stat1 = stat_exchange(1)

    def first_stat(rows, start, tile):
        back = column_sum(2, rows)
        unit = x[rows, :].astype(wide) * fs[rows, :1]
        small[0:1, :] += jnp.sum(back * unit, axis=0, keepdims=True)
        inner = jnp.sum(back * gain1[...] * unit, axis=1, keepdims=True)
        inner = jnp.broadcast_to(inner, (tile, lanes))
        stat_s[1, rows] = inner
        stat_r[1, me, rows] = inner

    each_tile(tokens, first_stat)
    summed = column_sum(2, pad)[:, :lanes]
    stat_s[1, pad] = summed
    stat_r[1, me, pad] = summed
    for shift in range(1, rows_of):
        stat1.start(shift)
    n_t[...] = n2[...].T
    for shift in range(rows_of):
        piece = gub if shift == 0 else gub_r.at[shift - 1]
        index = window(gates.source(shift), fw)
        gu[:, index] = dot(n_t[...], piece[:, fw:]).astype(low)
    for shift in range(1, rows_of):
        stat1.arrive(shift)

    def finish(rows, start, tile):
        first = fs[rows, :1]
        unit = x[rows, :].astype(wide) * first
        inner = stat1.total(rows)[:, :1] / width
        ig[rows, :] = mb[rows, :] + first * (column_sum(2, rows) * gain1[...] - unit * inner)

    each_tile(tokens, finish)
    small[8:16, :lanes] = stat1.total(pad)
    for exchange in (hide, gates, column0, column1, stat2, deliver, column2, stat1):
        exchange.finish()


def chunks_of(shape):
    rows, columns = shape
    count = 1
    while rows % count or (rows // count) * columns > chunk_limit:
        count += 1
    return count, rows // count


def combine_kernel(members, shapes, *refs):
    count = len(shapes)
    small, *own = refs[: count + 1]
    small_out, *out = refs[count + 1 : 2 * count + 2]
    near = refs[2 * count + 2 : 3 * count + 2]
    far = refs[3 * count + 2 : 4 * count + 2]
    small_r, in_send, near_sem, far_sem, out_send, small_send, small_recv = refs[4 * count + 2 :]
    greet((("dp", members),))
    me = lax.axis_index("dp")
    half = members // 2
    left = me < half
    place = jnp.where(left, half - 1 - me, me - half)
    inner = jnp.where(left, me + 1, me - 1)
    outer = jnp.where(left, jnp.maximum(me - 1, 0), jnp.minimum(me + 1, members - 1))
    is_mid = place == 0
    has_outer = place < half - 1
    ranked = Ranked("dp", members, lambda shift: small, small_r, small_send, small_recv)
    small_r[me] = small[...]
    for shift in range(1, members):
        ranked.start(shift)

    bases, base = [], 0
    for shape in shapes:
        bases.append(base)
        base += chunks_of(shape)[0]

    def inward(which, index, source, target, target_sem):
        rows = chunks_of(shapes[which])[1]
        spot = pl.ds(pl.multiple_of(index * rows, 16), rows)
        slot = bases[which] + index
        return remote(
            source[which].at[spot],
            target[which].at[spot],
            in_send.at[slot],
            target_sem.at[slot],
            "dp",
            inner,
        )

    def outward(which, index):
        rows = chunks_of(shapes[which])[1]
        spot = pl.ds(pl.multiple_of(index * rows, 16), rows)
        slot = bases[which] + index
        return remote(
            out[which].at[spot],
            far[which].at[spot],
            out_send.at[slot],
            far_sem.at[slot],
            "dp",
            outer,
        )

    def add(which, index, first, second, target):
        rows = chunks_of(shapes[which])[1]
        spot = pl.ds(pl.multiple_of(index * rows, 16), rows)
        total = first[which][spot, :].astype(wide) + second[which][spot, :].astype(wide)
        target[which][spot, :] = total.astype(low)

    def send_in(which, index):
        target, sem = near, near_sem

        @pl.when(has_outer)
        def _():
            inward(which, index, near, near, near_sem).wait_recv()
            add(which, index, own, near, near)

            @pl.when(is_mid)
            def _():
                inward(which, index, near, far, far_sem).start()

            @pl.when(jnp.logical_not(is_mid))
            def _():
                inward(which, index, near, near, near_sem).start()

        @pl.when(jnp.logical_not(has_outer))
        def _():
            @pl.when(is_mid)
            def _():
                inward(which, index, own, far, far_sem).start()

            @pl.when(jnp.logical_not(is_mid))
            def _():
                inward(which, index, own, near, near_sem).start()

    def finish_chunk(which, index):
        inward(which, index, own, far, far_sem).wait_recv()

        @pl.when(is_mid)
        def _():
            @pl.when(has_outer)
            def _():
                add(which, index, near, far, out)

            @pl.when(jnp.logical_not(has_outer))
            def _():
                add(which, index, own, far, out)

        @pl.when(jnp.logical_not(is_mid))
        def _():
            rows = chunks_of(shapes[which])[1]
            spot = pl.ds(pl.multiple_of(index * rows, 16), rows)
            out[which][spot, :] = far[which][spot, :]

        @pl.when(has_outer)
        def _():
            outward(which, index).start()

    def over(which, body):
        def step(index, carry):
            body(index)
            return carry

        lax.fori_loop(0, chunks_of(shapes[which])[0], step, 0)

    @pl.when(is_mid)
    def _():
        for which in range(count):

            def both(index, which=which):
                send_in(which, index)

                @pl.when(index > 0)
                def _():
                    finish_chunk(which, index - 1)

            over(which, both)
            finish_chunk(which, chunks_of(shapes[which])[0] - 1)

    @pl.when(jnp.logical_not(is_mid))
    def _():
        for which in range(count):
            over(which, lambda index, which=which: send_in(which, index))
        for which in range(count):
            over(which, lambda index, which=which: finish_chunk(which, index))

    for shift in range(1, members):
        ranked.arrive(shift)
    result = small_r[0]
    for member in range(1, members):
        result = result + small_r[member]
    small_out[...] = result
    ranked.finish()
    for which in range(count):

        def drain(index, which=which):
            inward(which, index, own, near, near_sem).wait_send()

            @pl.when(has_outer)
            def _():
                outward(which, index).wait_send()

        over(which, drain)


def vmem(shape, kind):
    return pltpu.VMEM(shape, kind)


def call(kernel, shapes, scratch, identity, arguments):
    inside = pl.BlockSpec(memory_space=pltpu.VMEM)
    return pl.pallas_call(
        kernel,
        out_shape=tuple(jax.ShapeDtypeStruct(shape, kind) for shape, kind in shapes),
        in_specs=[inside] * len(arguments),
        out_specs=tuple([inside] * len(shapes)),
        scratch_shapes=scratch,
        compiler_params=pltpu.CompilerParams(
            collective_id=identity, has_side_effects=True, vmem_limit_bytes=full_vmem
        ),
    )(*arguments)


def per_device(
    block_input,
    segments,
    attention_norm,
    query_weight,
    key_weight,
    value_weight,
    query_norm,
    key_norm,
    output_weight,
    feedforward_norm,
    gate_weight,
    up_weight,
    down_weight,
    cotangent,
):
    rows_of, cols_of, members = (lax.axis_size(name) for name in ("row", "col", "dp"))
    tokens, depth = block_input.shape
    size = query_norm.shape[0]
    qw, kw, fw = (
        weight.shape[1] // rows_of for weight in (query_weight, key_weight, gate_weight)
    )
    heads = qw // size
    others, beside = max(rows_of - 1, 1), max(cols_of - 1, 1)
    half = size // 2
    inverse = rope_base ** (-2.0 * jnp.arange(half, dtype=wide) / size)
    inverse = jnp.concatenate([inverse, inverse])[None, :]
    seg_row = segments.reshape(1, tokens)
    seg_col = segments.reshape(tokens, 1)
    gain1, gain2 = attention_norm[None, :], feedforward_norm[None, :]
    qn, kn = query_norm[None, :], key_norm[None, :]
    total = qw + 2 * kw
    dma = pltpu.SemaphoreType.DMA

    def sems(kinds):
        return [
            dma((4, others)),
            dma((4, others)),
            dma((2, others)),
            dma((2, others)),
            dma((kinds, beside)) if kinds > 1 else dma((beside,)),
            dma((kinds, beside)) if kinds > 1 else dma((beside,)),
        ]

    saved = call(
        partial(forward_kernel, rows_of, cols_of),
        (
            ((tokens, depth), low),
            ((tokens, lanes), wide),
            ((tokens, qw + kw), wide),
            ((tokens, total), low),
            ((heads, tokens, tokens), wide),
            ((2, tokens, size), wide),
            ((rows_of, tokens, qw), low),
            ((tokens, depth), wide),
            ((tokens, lanes), wide),
            ((tokens, depth), low),
            ((tokens, fw), low),
            ((tokens, 2 * fw), low),
        ),
        [
            vmem((tokens, depth), low),
            vmem((tokens, total), wide),
            vmem((others, tokens, total), low),
            vmem((others, tokens, total), low),
            vmem((tokens, fw), wide),
            vmem((others, tokens, fw), low),
            vmem((others, tokens, fw), low),
            vmem((tokens, 2 * fw), wide),
            vmem((others, tokens, 2 * fw), low),
            vmem((others, tokens, 2 * fw), low),
            vmem((others, tokens, qw), low),
            vmem((2, tokens, lanes), wide),
            vmem((2, rows_of, tokens, lanes), wide),
            vmem((tokens, depth), wide),
            vmem((beside, tokens, depth), wide),
        ]
        + sems(1),
        0,
        (
            block_input,
            seg_row,
            seg_col,
            inverse,
            gain1,
            query_weight,
            key_weight,
            value_weight,
            qn,
            kn,
            output_weight,
            gain2,
            gate_weight,
            up_weight,
            down_weight,
            cotangent,
        ),
    )
    weights = (query_weight, key_weight, value_weight, output_weight, gate_weight, up_weight)
    shapes = [weight.shape for weight in weights] + [down_weight.shape]
    block_output, input_gradient, small, *partials = call(
        partial(backward_kernel, rows_of, cols_of),
        (
            ((tokens, depth), low),
            ((tokens, depth), wide),
            ((16, depth), wide),
            *((shape, low) for shape in shapes),
        ),
        [
            vmem((others, tokens, fw), low),
            vmem((others, tokens, 2 * fw), low),
            vmem((depth, tokens), low),
            vmem((tokens, depth), wide),
            vmem((tokens, depth), low),
            vmem((tokens, qw), wide),
            vmem((others, tokens, qw), low),
            vmem((others, tokens, qw), low),
            vmem((heads, tokens, tokens), low),
            vmem((heads, tokens, tokens), low),
            vmem((tokens, total), low),
            vmem((others, tokens, total), low),
            vmem((8, lanes), wide),
            vmem((2, tokens + 8, lanes), wide),
            vmem((2, rows_of, tokens + 8, lanes), wide),
            vmem((3, tokens + 8, depth), wide),
            vmem((3, beside, tokens + 8, depth), wide),
        ]
        + sems(3),
        1,
        (
            block_input,
            cotangent,
            *saved,
            gain1,
            gain2,
            qn,
            kn,
            *weights,
            down_weight,
        ),
    )
    if members > 1:
        slots = sum(chunks_of(shape)[0] for shape in shapes)
        small, *partials = call(
            partial(combine_kernel, members, shapes),
            (((16, depth), wide), *((shape, low) for shape in shapes)),
            [vmem(shape, low) for shape in shapes] * 2
            + [vmem((members, 16, depth), wide)]
            + [dma((slots,))] * 4
            + [dma((members - 1,))] * 2,
            2,
            (small, *partials),
        )
    gq, gk, gv, go, gg, gu, gd = (partial_sum.astype(wide) for partial_sum in partials)
    return (
        block_output,
        input_gradient,
        small[0],
        gq,
        gk,
        gv,
        small[8, :size],
        small[9, :size],
        go,
        small[1],
        gg,
        gu,
        gd,
    )


def solution(mesh):
    return jax.shard_map(
        per_device,
        mesh=mesh,
        in_specs=(
            P("dp", "row"),
            P("dp", None),
            P("row"),
            P("row", "col"),
            P("row", "col"),
            P("row", "col"),
            P(),
            P(),
            P("col", "row"),
            P("row"),
            P("row", "col"),
            P("row", "col"),
            P("col", "row"),
            P("dp", "row"),
        ),
        out_specs=(
            P("dp", "row"),
            P("dp", "row"),
            P("row"),
            P("row", "col"),
            P("row", "col"),
            P("row", "col"),
            P(),
            P(),
            P("col", "row"),
            P("row"),
            P("row", "col"),
            P("row", "col"),
            P("col", "row"),
        ),
        check_vma=False,
    )
```

```python
from functools import partial

import jax
import jax.numpy as jnp
from jax import lax
from jax.experimental import pallas as pl
from jax.experimental.pallas import tpu as pltpu
from jax.sharding import PartitionSpec as P

epsilon = 1e-06
rope_base = 1000000.0
lanes = 128
full_vmem = 67043328
chunk_limit = 262144
low = jnp.bfloat16
wide = jnp.float32


def dot(a, b, contract=((1,), (0,))):
    return lax.dot_general(a, b, (contract, ((), ())), preferred_element_type=wide)


def dot_t(a, b):
    return dot(a, b, ((1,), (1,)))


def t_dot(a, b):
    return dot(a, b, ((0,), (0,)))


def window(index, size):
    return pl.ds(pl.multiple_of(index * size, lanes), size)


def remote(source, target, send, receive, axis, index):
    return pltpu.make_async_remote_copy(
        src_ref=source,
        dst_ref=target,
        send_sem=send,
        recv_sem=receive,
        device_id={axis: index},
        device_id_type=pl.DeviceIdType.MESH,
    )


def greet(groups):
    barrier = pltpu.get_barrier_semaphore()
    total = 0
    for axis, size in groups:
        me = lax.axis_index(axis)
        for shift in range(1, size):
            pl.semaphore_signal(
                barrier,
                inc=1,
                device_id={axis: lax.rem(me + shift, size)},
                device_id_type=pl.DeviceIdType.MESH,
            )
            total += 1
    if total:
        pl.semaphore_wait(barrier, total)


def half_turn(values):
    size = values.shape[-1]
    turned = pltpu.roll(values, size // 2, axis=1)
    lane = lax.broadcasted_iota(jnp.int32, values.shape, 1)
    return jnp.where(lane < size // 2, -turned, turned)


class Exchange:
    def __init__(self, axis, size, send, receive, send_sem, receive_sem):
        self.axis, self.size = axis, size
        self.send, self.receive = send, receive
        self.send_sem, self.receive_sem = send_sem, receive_sem
        self.me = lax.axis_index(axis)

    def target(self, shift):
        return lax.rem(self.me + shift, self.size)

    def source(self, shift):
        return lax.rem(self.me + self.size - shift, self.size)

    def copy(self, shift):
        sent = self.send(shift)
        return remote(
            sent,
            self.receive.at[shift - 1],
            self.send_sem.at[shift - 1],
            self.receive_sem.at[shift - 1],
            self.axis,
            self.target(shift),
        )

    def start(self, shift):
        self.copy(shift).start()

    def arrive(self, shift):
        self.copy(shift).wait_recv()

    def finish(self):
        for shift in range(1, self.size):
            self.copy(shift).wait_send()


class Ranked(Exchange):
    def copy(self, shift):
        return remote(
            self.send(shift),
            self.receive.at[self.me],
            self.send_sem.at[shift - 1],
            self.receive_sem.at[shift - 1],
            self.axis,
            self.target(shift),
        )

    def total(self, rows):
        result = self.receive[0, rows]
        for member in range(1, self.size):
            result = result + self.receive[member, rows]
        return result


def each_tile(rows, body):
    tile = lanes if rows % lanes == 0 else rows

    def step(index, carry):
        body(pl.ds(pl.multiple_of(index * tile, tile), tile), index * tile, tile)
        return carry

    lax.fori_loop(0, rows // tile, step, 0)


def forward_kernel(
    rows_of,
    cols_of,
    need,
    x,
    seg_row,
    seg_col,
    inverse,
    gain1,
    wq,
    wk,
    wv,
    qn,
    kn,
    wo,
    gain2,
    wg,
    wu,
    wd,
    ct,
    n1,
    fs,
    raw,
    lows,
    shares,
    trig,
    mixed,
    mid,
    ss,
    n2,
    hid,
    gub,
    unit,
    pq_own,
    pq_s,
    pq_r,
    ph_own,
    ph_s,
    ph_r,
    pg_own,
    pg_s,
    pg_r,
    mixed_r,
    stat_s,
    stat_r,
    ox_s,
    ox_r,
    row_send,
    row_recv,
    stat_send,
    stat_recv,
    col_send,
    col_recv,
):
    tokens, depth = x.shape
    width = depth * rows_of
    qw, kw, fw = wq.shape[1] // rows_of, wk.shape[1] // rows_of, wg.shape[1] // rows_of
    size = qn.shape[1]
    heads, key_heads = qw // size, kw // size
    group = heads // key_heads
    scale = size ** (-0.5)
    me = lax.axis_index("row")
    greet((("row", rows_of), ("col", cols_of)))

    def row_exchange(kind, send, receive):
        return Exchange("row", rows_of, send, receive, row_send.at[kind], row_recv.at[kind])

    def stat_exchange(kind):
        return Ranked(
            "row",
            rows_of,
            lambda shift: stat_s.at[kind],
            stat_r.at[kind],
            stat_send.at[kind],
            stat_recv.at[kind],
        )

    stat1 = stat_exchange(0)

    def prepare(rows, start, tile):
        value = x[rows, :].astype(wide)
        square = jnp.broadcast_to(jnp.sum(value * value, axis=1, keepdims=True), (tile, lanes))
        stat_s[0, rows] = square
        stat_r[0, me, rows] = square
        unit[rows, :] = (value * gain1[...]).astype(low)

    each_tile(tokens, prepare)
    for shift in range(1, rows_of):
        stat1.start(shift)

    def project(index, target, slot):
        u = unit[...]
        q = dot(u, wq[:, window(index, qw)])
        k = dot(u, wk[:, window(index, kw)])
        v = dot(u, wv[:, window(index, kw)])
        kind = target.dtype
        if slot is None:
            target[:, :qw] = q.astype(kind)
            target[:, qw : qw + kw] = k.astype(kind)
            target[:, qw + kw :] = v.astype(kind)
        else:
            target[slot, :, :qw] = q.astype(kind)
            target[slot, :, qw : qw + kw] = k.astype(kind)
            target[slot, :, qw + kw :] = v.astype(kind)

    qkv = row_exchange(0, lambda shift: pq_s.at[shift - 1], pq_r)
    for shift in range(1, rows_of):
        project(qkv.target(shift), pq_s, shift - 1)
        qkv.start(shift)
    project(me, pq_own, None)

    need("wd", "ct")
    back = row_exchange(1, lambda shift: ph_s.at[shift - 1], ph_r)
    for shift in range(1, rows_of):
        ph_s[shift - 1] = dot_t(ct[...], wd[window(back.target(shift), fw), :]).astype(low)
        back.start(shift)
    ph_own[...] = dot_t(ct[...], wd[window(me, fw), :])

    def tables(rows, start, tile):
        key = lax.broadcasted_iota(jnp.int32, (tile, tokens), 1)
        query = lax.broadcasted_iota(jnp.int32, (tile, tokens), 0) + start
        allowed = (seg_col[rows, :] == seg_row[...]) & (key <= query)
        count = jnp.sum(jnp.where(allowed, 1.0, 0.0), axis=1, keepdims=True) - 1.0
        angle = count * inverse[...]
        trig[0, rows, :] = jnp.cos(angle)
        trig[1, rows, :] = jnp.sin(angle)

    each_tile(tokens, tables)

    for shift in range(1, rows_of):
        stat1.arrive(shift)
        qkv.arrive(shift)

    def heads_in(rows, start, tile):
        first = lax.rsqrt(stat1.total(rows) / width + epsilon)
        fs[rows, :] = first
        first = first[:, :1]
        n1[rows, :] = (x[rows, :].astype(wide) * first * gain1[...]).astype(low)
        value = pq_own[rows, :]
        for shift in range(1, rows_of):
            value = value + pq_r[shift - 1, rows, :].astype(wide)
        value = value * first
        raw[rows, :] = value[:, : qw + kw]
        cosine, sine = trig[0, rows, :], trig[1, rows, :]
        for head in range(heads + key_heads):
            piece = value[:, head * size : (head + 1) * size]
            gain = qn[...] if head < heads else kn[...]
            norm = lax.rsqrt(jnp.mean(piece * piece, axis=1, keepdims=True) + epsilon)
            normed = piece * norm * gain
            rotated = normed * cosine + half_turn(normed) * sine
            lows[rows, head * size : (head + 1) * size] = rotated.astype(low)
        lows[rows, qw + kw :] = value[:, qw + kw :].astype(low)

    each_tile(tokens, heads_in)

    def attend(rows, start, tile):
        key = lax.broadcasted_iota(jnp.int32, (tile, tokens), 1)
        query = lax.broadcasted_iota(jnp.int32, (tile, tokens), 0) + start
        allowed = (seg_col[rows, :] == seg_row[...]) & (key <= query)
        for head in range(heads):
            pair = head // group
            keys = lows[:, qw + pair * size : qw + (pair + 1) * size]
            values = lows[:, qw + kw + pair * size : qw + kw + (pair + 1) * size]
            scores = dot_t(lows[rows, head * size : (head + 1) * size], keys) * scale
            numerators = jnp.where(allowed, jnp.exp(scores), 0.0)
            share = numerators / jnp.sum(numerators, axis=1, keepdims=True)
            shares[head, rows, :] = share
            mixed[0, rows, head * size : (head + 1) * size] = dot(
                share.astype(low), values
            ).astype(low)

    each_tile(tokens, attend)

    gather = row_exchange(2, lambda shift: mixed.at[0], mixed_r)
    for shift in range(1, rows_of):
        gather.start(shift)
    need("wo")
    ox_s[...] = dot(mixed[0], wo[window(me, qw), :])
    for shift in range(1, rows_of):
        gather.arrive(shift)
        mixed[shift] = mixed_r[shift - 1]
        ox_s[...] += dot(mixed_r[shift - 1], wo[window(gather.source(shift), qw), :])
    column = Exchange("col", cols_of, lambda shift: ox_s, ox_r, col_send, col_recv)
    for shift in range(1, cols_of):
        column.start(shift)
    for shift in range(1, cols_of):
        column.arrive(shift)

    stat2 = stat_exchange(1)

    def middle(rows, start, tile):
        value = ox_s[rows, :]
        for shift in range(1, cols_of):
            value = value + ox_r[shift - 1, rows, :]
        value = x[rows, :].astype(wide) + value
        mid[rows, :] = value
        square = jnp.broadcast_to(jnp.sum(value * value, axis=1, keepdims=True), (tile, lanes))
        stat_s[1, rows] = square
        stat_r[1, me, rows] = square
        unit[rows, :] = (value * gain2[...]).astype(low)

    each_tile(tokens, middle)
    for shift in range(1, rows_of):
        stat2.start(shift)

    need("wg", "wu")
    feed = row_exchange(3, lambda shift: pg_s.at[shift - 1], pg_r)
    for shift in range(1, rows_of):
        columns = window(feed.target(shift), fw)
        pg_s[shift - 1, :, :fw] = dot(unit[...], wg[:, columns]).astype(low)
        pg_s[shift - 1, :, fw:] = dot(unit[...], wu[:, columns]).astype(low)
        feed.start(shift)
    pg_own[:, :fw] = dot(unit[...], wg[:, window(me, fw)])
    pg_own[:, fw:] = dot(unit[...], wu[:, window(me, fw)])
    for shift in range(1, rows_of):
        stat2.arrive(shift)
        back.arrive(shift)

    def scale_rows(rows, start, tile):
        second = lax.rsqrt(stat2.total(rows) / width + epsilon)
        ss[rows, :] = second
        n2[rows, :] = (mid[rows, :] * second[:, :1] * gain2[...]).astype(low)

    each_tile(tokens, scale_rows)
    for shift in range(1, rows_of):
        feed.arrive(shift)

    def activate(rows, start, tile):
        second = ss[rows, :1]
        gate = pg_own[rows, :fw]
        upward = pg_own[rows, fw:]
        for shift in range(1, rows_of):
            gate = gate + pg_r[shift - 1, rows, :fw].astype(wide)
            upward = upward + pg_r[shift - 1, rows, fw:].astype(wide)
        gate = gate * second
        upward = upward * second
        behind = ph_own[rows, :]
        for shift in range(1, rows_of):
            behind = behind + ph_r[shift - 1, rows, :].astype(wide)
        sigmoid = jax.nn.sigmoid(gate)
        silu = gate * sigmoid
        hid[rows, :] = (silu * upward).astype(low)
        gub[rows, :fw] = (behind * upward * sigmoid * (1.0 + gate * (1.0 - sigmoid))).astype(low)
        gub[rows, fw:] = (behind * silu).astype(low)

    each_tile(tokens, activate)
    for exchange in (stat1, qkv, back, gather, column, stat2, feed):
        exchange.finish()


def split(rows, columns):
    count = 1
    while rows % count or (rows // count) * columns > chunk_limit:
        count += 1
    return count


class Line:
    def __init__(self, members, out, near, far, spares, sems):
        self.members, self.out, self.near, self.far = members, out, near, far
        self.spares = spares
        self.in_send, self.near_sem, self.far_sem, self.out_send, self.load_sem = sems
        me = lax.axis_index("dp")
        half = members // 2
        left = me < half
        place = jnp.where(left, half - 1 - me, me - half)
        self.inner = jnp.where(left, me + 1, me - 1)
        self.outer = jnp.where(left, jnp.maximum(me - 1, 0), jnp.minimum(me + 1, members - 1))
        self.is_mid = place == 0
        self.not_mid = place > 0
        self.has_outer = place < half - 1
        self.is_end = place == half - 1
        self.chunks, self.done = [], 0

    def view(self, refs, index):
        which, row, rows, column, columns = self.chunks[index]
        if not isinstance(row, int):
            row = pl.multiple_of(row, 16)
        if not isinstance(column, int):
            column = pl.multiple_of(column, lanes)
        return refs[which].at[pl.ds(row, rows), pl.ds(column, columns)]

    def inward(self, index, target, sem):
        return remote(
            self.view(self.out, index),
            self.view(target, index),
            self.in_send.at[index],
            sem.at[index],
            "dp",
            self.inner,
        )

    def outward(self, index):
        return remote(
            self.view(self.out, index),
            self.view(self.far, index),
            self.out_send.at[index],
            self.far_sem.at[index],
            "dp",
            self.outer,
        )

    def send_in(self, index):
        @pl.when(self.is_mid)
        def _():
            self.inward(index, self.far, self.far_sem).start()

        @pl.when(self.not_mid)
        def _():
            self.inward(index, self.near, self.near_sem).start()

    def release(self, which, row, rows, column, columns):
        if self.members == 1:
            return
        count = split(rows, columns)
        for part in range(count):
            size = rows // count
            self.chunks.append((which, row + part * size, size, column, columns))
            index = len(self.chunks) - 1

            @pl.when(self.is_end)
            def _(index=index):
                self.send_in(index)

    def spare(self, index, kind):
        _, _, rows, _, columns = self.chunks[index]
        for ref in self.spares:
            if ref.shape[1:] == (rows, columns):
                return ref.at[kind]
        raise ValueError("no spare")

    def load(self, index, kind):
        source = self.view((self.near, self.far)[kind], index)
        return pltpu.make_async_copy(source, self.spare(index, kind), self.load_sem.at[kind])

    def add(self, index, kind):
        target, other = self.view(self.out, index), self.spare(index, kind)
        rows = other.shape[0]
        tile = 32 if rows % 32 == 0 else rows

        def step(part, carry):
            spot = pl.ds(pl.multiple_of(part * tile, 16), tile)
            target[spot, :] = (target[spot, :].astype(wide) + other[spot, :].astype(wide)).astype(low)
            return carry

        lax.fori_loop(0, rows // tile, step, 0)

    def begin_total(self, index):
        @pl.when(self.is_mid)
        def _():
            self.inward(index, self.far, self.far_sem).wait_recv()
            self.load(index, 1).start()

    def end_total(self, index):
        @pl.when(self.is_mid)
        def _():
            self.load(index, 1).wait()
            self.inward(index, self.far, self.far_sem).wait_send()
            self.add(index, 1)

            @pl.when(self.has_outer)
            def _():
                self.outward(index).start()

    def advance(self, count):
        if self.members == 1:
            return
        for _ in range(count):
            index = self.done
            self.done += 1

            @pl.when(self.has_outer)
            def _():
                self.inward(index, self.near, self.near_sem).wait_recv()
                self.load(index, 0).start()

            if index:
                self.begin_total(index - 1)

            @pl.when(self.has_outer)
            def _():
                self.load(index, 0).wait()
                self.add(index, 0)
                self.send_in(index)

            if index:
                self.end_total(index - 1)

    def settle(self):
        total = len(self.chunks)
        self.advance(total - self.done)
        self.begin_total(total - 1)
        self.end_total(total - 1)

        @pl.when(self.not_mid)
        def _():
            for index in range(total):
                self.inward(index, self.far, self.far_sem).wait_recv()
                self.inward(index, self.near, self.near_sem).wait_send()
                source, target = self.view(self.far, index), self.view(self.out, index)
                copy = pltpu.make_async_copy(source, target, self.load_sem.at[0])
                copy.start()
                copy.wait()

                @pl.when(self.has_outer)
                def _():
                    self.outward(index).start()

        @pl.when(self.has_outer)
        def _():
            for index in range(total):
                self.outward(index).wait_send()


def backward_kernel(
    rows_of,
    cols_of,
    members,
    need,
    x,
    ct,
    n1,
    fs,
    raw,
    lows,
    shares,
    trig,
    mixed,
    mid,
    ss,
    n2,
    hid,
    gub,
    gain1,
    gain2,
    qn,
    kn,
    wq,
    wk,
    wv,
    wo,
    wg,
    wu,
    wd,
    bo,
    ig,
    small,
    gq,
    gk,
    gv,
    go,
    gg,
    gu,
    gd,
    *rest,
):
    near, far, rest = rest[:7], rest[7:14], rest[14:]
    (
        hid_r,
    gub_r,
    n_t,
    mb,
    ml,
    pm_own,
    pm_s,
    pm_r,
    sl,
    sb,
    dqkv,
    dqkv_r,
    gains,
    stat_s,
    stat_r,
    ox_s,
    ox_r,
    row_send,
    row_recv,
    stat_send,
    stat_recv,
        col_send,
        col_recv,
        small_r,
        small_send,
        small_recv,
        in_send,
        near_sem,
        far_sem,
        out_send,
        load_sem,
        *spares,
    ) = rest
    tokens, depth = x.shape
    width = depth * rows_of
    qw, kw, fw = wq.shape[1] // rows_of, wk.shape[1] // rows_of, wg.shape[1] // rows_of
    size = qn.shape[1]
    heads, key_heads = qw // size, kw // size
    group = heads // key_heads
    scale = size ** (-0.5)
    me = lax.axis_index("row")
    greet((("row", rows_of), ("col", cols_of), ("dp", members)))
    line = Line(
        members,
        (gq, gk, gv, go, gg, gu, gd),
        near,
        far,
        spares,
        (in_send, near_sem, far_sem, out_send, load_sem),
    )

    def row_exchange(kind, send, receive):
        return Exchange("row", rows_of, send, receive, row_send.at[kind], row_recv.at[kind])

    def stat_exchange(kind):
        return Ranked(
            "row",
            rows_of,
            lambda shift: stat_s.at[kind],
            stat_r.at[kind],
            stat_send.at[kind],
            stat_recv.at[kind],
        )

    def column_exchange(kind):
        return Exchange(
            "col",
            cols_of,
            lambda shift: ox_s.at[kind],
            ox_r.at[kind],
            col_send.at[kind],
            col_recv.at[kind],
        )

    def column_sum(kind, rows):
        value = ox_s[kind, rows, :]
        for shift in range(1, cols_of):
            value = value + ox_r[kind, shift - 1, rows, :]
        return value

    hide = row_exchange(0, lambda shift: hid, hid_r)
    gates = row_exchange(1, lambda shift: gub, gub_r)
    for shift in range(1, rows_of):
        hide.start(shift)
    for shift in range(1, rows_of):
        gates.start(shift)
    body = pl.ds(0, tokens)
    cut = ct[...]
    for shift in range(rows_of):
        if shift:
            hide.arrive(shift)
        piece = hid[...] if shift == 0 else hid_r[shift - 1]
        index = window(hide.source(shift), fw)
        part = dot(piece, wd[index, :])
        if shift == 0:
            ox_s[0, body, :] = part
        else:
            ox_s[0, body, :] += part
        gd[index, :] = t_dot(piece, cut).astype(low)
        line.release(6, hide.source(shift) * fw, fw, 0, depth)
    column0 = column_exchange(0)
    for shift in range(1, cols_of):
        column0.start(shift)
    n_t[...] = n2[...].T
    need("wg", "wu")
    for shift in range(rows_of):
        line.advance(1)
        if shift:
            gates.arrive(shift)
        piece = gub if shift == 0 else gub_r.at[shift - 1]
        index = window(gates.source(shift), fw)
        part = dot_t(piece[:, :fw], wg[:, index]) + dot_t(piece[:, fw:], wu[:, index])
        if shift == 0:
            ox_s[1, body, :] = part
        else:
            ox_s[1, body, :] += part
        gg[:, index] = dot(n_t[...], piece[:, :fw]).astype(low)
        line.release(4, 0, depth, gates.source(shift) * fw, fw)
        gu[:, index] = dot(n_t[...], piece[:, fw:]).astype(low)
        line.release(5, 0, depth, gates.source(shift) * fw, fw)
    column1 = column_exchange(1)
    for shift in range(1, cols_of):
        column1.start(shift)
    for shift in range(1, cols_of):
        column0.arrive(shift)

    def result(rows, start, tile):
        bo[rows, :] = (mid[rows, :] + column_sum(0, rows)).astype(low)

    each_tile(tokens, result)
    for shift in range(1, cols_of):
        column1.arrive(shift)

    stat2 = stat_exchange(0)
    small[...] = jnp.zeros_like(small)
    gains[...] = jnp.zeros_like(gains)

    def feed_stat(rows, start, tile):
        back = column_sum(1, rows)
        unit = mid[rows, :] * ss[rows, :1]
        small[1:2, :] += jnp.sum(back * unit, axis=0, keepdims=True)
        inner = jnp.sum(back * gain2[...] * unit, axis=1, keepdims=True)
        inner = jnp.broadcast_to(inner, (tile, lanes))
        stat_s[0, rows] = inner
        stat_r[0, me, rows] = inner

    each_tile(tokens, feed_stat)
    pad = pl.ds(tokens, 8)
    stat_s[0, pad] = jnp.zeros((8, lanes), wide)
    for shift in range(1, rows_of):
        stat2.start(shift)
    need("wo", "mixed", "lows", "shares")
    for shift in range(1, rows_of):
        stat2.arrive(shift)

    def middle_back(rows, start, tile):
        second = ss[rows, :1]
        unit = mid[rows, :] * second
        inner = stat2.total(rows)[:, :1] / width
        value = ct[rows, :].astype(wide) + second * (
            column_sum(1, rows) * gain2[...] - unit * inner
        )
        mb[rows, :] = value
        ml[rows, :] = value.astype(low)

    each_tile(tokens, middle_back)
    blend = row_exchange(2, lambda shift: pm_s.at[shift - 1], pm_r)
    for shift in range(1, rows_of):
        pm_s[shift - 1] = dot_t(ml[...], wo[window(blend.target(shift), qw), :]).astype(low)
        blend.start(shift)
    pm_own[...] = dot_t(ml[...], wo[window(me, qw), :])
    for shift in range(rows_of):
        index = window(blend.source(shift), qw)
        go[index, :] = t_dot(mixed[shift], ml[...]).astype(low)
        line.release(3, blend.source(shift) * qw, qw, 0, depth)
    line.advance(2)
    for shift in range(1, rows_of):
        blend.arrive(shift)

    def share_back(rows, start, tile):
        value = pm_own[rows, :]
        for shift in range(1, rows_of):
            value = value + pm_r[shift - 1, rows, :].astype(wide)
        incoming = value.astype(low)
        pm_s[0, rows, :] = incoming
        product = incoming.astype(wide) * mixed[0, rows, :].astype(wide)
        for head in range(heads):
            pair = head // group
            part = slice(head * size, (head + 1) * size)
            values = lows[:, qw + kw + pair * size : qw + kw + (pair + 1) * size]
            delta = jnp.sum(product[:, part], axis=1, keepdims=True)
            share = shares[head, rows, :]
            sl[head, rows, :] = share.astype(low)
            sb[head, rows, :] = (share * (dot_t(incoming[:, part], values) - delta)).astype(low)

    blend.finish()
    each_tile(tokens, share_back)
    need("n1", "raw", "trig")
    n_t[...] = n1[...].T

    def pull(head, back, gain, row):
        raw_piece = raw[:, head * size : (head + 1) * size]
        norm = lax.rsqrt(jnp.mean(raw_piece * raw_piece, axis=1, keepdims=True) + epsilon)
        unit = raw_piece * norm
        normed_back = back * trig[0] - half_turn(back * trig[1])
        gains[row : row + 1, :] += jnp.sum(normed_back * unit, axis=0, keepdims=True)
        unit_back = normed_back * gain
        return norm * (unit_back - unit * jnp.mean(unit_back * unit, axis=1, keepdims=True))

    for pair in range(key_heads):
        keys = lows[:, qw + pair * size : qw + (pair + 1) * size]
        key_back = jnp.zeros((tokens, size), wide)
        value_back = jnp.zeros((tokens, size), wide)
        for head in range(pair * group, (pair + 1) * group):
            part = slice(head * size, (head + 1) * size)
            value_back = value_back + t_dot(sl[head], pm_s[0, :, part])
            key_back = key_back + scale * t_dot(sb[head], lows[:, part])
            query_back = scale * dot(sb[head], keys)
            dqkv[:, part] = pull(head, query_back, qn[...], 0).astype(low)
        spot = qw + pair * size
        dqkv[:, spot : spot + size] = pull(heads + pair, key_back, kn[...], 1).astype(low)
        spot = qw + kw + pair * size
        dqkv[:, spot : spot + size] = value_back.astype(low)

    deliver = row_exchange(3, lambda shift: dqkv, dqkv_r)
    for shift in range(1, rows_of):
        deliver.start(shift)
    need("wq", "wk", "wv")
    line.advance(1)
    for shift in range(rows_of):
        if shift:
            deliver.arrive(shift)
        piece = dqkv if shift == 0 else dqkv_r.at[shift - 1]
        source = deliver.source(shift)
        part = dot_t(piece[:, :qw], wq[:, window(source, qw)])
        part = part + dot_t(piece[:, qw : qw + kw], wk[:, window(source, kw)])
        part = part + dot_t(piece[:, qw + kw :], wv[:, window(source, kw)])
        if shift == 0:
            ox_s[2, body, :] = part
        else:
            ox_s[2, body, :] += part
    ox_s[2, pad, :] = jnp.zeros((8, depth), wide)
    ox_s[2, pad, :lanes] = gains[...]
    column2 = column_exchange(2)
    for shift in range(1, cols_of):
        column2.start(shift)
    for shift in range(rows_of):
        piece = dqkv if shift == 0 else dqkv_r.at[shift - 1]
        source = deliver.source(shift)
        gq[:, window(source, qw)] = dot(n_t[...], piece[:, :qw]).astype(low)
        gk[:, window(source, kw)] = dot(n_t[...], piece[:, qw : qw + kw]).astype(low)
        gv[:, window(source, kw)] = dot(n_t[...], piece[:, qw + kw :]).astype(low)
    line.release(0, 0, depth, 0, qw * rows_of)
    line.release(1, 0, depth, 0, kw * rows_of)
    line.release(2, 0, depth, 0, kw * rows_of)
    for shift in range(1, cols_of):
        column2.arrive(shift)
    need("x", "fs")

    stat1 = stat_exchange(1)

    def first_stat(rows, start, tile):
        back = column_sum(2, rows)
        unit = x[rows, :].astype(wide) * fs[rows, :1]
        small[0:1, :] += jnp.sum(back * unit, axis=0, keepdims=True)
        inner = jnp.sum(back * gain1[...] * unit, axis=1, keepdims=True)
        inner = jnp.broadcast_to(inner, (tile, lanes))
        stat_s[1, rows] = inner
        stat_r[1, me, rows] = inner

    each_tile(tokens, first_stat)
    summed = column_sum(2, pad)[:, :lanes]
    stat_s[1, pad] = summed
    stat_r[1, me, pad] = summed
    for shift in range(1, rows_of):
        stat1.start(shift)
    for shift in range(1, rows_of):
        stat1.arrive(shift)

    def finish(rows, start, tile):
        first = fs[rows, :1]
        unit = x[rows, :].astype(wide) * first
        inner = stat1.total(rows)[:, :1] / width
        ig[rows, :] = mb[rows, :] + first * (column_sum(2, rows) * gain1[...] - unit * inner)

    each_tile(tokens, finish)
    small[8:16, :lanes] = stat1.total(pad)
    ranked = Ranked("dp", members, lambda shift: small, small_r, small_send, small_recv)
    if members > 1:
        small_r[lax.axis_index("dp")] = small[...]
        for shift in range(1, members):
            ranked.start(shift)
        line.settle()
        for shift in range(1, members):
            ranked.arrive(shift)
        ranked.finish()
        summed = small_r[0]
        for member in range(1, members):
            summed = summed + small_r[member]
        small[...] = summed
    for exchange in (hide, gates, column0, column1, stat2, deliver, column2, stat1):
        exchange.finish()


def vmem(shape, kind):
    return pltpu.VMEM(shape, kind)


def call(kernel, shapes, scratch, identity, arguments, late=(), outside=()):
    inside, away = pl.BlockSpec(memory_space=pltpu.VMEM), pl.BlockSpec(memory_space=pl.ANY)
    names = list(arguments)
    late = [name for name in names if name in late]

    def body(*refs):
        given = dict(zip(names, refs))
        rest = refs[len(names) :]
        copies = {}
        if late:
            holders, sem = rest[-len(late) - 1 : -1], rest[-1]
            rest = rest[: -len(late) - 1]
            for index, name in enumerate(late):
                copies[name] = pltpu.make_async_copy(given[name], holders[index], sem.at[index])
                copies[name].start()
                given[name] = holders[index]

        def need(*wanted):
            for name in wanted:
                copy = copies.pop(name, None)
                if copy is not None:
                    copy.wait()

        kernel(need, *given.values(), *rest)
        need(*list(copies))

    extra = []
    if late:
        extra = [vmem(arguments[name].shape, arguments[name].dtype) for name in late]
        extra.append(pltpu.SemaphoreType.DMA((len(late),)))
    return pl.pallas_call(
        body,
        out_shape=tuple(jax.ShapeDtypeStruct(shape, kind) for shape, kind in shapes),
        in_specs=[away if name in late else inside for name in names],
        out_specs=tuple(away if index in outside else inside for index in range(len(shapes))),
        scratch_shapes=scratch + extra,
        compiler_params=pltpu.CompilerParams(
            collective_id=identity, has_side_effects=True, vmem_limit_bytes=full_vmem
        ),
    )(*arguments.values())


def per_device(
    block_input,
    segments,
    attention_norm,
    query_weight,
    key_weight,
    value_weight,
    query_norm,
    key_norm,
    output_weight,
    feedforward_norm,
    gate_weight,
    up_weight,
    down_weight,
    cotangent,
):
    rows_of, cols_of, members = (lax.axis_size(name) for name in ("row", "col", "dp"))
    tokens, depth = block_input.shape
    size = query_norm.shape[0]
    qw, kw, fw = (
        weight.shape[1] // rows_of for weight in (query_weight, key_weight, gate_weight)
    )
    heads = qw // size
    others, beside = max(rows_of - 1, 1), max(cols_of - 1, 1)
    half = size // 2
    inverse = rope_base ** (-2.0 * jnp.arange(half, dtype=wide) / size)
    inverse = jnp.concatenate([inverse, inverse])[None, :]
    seg_row = segments.reshape(1, tokens)
    seg_col = segments.reshape(tokens, 1)
    gain1, gain2 = attention_norm[None, :], feedforward_norm[None, :]
    qn, kn = query_norm[None, :], key_norm[None, :]
    total = qw + 2 * kw
    dma = pltpu.SemaphoreType.DMA

    def sems(kinds):
        return [
            dma((4, others)),
            dma((4, others)),
            dma((2, others)),
            dma((2, others)),
            dma((kinds, beside)) if kinds > 1 else dma((beside,)),
            dma((kinds, beside)) if kinds > 1 else dma((beside,)),
        ]

    saved = call(
        partial(forward_kernel, rows_of, cols_of),
        (
            ((tokens, depth), low),
            ((tokens, lanes), wide),
            ((tokens, qw + kw), wide),
            ((tokens, total), low),
            ((heads, tokens, tokens), wide),
            ((2, tokens, size), wide),
            ((rows_of, tokens, qw), low),
            ((tokens, depth), wide),
            ((tokens, lanes), wide),
            ((tokens, depth), low),
            ((tokens, fw), low),
            ((tokens, 2 * fw), low),
        ),
        [
            vmem((tokens, depth), low),
            vmem((tokens, total), wide),
            vmem((others, tokens, total), low),
            vmem((others, tokens, total), low),
            vmem((tokens, fw), wide),
            vmem((others, tokens, fw), low),
            vmem((others, tokens, fw), low),
            vmem((tokens, 2 * fw), wide),
            vmem((others, tokens, 2 * fw), low),
            vmem((others, tokens, 2 * fw), low),
            vmem((others, tokens, qw), low),
            vmem((2, tokens, lanes), wide),
            vmem((2, rows_of, tokens, lanes), wide),
            vmem((tokens, depth), wide),
            vmem((beside, tokens, depth), wide),
        ]
        + sems(1),
        0,
        dict(
            x=block_input,
            seg_row=seg_row,
            seg_col=seg_col,
            inverse=inverse,
            gain1=gain1,
            wq=query_weight,
            wk=key_weight,
            wv=value_weight,
            qn=qn,
            kn=kn,
            wo=output_weight,
            gain2=gain2,
            wg=gate_weight,
            wu=up_weight,
            wd=down_weight,
            ct=cotangent,
        ),
        late=("wo", "wg", "wu", "wd", "ct"),
    )
    saved = dict(
        zip(("n1", "fs", "raw", "lows", "shares", "trig", "mixed", "mid", "ss", "n2", "hid", "gub"), saved)
    )
    weights = (query_weight, key_weight, value_weight, output_weight, gate_weight, up_weight)
    shapes = [weight.shape for weight in weights] + [down_weight.shape]
    pieces = {
        (fw, depth): rows_of,
        (depth, fw): 2 * rows_of,
        (qw, depth): rows_of,
        (depth, qw * rows_of): 1,
        (depth, kw * rows_of): 2,
    }
    slots = sum(split(*shape) * times for shape, times in pieces.items())
    spares = {(shape[0] // split(*shape), shape[1]) for shape in pieces}
    peers = max(members - 1, 1)
    done = call(
        partial(backward_kernel, rows_of, cols_of, members),
        (
            ((tokens, depth), low),
            ((tokens, depth), wide),
            ((16, depth), wide),
            *((shape, low) for shape in shapes * 3),
        ),
        [
            vmem((others, tokens, fw), low),
            vmem((others, tokens, 2 * fw), low),
            vmem((depth, tokens), low),
            vmem((tokens, depth), wide),
            vmem((tokens, depth), low),
            vmem((tokens, qw), wide),
            vmem((others, tokens, qw), low),
            vmem((others, tokens, qw), low),
            vmem((heads, tokens, tokens), low),
            vmem((heads, tokens, tokens), low),
            vmem((tokens, total), low),
            vmem((others, tokens, total), low),
            vmem((8, lanes), wide),
            vmem((2, tokens + 8, lanes), wide),
            vmem((2, rows_of, tokens + 8, lanes), wide),
            vmem((3, tokens + 8, depth), wide),
            vmem((3, beside, tokens + 8, depth), wide),
        ]
        + sems(3)
        + [vmem((members, 16, depth), wide), dma((peers,)), dma((peers,))]
        + [dma((slots,))] * 4
        + [dma((2,))]
        + [vmem((2, *shape), low) for shape in sorted(spares)],
        1,
        dict(
            x=block_input,
            ct=cotangent,
            **saved,
            gain1=gain1,
            gain2=gain2,
            qn=qn,
            kn=kn,
            wq=query_weight,
            wk=key_weight,
            wv=value_weight,
            wo=output_weight,
            wg=gate_weight,
            wu=up_weight,
            wd=down_weight,
        ),
        late=("x", "n1", "fs", "raw", "lows", "shares", "trig", "mixed", "wq", "wk", "wv", "wo", "wg", "wu"),
        outside=range(10, 24),
    )
    block_output, input_gradient, small, *partials = done[:10]
    gq, gk, gv, go, gg, gu, gd = (partial_sum.astype(wide) for partial_sum in partials)
    return (
        block_output,
        input_gradient,
        small[0],
        gq,
        gk,
        gv,
        small[8, :size],
        small[9, :size],
        go,
        small[1],
        gg,
        gu,
        gd,
    )


def solution(mesh):
    return jax.shard_map(
        per_device,
        mesh=mesh,
        in_specs=(
            P("dp", "row"),
            P("dp", None),
            P("row"),
            P("row", "col"),
            P("row", "col"),
            P("row", "col"),
            P(),
            P(),
            P("col", "row"),
            P("row"),
            P("row", "col"),
            P("row", "col"),
            P("col", "row"),
            P("dp", "row"),
        ),
        out_specs=(
            P("dp", "row"),
            P("dp", "row"),
            P("row"),
            P("row", "col"),
            P("row", "col"),
            P("row", "col"),
            P(),
            P(),
            P("col", "row"),
            P("row"),
            P("row", "col"),
            P("row", "col"),
            P("col", "row"),
        ),
        check_vma=False,
    )
```

```python
from functools import partial

import jax
import jax.numpy as jnp
from jax import lax
from jax.experimental import pallas as pl
from jax.experimental.pallas import tpu as pltpu
from jax.sharding import PartitionSpec as P

epsilon = 1e-06
rope_base = 1000000.0
lanes = 128
full_vmem = 67043328
chunk_limit = 262144
lag = 2
low = jnp.bfloat16
wide = jnp.float32


def dot(a, b, contract=((1,), (0,))):
    return lax.dot_general(a, b, (contract, ((), ())), preferred_element_type=wide)


def dot_t(a, b):
    return dot(a, b, ((1,), (1,)))


def t_dot(a, b):
    return dot(a, b, ((0,), (0,)))


def window(index, size):
    return pl.ds(pl.multiple_of(index * size, lanes), size)


def remote(source, target, send, receive, axis, index):
    return pltpu.make_async_remote_copy(
        src_ref=source,
        dst_ref=target,
        send_sem=send,
        recv_sem=receive,
        device_id={axis: index},
        device_id_type=pl.DeviceIdType.MESH,
    )


def greet(groups):
    barrier = pltpu.get_barrier_semaphore()
    total = 0
    for axis, size in groups:
        me = lax.axis_index(axis)
        for shift in range(1, size):
            pl.semaphore_signal(
                barrier,
                inc=1,
                device_id={axis: lax.rem(me + shift, size)},
                device_id_type=pl.DeviceIdType.MESH,
            )
            total += 1
    if total:
        pl.semaphore_wait(barrier, total)


def half_turn(values):
    size = values.shape[-1]
    turned = pltpu.roll(values, size // 2, axis=1)
    lane = lax.broadcasted_iota(jnp.int32, values.shape, 1)
    return jnp.where(lane < size // 2, -turned, turned)


class Exchange:
    def __init__(self, axis, size, send, receive, send_sem, receive_sem):
        self.axis, self.size = axis, size
        self.send, self.receive = send, receive
        self.send_sem, self.receive_sem = send_sem, receive_sem
        self.me = lax.axis_index(axis)

    def target(self, shift):
        return lax.rem(self.me + shift, self.size)

    def source(self, shift):
        return lax.rem(self.me + self.size - shift, self.size)

    def copy(self, shift):
        sent = self.send(shift)
        return remote(
            sent,
            self.receive.at[shift - 1],
            self.send_sem.at[shift - 1],
            self.receive_sem.at[shift - 1],
            self.axis,
            self.target(shift),
        )

    def start(self, shift):
        self.copy(shift).start()

    def arrive(self, shift):
        self.copy(shift).wait_recv()

    def finish(self):
        for shift in range(1, self.size):
            self.copy(shift).wait_send()


class Ranked(Exchange):
    def copy(self, shift):
        return remote(
            self.send(shift),
            self.receive.at[self.me],
            self.send_sem.at[shift - 1],
            self.receive_sem.at[shift - 1],
            self.axis,
            self.target(shift),
        )

    def total(self, rows):
        result = self.receive[0, rows]
        for member in range(1, self.size):
            result = result + self.receive[member, rows]
        return result


def each_tile(rows, body):
    tile = lanes if rows % lanes == 0 else rows

    def step(index, carry):
        body(pl.ds(pl.multiple_of(index * tile, tile), tile), index * tile, tile)
        return carry

    lax.fori_loop(0, rows // tile, step, 0)


def forward_kernel(
    rows_of,
    cols_of,
    need,
    x,
    seg_row,
    seg_col,
    inverse,
    gain1,
    wq,
    wk,
    wv,
    qn,
    kn,
    wo,
    gain2,
    wg,
    wu,
    n1,
    fs,
    raw,
    lows,
    shares,
    trig,
    mixed,
    mid,
    ss,
    n2,
    hid,
    slope,
    unit,
    pq_own,
    pq_s,
    pq_r,
    pg_own,
    pg_s,
    pg_r,
    mixed_r,
    stat_s,
    stat_r,
    ox_s,
    ox_r,
    row_send,
    row_recv,
    stat_send,
    stat_recv,
    col_send,
    col_recv,
):
    tokens, depth = x.shape
    width = depth * rows_of
    qw, kw, fw = wq.shape[1] // rows_of, wk.shape[1] // rows_of, wg.shape[1] // rows_of
    size = qn.shape[1]
    heads, key_heads = qw // size, kw // size
    group = heads // key_heads
    scale = size ** (-0.5)
    me = lax.axis_index("row")
    greet((("row", rows_of), ("col", cols_of)))

    def row_exchange(kind, send, receive):
        return Exchange("row", rows_of, send, receive, row_send.at[kind], row_recv.at[kind])

    def stat_exchange(kind):
        return Ranked(
            "row",
            rows_of,
            lambda shift: stat_s.at[kind],
            stat_r.at[kind],
            stat_send.at[kind],
            stat_recv.at[kind],
        )

    stat1 = stat_exchange(0)

    def prepare(rows, start, tile):
        value = x[rows, :].astype(wide)
        square = jnp.broadcast_to(jnp.sum(value * value, axis=1, keepdims=True), (tile, lanes))
        stat_s[0, rows] = square
        stat_r[0, me, rows] = square
        unit[rows, :] = (value * gain1[...]).astype(low)

    each_tile(tokens, prepare)
    for shift in range(1, rows_of):
        stat1.start(shift)

    def project(index, target, slot):
        u = unit[...]
        q = dot(u, wq[:, window(index, qw)])
        k = dot(u, wk[:, window(index, kw)])
        v = dot(u, wv[:, window(index, kw)])
        kind = target.dtype
        if slot is None:
            target[:, :qw] = q.astype(kind)
            target[:, qw : qw + kw] = k.astype(kind)
            target[:, qw + kw :] = v.astype(kind)
        else:
            target[slot, :, :qw] = q.astype(kind)
            target[slot, :, qw : qw + kw] = k.astype(kind)
            target[slot, :, qw + kw :] = v.astype(kind)

    qkv = row_exchange(0, lambda shift: pq_s.at[shift - 1], pq_r)
    for shift in range(1, rows_of):
        project(qkv.target(shift), pq_s, shift - 1)
        qkv.start(shift)
    project(me, pq_own, None)

    def tables(rows, start, tile):
        key = lax.broadcasted_iota(jnp.int32, (tile, tokens), 1)
        query = lax.broadcasted_iota(jnp.int32, (tile, tokens), 0) + start
        allowed = (seg_col[rows, :] == seg_row[...]) & (key <= query)
        count = jnp.sum(jnp.where(allowed, 1.0, 0.0), axis=1, keepdims=True) - 1.0
        angle = count * inverse[...]
        trig[0, rows, :] = jnp.cos(angle)
        trig[1, rows, :] = jnp.sin(angle)

    each_tile(tokens, tables)

    for shift in range(1, rows_of):
        stat1.arrive(shift)
        qkv.arrive(shift)

    def heads_in(rows, start, tile):
        first = lax.rsqrt(stat1.total(rows) / width + epsilon)
        fs[rows, :] = first
        first = first[:, :1]
        n1[rows, :] = (x[rows, :].astype(wide) * first * gain1[...]).astype(low)
        value = pq_own[rows, :]
        for shift in range(1, rows_of):
            value = value + pq_r[shift - 1, rows, :].astype(wide)
        value = value * first
        raw[rows, :] = value[:, : qw + kw]
        cosine, sine = trig[0, rows, :], trig[1, rows, :]
        for head in range(heads + key_heads):
            piece = value[:, head * size : (head + 1) * size]
            gain = qn[...] if head < heads else kn[...]
            norm = lax.rsqrt(jnp.mean(piece * piece, axis=1, keepdims=True) + epsilon)
            normed = piece * norm * gain
            rotated = normed * cosine + half_turn(normed) * sine
            lows[rows, head * size : (head + 1) * size] = rotated.astype(low)
        lows[rows, qw + kw :] = value[:, qw + kw :].astype(low)

    each_tile(tokens, heads_in)

    def attend(rows, start, tile):
        key = lax.broadcasted_iota(jnp.int32, (tile, tokens), 1)
        query = lax.broadcasted_iota(jnp.int32, (tile, tokens), 0) + start
        allowed = (seg_col[rows, :] == seg_row[...]) & (key <= query)
        for head in range(heads):
            pair = head // group
            keys = lows[:, qw + pair * size : qw + (pair + 1) * size]
            values = lows[:, qw + kw + pair * size : qw + kw + (pair + 1) * size]
            scores = dot_t(lows[rows, head * size : (head + 1) * size], keys) * scale
            numerators = jnp.where(allowed, jnp.exp(scores), 0.0)
            share = numerators / jnp.sum(numerators, axis=1, keepdims=True)
            shares[head, rows, :] = share
            mixed[0, rows, head * size : (head + 1) * size] = dot(
                share.astype(low), values
            ).astype(low)

    each_tile(tokens, attend)

    gather = row_exchange(2, lambda shift: mixed.at[0], mixed_r)
    for shift in range(1, rows_of):
        gather.start(shift)
    need("wo")
    ox_s[...] = dot(mixed[0], wo[window(me, qw), :])
    for shift in range(1, rows_of):
        gather.arrive(shift)
        mixed[shift] = mixed_r[shift - 1]
        ox_s[...] += dot(mixed_r[shift - 1], wo[window(gather.source(shift), qw), :])
    column = Exchange("col", cols_of, lambda shift: ox_s, ox_r, col_send, col_recv)
    for shift in range(1, cols_of):
        column.start(shift)
    for shift in range(1, cols_of):
        column.arrive(shift)

    stat2 = stat_exchange(1)

    def middle(rows, start, tile):
        value = ox_s[rows, :]
        for shift in range(1, cols_of):
            value = value + ox_r[shift - 1, rows, :]
        value = x[rows, :].astype(wide) + value
        mid[rows, :] = value
        square = jnp.broadcast_to(jnp.sum(value * value, axis=1, keepdims=True), (tile, lanes))
        stat_s[1, rows] = square
        stat_r[1, me, rows] = square
        unit[rows, :] = (value * gain2[...]).astype(low)

    each_tile(tokens, middle)
    for shift in range(1, rows_of):
        stat2.start(shift)

    need("wg", "wu")
    feed = row_exchange(3, lambda shift: pg_s.at[shift - 1], pg_r)
    for shift in range(1, rows_of):
        columns = window(feed.target(shift), fw)
        pg_s[shift - 1, :, :fw] = dot(unit[...], wg[:, columns]).astype(low)
        pg_s[shift - 1, :, fw:] = dot(unit[...], wu[:, columns]).astype(low)
        feed.start(shift)
    pg_own[:, :fw] = dot(unit[...], wg[:, window(me, fw)])
    pg_own[:, fw:] = dot(unit[...], wu[:, window(me, fw)])
    for shift in range(1, rows_of):
        stat2.arrive(shift)

    def scale_rows(rows, start, tile):
        second = lax.rsqrt(stat2.total(rows) / width + epsilon)
        ss[rows, :] = second
        n2[rows, :] = (mid[rows, :] * second[:, :1] * gain2[...]).astype(low)

    each_tile(tokens, scale_rows)
    for shift in range(1, rows_of):
        feed.arrive(shift)

    def activate(rows, start, tile):
        second = ss[rows, :1]
        gate = pg_own[rows, :fw]
        upward = pg_own[rows, fw:]
        for shift in range(1, rows_of):
            gate = gate + pg_r[shift - 1, rows, :fw].astype(wide)
            upward = upward + pg_r[shift - 1, rows, fw:].astype(wide)
        gate = gate * second
        upward = upward * second
        sigmoid = jax.nn.sigmoid(gate)
        silu = gate * sigmoid
        hid[rows, :] = (silu * upward).astype(low)
        slope[rows, :fw] = upward * sigmoid * (1.0 + gate * (1.0 - sigmoid))
        slope[rows, fw:] = silu

    each_tile(tokens, activate)
    for exchange in (stat1, qkv, gather, column, stat2, feed):
        exchange.finish()


def split(rows, columns):
    count = 1
    while rows % count or (rows // count) * columns > chunk_limit:
        count += 1
    return count


class Line:
    def __init__(self, members, out, near, far, spares, sems):
        self.members, self.out, self.near, self.far = members, out, near, far
        self.spares = spares
        self.in_send, self.near_sem, self.far_sem, self.out_send, self.store_sem, self.load_sem = sems
        me = lax.axis_index("dp")
        half = members // 2
        left = me < half
        place = jnp.where(left, half - 1 - me, me - half)
        self.inner = jnp.where(left, me + 1, me - 1)
        self.outer = jnp.where(left, jnp.maximum(me - 1, 0), jnp.minimum(me + 1, members - 1))
        self.is_mid = place == 0
        self.not_mid = place > 0
        self.has_outer = place < half - 1
        self.is_end = place == half - 1
        self.chunks, self.done = [], 0

    def view(self, refs, index):
        which, row, rows, column, columns = self.chunks[index]
        if not isinstance(row, int):
            row = pl.multiple_of(row, 16)
        if not isinstance(column, int):
            column = pl.multiple_of(column, lanes)
        return refs[which].at[pl.ds(row, rows), pl.ds(column, columns)]

    def inward(self, index, target, sem):
        return remote(
            self.view(self.out, index),
            self.view(target, index),
            self.in_send.at[index],
            sem.at[index],
            "dp",
            self.inner,
        )

    def outward(self, index):
        return remote(
            self.view(self.out, index),
            self.view(self.far, index),
            self.out_send.at[index],
            self.far_sem.at[index],
            "dp",
            self.outer,
        )

    def relay(self, index):
        return remote(
            self.view(self.far, index),
            self.view(self.far, index),
            self.out_send.at[index],
            self.far_sem.at[index],
            "dp",
            self.outer,
        )

    def send_in(self, index):
        @pl.when(self.is_mid)
        def _():
            self.inward(index, self.far, self.far_sem).start()

        @pl.when(self.not_mid)
        def _():
            self.inward(index, self.near, self.near_sem).start()

    def release(self, which, row, rows, column, columns):
        if self.members == 1:
            return
        count = split(rows, columns)
        for part in range(count):
            size = rows // count
            self.chunks.append((which, row + part * size, size, column, columns))
            index = len(self.chunks) - 1

            @pl.when(self.is_end)
            def _(index=index):
                self.send_in(index)

    def spare(self, index, kind):
        _, _, rows, _, columns = self.chunks[index]
        for ref in self.spares:
            if ref.shape[1:] == (rows, columns):
                return ref.at[kind]
        raise ValueError("no spare")

    def load(self, index, kind):
        source = self.view((self.near, self.far)[kind], index)
        return pltpu.make_async_copy(source, self.spare(index, kind), self.load_sem.at[kind])

    def add(self, index, kind):
        target, other = self.view(self.out, index), self.spare(index, kind)
        rows = other.shape[0]
        tile = 32 if rows % 32 == 0 else rows

        def step(part, carry):
            spot = pl.ds(pl.multiple_of(part * tile, 16), tile)
            target[spot, :] = (target[spot, :].astype(wide) + other[spot, :].astype(wide)).astype(low)
            return carry

        lax.fori_loop(0, rows // tile, step, 0)

    def begin_total(self, index):
        @pl.when(self.is_mid)
        def _():
            self.inward(index, self.far, self.far_sem).wait_recv()
            self.load(index, 1).start()

    def store(self, index):
        return pltpu.make_async_copy(
            self.view(self.out, index), self.view(self.far, index), self.store_sem.at[index]
        )

    def end_total(self, index):
        @pl.when(self.is_mid)
        def _():
            self.load(index, 1).wait()
            self.inward(index, self.far, self.far_sem).wait_send()
            self.add(index, 1)

            @pl.when(self.has_outer)
            def _():
                self.outward(index).start()

            self.store(index).start()

    def advance(self, count):
        if self.members == 1:
            return
        for _ in range(count):
            index = self.done
            self.done += 1

            @pl.when(self.has_outer)
            def _():
                self.inward(index, self.near, self.near_sem).wait_recv()
                self.load(index, 0).start()

            if index >= lag:
                self.begin_total(index - lag)

            @pl.when(self.has_outer)
            def _():
                self.load(index, 0).wait()
                self.add(index, 0)
                self.send_in(index)

            if index >= lag:
                self.end_total(index - lag)

    def settle(self):
        total = len(self.chunks)
        self.advance(total - self.done)
        for index in range(max(total - lag, 0), total):
            self.begin_total(index)
            self.end_total(index)

        @pl.when(self.not_mid)
        def _():
            for index in range(total):
                self.inward(index, self.far, self.far_sem).wait_recv()

                @pl.when(self.has_outer)
                def _():
                    self.relay(index).start()

            for index in range(total):
                self.inward(index, self.near, self.near_sem).wait_send()

                @pl.when(self.has_outer)
                def _():
                    self.relay(index).wait_send()

        @pl.when(self.is_mid)
        def _():
            for index in range(total):
                self.store(index).wait()

                @pl.when(self.has_outer)
                def _():
                    self.outward(index).wait_send()


def backward_kernel(
    rows_of,
    cols_of,
    members,
    need,
    x,
    ct,
    n1,
    fs,
    raw,
    lows,
    shares,
    trig,
    mixed,
    mid,
    ss,
    n2,
    hid,
    slope,
    gain1,
    gain2,
    qn,
    kn,
    wq,
    wk,
    wv,
    wo,
    wg,
    wu,
    wd,
    bo,
    ig,
    small,
    *rest,
):
    far, near, rest = rest[:7], rest[7:14], rest[14:]
    grads, rest = rest[:7], rest[7:]
    gq, gk, gv, go, gg, gu, gd = grads
    (
        gub,
        ph_s,
        ph_r,
        hid_r,
    gub_r,
    n_t,
    mb,
    ml,
    pm_own,
    pm_s,
    pm_r,
    sl,
    sb,
    dqkv,
    dqkv_r,
    gains,
    stat_s,
    stat_r,
    ox_s,
    ox_r,
    row_send,
    row_recv,
    stat_send,
    stat_recv,
        col_send,
        col_recv,
        small_r,
        small_send,
        small_recv,
        in_send,
        near_sem,
        far_sem,
        out_send,
        store_sem,
        load_sem,
        *spares,
    ) = rest
    tokens, depth = x.shape
    width = depth * rows_of
    qw, kw, fw = wq.shape[1] // rows_of, wk.shape[1] // rows_of, wg.shape[1] // rows_of
    size = qn.shape[1]
    heads, key_heads = qw // size, kw // size
    group = heads // key_heads
    scale = size ** (-0.5)
    me = lax.axis_index("row")
    greet((("row", rows_of), ("col", cols_of), ("dp", members)))
    line = Line(
        members,
        grads,
        near,
        far,
        spares,
        (in_send, near_sem, far_sem, out_send, store_sem, load_sem),
    )

    def row_exchange(kind, send, receive):
        return Exchange("row", rows_of, send, receive, row_send.at[kind], row_recv.at[kind])

    def stat_exchange(kind):
        return Ranked(
            "row",
            rows_of,
            lambda shift: stat_s.at[kind],
            stat_r.at[kind],
            stat_send.at[kind],
            stat_recv.at[kind],
        )

    def column_exchange(kind):
        return Exchange(
            "col",
            cols_of,
            lambda shift: ox_s.at[kind],
            ox_r.at[kind],
            col_send.at[kind],
            col_recv.at[kind],
        )

    def column_sum(kind, rows):
        value = ox_s[kind, rows, :]
        for shift in range(1, cols_of):
            value = value + ox_r[kind, shift - 1, rows, :]
        return value

    hide = row_exchange(0, lambda shift: hid, hid_r)
    gates = row_exchange(1, lambda shift: gub, gub_r)
    for shift in range(1, rows_of):
        hide.start(shift)
    body = pl.ds(0, tokens)
    cut = ct[...]
    back = row_exchange(4, lambda shift: ph_s.at[shift - 1], ph_r)
    for shift in range(rows_of):
        if shift:
            hide.arrive(shift)
        piece = hid[...] if shift == 0 else hid_r[shift - 1]
        index = window(hide.source(shift), fw)
        part = dot(piece, wd[index, :])
        if shift == 0:
            ox_s[0, body, :] = part
        else:
            ox_s[0, body, :] += part
        gd[index, :] = t_dot(piece, cut).astype(low)
        line.release(6, hide.source(shift) * fw, fw, 0, depth)
        if shift == 0:
            for other in range(1, rows_of):
                ph_s[other - 1] = dot_t(cut, wd[window(back.target(other), fw), :]).astype(low)
                back.start(other)
        else:
            line.advance(1)
    column0 = column_exchange(0)
    for shift in range(1, cols_of):
        column0.start(shift)
    n_t[...] = n2[...].T
    need("slope")
    line.advance(2)
    for shift in range(1, rows_of):
        back.arrive(shift)

    def behind(rows, start, tile):
        value = dot_t(ct[rows, :], wd[window(me, fw), :])
        for shift in range(1, rows_of):
            value = value + ph_r[shift - 1, rows, :].astype(wide)
        gub[rows, :fw] = (value * slope[rows, :fw]).astype(low)
        gub[rows, fw:] = (value * slope[rows, fw:]).astype(low)

    each_tile(tokens, behind)
    for shift in range(1, rows_of):
        gates.start(shift)
    need("wg", "wu")
    for shift in range(rows_of):
        if shift:
            line.advance(2)
            gates.arrive(shift)
        piece = gub if shift == 0 else gub_r.at[shift - 1]
        index = window(gates.source(shift), fw)
        part = dot_t(piece[:, :fw], wg[:, index]) + dot_t(piece[:, fw:], wu[:, index])
        if shift == 0:
            ox_s[1, body, :] = part
        else:
            ox_s[1, body, :] += part
        gg[:, index] = dot(n_t[...], piece[:, :fw]).astype(low)
        line.release(4, 0, depth, gates.source(shift) * fw, fw)
        gu[:, index] = dot(n_t[...], piece[:, fw:]).astype(low)
        line.release(5, 0, depth, gates.source(shift) * fw, fw)
    column1 = column_exchange(1)
    for shift in range(1, cols_of):
        column1.start(shift)
    line.advance(1)
    for shift in range(1, cols_of):
        column0.arrive(shift)

    def result(rows, start, tile):
        bo[rows, :] = (mid[rows, :] + column_sum(0, rows)).astype(low)

    each_tile(tokens, result)
    for shift in range(1, cols_of):
        column1.arrive(shift)

    stat2 = stat_exchange(0)
    small[...] = jnp.zeros_like(small)
    gains[...] = jnp.zeros_like(gains)

    def feed_stat(rows, start, tile):
        back = column_sum(1, rows)
        unit = mid[rows, :] * ss[rows, :1]
        small[1:2, :] += jnp.sum(back * unit, axis=0, keepdims=True)
        inner = jnp.sum(back * gain2[...] * unit, axis=1, keepdims=True)
        inner = jnp.broadcast_to(inner, (tile, lanes))
        stat_s[0, rows] = inner
        stat_r[0, me, rows] = inner

    each_tile(tokens, feed_stat)
    pad = pl.ds(tokens, 8)
    stat_s[0, pad] = jnp.zeros((8, lanes), wide)
    for shift in range(1, rows_of):
        stat2.start(shift)
    need("wo", "mixed", "lows", "shares")
    line.advance(1)
    for shift in range(1, rows_of):
        stat2.arrive(shift)

    def middle_back(rows, start, tile):
        second = ss[rows, :1]
        unit = mid[rows, :] * second
        inner = stat2.total(rows)[:, :1] / width
        value = ct[rows, :].astype(wide) + second * (
            column_sum(1, rows) * gain2[...] - unit * inner
        )
        mb[rows, :] = value
        ml[rows, :] = value.astype(low)

    each_tile(tokens, middle_back)
    blend = row_exchange(2, lambda shift: pm_s.at[shift - 1], pm_r)
    for shift in range(1, rows_of):
        pm_s[shift - 1] = dot_t(ml[...], wo[window(blend.target(shift), qw), :]).astype(low)
        blend.start(shift)
    pm_own[...] = dot_t(ml[...], wo[window(me, qw), :])
    for shift in range(rows_of):
        index = window(blend.source(shift), qw)
        go[index, :] = t_dot(mixed[shift], ml[...]).astype(low)
        line.release(3, blend.source(shift) * qw, qw, 0, depth)
    line.advance(2)
    for shift in range(1, rows_of):
        blend.arrive(shift)

    def share_back(rows, start, tile):
        value = pm_own[rows, :]
        for shift in range(1, rows_of):
            value = value + pm_r[shift - 1, rows, :].astype(wide)
        incoming = value.astype(low)
        pm_s[0, rows, :] = incoming
        product = incoming.astype(wide) * mixed[0, rows, :].astype(wide)
        for head in range(heads):
            pair = head // group
            part = slice(head * size, (head + 1) * size)
            values = lows[:, qw + kw + pair * size : qw + kw + (pair + 1) * size]
            delta = jnp.sum(product[:, part], axis=1, keepdims=True)
            share = shares[head, rows, :]
            sl[head, rows, :] = share.astype(low)
            sb[head, rows, :] = (share * (dot_t(incoming[:, part], values) - delta)).astype(low)

    blend.finish()
    each_tile(tokens, share_back)
    need("n1", "raw", "trig")
    n_t[...] = n1[...].T
    line.advance(1)

    def pull(head, back, gain, row):
        raw_piece = raw[:, head * size : (head + 1) * size]
        norm = lax.rsqrt(jnp.mean(raw_piece * raw_piece, axis=1, keepdims=True) + epsilon)
        unit = raw_piece * norm
        normed_back = back * trig[0] - half_turn(back * trig[1])
        gains[row : row + 1, :] += jnp.sum(normed_back * unit, axis=0, keepdims=True)
        unit_back = normed_back * gain
        return norm * (unit_back - unit * jnp.mean(unit_back * unit, axis=1, keepdims=True))

    for pair in range(key_heads):
        keys = lows[:, qw + pair * size : qw + (pair + 1) * size]
        key_back = jnp.zeros((tokens, size), wide)
        value_back = jnp.zeros((tokens, size), wide)
        for head in range(pair * group, (pair + 1) * group):
            part = slice(head * size, (head + 1) * size)
            value_back = value_back + t_dot(sl[head], pm_s[0, :, part])
            key_back = key_back + scale * t_dot(sb[head], lows[:, part])
            query_back = scale * dot(sb[head], keys)
            dqkv[:, part] = pull(head, query_back, qn[...], 0).astype(low)
        spot = qw + pair * size
        dqkv[:, spot : spot + size] = pull(heads + pair, key_back, kn[...], 1).astype(low)
        spot = qw + kw + pair * size
        dqkv[:, spot : spot + size] = value_back.astype(low)

    deliver = row_exchange(3, lambda shift: dqkv, dqkv_r)
    for shift in range(1, rows_of):
        deliver.start(shift)
    need("wq", "wk", "wv")
    for shift in range(rows_of):
        if shift:
            line.advance(1)
            deliver.arrive(shift)
        piece = dqkv if shift == 0 else dqkv_r.at[shift - 1]
        source = deliver.source(shift)
        part = dot_t(piece[:, :qw], wq[:, window(source, qw)])
        part = part + dot_t(piece[:, qw : qw + kw], wk[:, window(source, kw)])
        part = part + dot_t(piece[:, qw + kw :], wv[:, window(source, kw)])
        if shift == 0:
            ox_s[2, body, :] = part
        else:
            ox_s[2, body, :] += part
    ox_s[2, pad, :] = jnp.zeros((8, depth), wide)
    ox_s[2, pad, :lanes] = gains[...]
    column2 = column_exchange(2)
    for shift in range(1, cols_of):
        column2.start(shift)
    for shift in range(rows_of):
        piece = dqkv if shift == 0 else dqkv_r.at[shift - 1]
        source = deliver.source(shift)
        gq[:, window(source, qw)] = dot(n_t[...], piece[:, :qw]).astype(low)
        gk[:, window(source, kw)] = dot(n_t[...], piece[:, qw : qw + kw]).astype(low)
        gv[:, window(source, kw)] = dot(n_t[...], piece[:, qw + kw :]).astype(low)
    line.release(0, 0, depth, 0, qw * rows_of)
    line.release(1, 0, depth, 0, kw * rows_of)
    line.release(2, 0, depth, 0, kw * rows_of)
    line.advance(1)
    for shift in range(1, cols_of):
        column2.arrive(shift)
    need("x", "fs")

    stat1 = stat_exchange(1)

    def first_stat(rows, start, tile):
        back = column_sum(2, rows)
        unit = x[rows, :].astype(wide) * fs[rows, :1]
        small[0:1, :] += jnp.sum(back * unit, axis=0, keepdims=True)
        inner = jnp.sum(back * gain1[...] * unit, axis=1, keepdims=True)
        inner = jnp.broadcast_to(inner, (tile, lanes))
        stat_s[1, rows] = inner
        stat_r[1, me, rows] = inner

    each_tile(tokens, first_stat)
    summed = column_sum(2, pad)[:, :lanes]
    stat_s[1, pad] = summed
    stat_r[1, me, pad] = summed
    for shift in range(1, rows_of):
        stat1.start(shift)
    line.advance(1)
    for shift in range(1, rows_of):
        stat1.arrive(shift)

    def finish(rows, start, tile):
        first = fs[rows, :1]
        unit = x[rows, :].astype(wide) * first
        inner = stat1.total(rows)[:, :1] / width
        ig[rows, :] = mb[rows, :] + first * (column_sum(2, rows) * gain1[...] - unit * inner)

    each_tile(tokens, finish)
    small[8:16, :lanes] = stat1.total(pad)
    ranked = Ranked("dp", members, lambda shift: small, small_r, small_send, small_recv)
    if members > 1:
        small_r[lax.axis_index("dp")] = small[...]
        for shift in range(1, members):
            ranked.start(shift)
        line.settle()
        for shift in range(1, members):
            ranked.arrive(shift)
        ranked.finish()
        summed = small_r[0]
        for member in range(1, members):
            summed = summed + small_r[member]
        small[...] = summed
    for exchange in (hide, back, gates, column0, column1, stat2, deliver, column2, stat1):
        exchange.finish()


def vmem(shape, kind):
    return pltpu.VMEM(shape, kind)


def call(kernel, shapes, scratch, identity, arguments, late=(), outside=()):
    inside, away = pl.BlockSpec(memory_space=pltpu.VMEM), pl.BlockSpec(memory_space=pl.ANY)
    names = list(arguments)
    late = [name for name in names if name in late]

    def body(*refs):
        given = dict(zip(names, refs))
        rest = refs[len(names) :]
        copies = {}
        if late:
            holders, sem = rest[-len(late) - 1 : -1], rest[-1]
            rest = rest[: -len(late) - 1]
            for index, name in enumerate(late):
                copies[name] = pltpu.make_async_copy(given[name], holders[index], sem.at[index])
                copies[name].start()
                given[name] = holders[index]

        def need(*wanted):
            for name in wanted:
                copy = copies.pop(name, None)
                if copy is not None:
                    copy.wait()

        kernel(need, *given.values(), *rest)
        need(*list(copies))

    extra = []
    if late:
        extra = [vmem(arguments[name].shape, arguments[name].dtype) for name in late]
        extra.append(pltpu.SemaphoreType.DMA((len(late),)))
    return pl.pallas_call(
        body,
        out_shape=tuple(jax.ShapeDtypeStruct(shape, kind) for shape, kind in shapes),
        in_specs=[away if name in late else inside for name in names],
        out_specs=tuple(away if index in outside else inside for index in range(len(shapes))),
        scratch_shapes=scratch + extra,
        compiler_params=pltpu.CompilerParams(
            collective_id=identity, has_side_effects=True, vmem_limit_bytes=full_vmem
        ),
    )(*arguments.values())


def per_device(
    block_input,
    segments,
    attention_norm,
    query_weight,
    key_weight,
    value_weight,
    query_norm,
    key_norm,
    output_weight,
    feedforward_norm,
    gate_weight,
    up_weight,
    down_weight,
    cotangent,
):
    rows_of, cols_of, members = (lax.axis_size(name) for name in ("row", "col", "dp"))
    tokens, depth = block_input.shape
    size = query_norm.shape[0]
    qw, kw, fw = (
        weight.shape[1] // rows_of for weight in (query_weight, key_weight, gate_weight)
    )
    heads = qw // size
    others, beside = max(rows_of - 1, 1), max(cols_of - 1, 1)
    half = size // 2
    inverse = rope_base ** (-2.0 * jnp.arange(half, dtype=wide) / size)
    inverse = jnp.concatenate([inverse, inverse])[None, :]
    seg_row = segments.reshape(1, tokens)
    seg_col = segments.reshape(tokens, 1)
    gain1, gain2 = attention_norm[None, :], feedforward_norm[None, :]
    qn, kn = query_norm[None, :], key_norm[None, :]
    total = qw + 2 * kw
    dma = pltpu.SemaphoreType.DMA

    def sems(kinds):
        return [
            dma((5, others)),
            dma((5, others)),
            dma((2, others)),
            dma((2, others)),
            dma((kinds, beside)) if kinds > 1 else dma((beside,)),
            dma((kinds, beside)) if kinds > 1 else dma((beside,)),
        ]

    saved = call(
        partial(forward_kernel, rows_of, cols_of),
        (
            ((tokens, depth), low),
            ((tokens, lanes), wide),
            ((tokens, qw + kw), wide),
            ((tokens, total), low),
            ((heads, tokens, tokens), wide),
            ((2, tokens, size), wide),
            ((rows_of, tokens, qw), low),
            ((tokens, depth), wide),
            ((tokens, lanes), wide),
            ((tokens, depth), low),
            ((tokens, fw), low),
            ((tokens, 2 * fw), wide),
        ),
        [
            vmem((tokens, depth), low),
            vmem((tokens, total), wide),
            vmem((others, tokens, total), low),
            vmem((others, tokens, total), low),
            vmem((tokens, 2 * fw), wide),
            vmem((others, tokens, 2 * fw), low),
            vmem((others, tokens, 2 * fw), low),
            vmem((others, tokens, qw), low),
            vmem((2, tokens, lanes), wide),
            vmem((2, rows_of, tokens, lanes), wide),
            vmem((tokens, depth), wide),
            vmem((beside, tokens, depth), wide),
        ]
        + sems(1),
        0,
        dict(
            x=block_input,
            seg_row=seg_row,
            seg_col=seg_col,
            inverse=inverse,
            gain1=gain1,
            wq=query_weight,
            wk=key_weight,
            wv=value_weight,
            qn=qn,
            kn=kn,
            wo=output_weight,
            gain2=gain2,
            wg=gate_weight,
            wu=up_weight,
        ),
        late=("wo", "wg", "wu"),
    )
    saved = dict(
        zip(("n1", "fs", "raw", "lows", "shares", "trig", "mixed", "mid", "ss", "n2", "hid", "slope"), saved)
    )
    weights = (query_weight, key_weight, value_weight, output_weight, gate_weight, up_weight)
    shapes = [weight.shape for weight in weights] + [down_weight.shape]
    pieces = {
        (fw, depth): rows_of,
        (depth, fw): 2 * rows_of,
        (qw, depth): rows_of,
        (depth, qw * rows_of): 1,
        (depth, kw * rows_of): 2,
    }
    slots = sum(split(*shape) * times for shape, times in pieces.items())
    spares = {(shape[0] // split(*shape), shape[1]) for shape in pieces}
    peers = max(members - 1, 1)
    done = call(
        partial(backward_kernel, rows_of, cols_of, members),
        (
            ((tokens, depth), low),
            ((tokens, depth), wide),
            ((16, depth), wide),
            *((shape, low) for shape in shapes * 2),
        ),
        [vmem(shape, low) for shape in shapes]
        + [
            vmem((tokens, 2 * fw), low),
            vmem((others, tokens, fw), low),
            vmem((others, tokens, fw), low),
            vmem((others, tokens, fw), low),
            vmem((others, tokens, 2 * fw), low),
            vmem((depth, tokens), low),
            vmem((tokens, depth), wide),
            vmem((tokens, depth), low),
            vmem((tokens, qw), wide),
            vmem((others, tokens, qw), low),
            vmem((others, tokens, qw), low),
            vmem((heads, tokens, tokens), low),
            vmem((heads, tokens, tokens), low),
            vmem((tokens, total), low),
            vmem((others, tokens, total), low),
            vmem((8, lanes), wide),
            vmem((2, tokens + 8, lanes), wide),
            vmem((2, rows_of, tokens + 8, lanes), wide),
            vmem((3, tokens + 8, depth), wide),
            vmem((3, beside, tokens + 8, depth), wide),
        ]
        + sems(3)
        + [vmem((members, 16, depth), wide), dma((peers,)), dma((peers,))]
        + [dma((slots,))] * 5
        + [dma((2,))]
        + [vmem((2, *shape), low) for shape in sorted(spares)],
        1,
        dict(
            x=block_input,
            ct=cotangent,
            **saved,
            gain1=gain1,
            gain2=gain2,
            qn=qn,
            kn=kn,
            wq=query_weight,
            wk=key_weight,
            wv=value_weight,
            wo=output_weight,
            wg=gate_weight,
            wu=up_weight,
            wd=down_weight,
        ),
        late=("x", "n1", "fs", "raw", "lows", "shares", "trig", "mixed", "slope", "wq", "wk", "wv", "wo", "wg", "wu"),
        outside=range(3, 17),
    )
    block_output, input_gradient, small, *partials = done[:10]
    gq, gk, gv, go, gg, gu, gd = (partial_sum.astype(wide) for partial_sum in partials)
    return (
        block_output,
        input_gradient,
        small[0],
        gq,
        gk,
        gv,
        small[8, :size],
        small[9, :size],
        go,
        small[1],
        gg,
        gu,
        gd,
    )


def solution(mesh):
    return jax.shard_map(
        per_device,
        mesh=mesh,
        in_specs=(
            P("dp", "row"),
            P("dp", None),
            P("row"),
            P("row", "col"),
            P("row", "col"),
            P("row", "col"),
            P(),
            P(),
            P("col", "row"),
            P("row"),
            P("row", "col"),
            P("row", "col"),
            P("col", "row"),
            P("dp", "row"),
        ),
        out_specs=(
            P("dp", "row"),
            P("dp", "row"),
            P("row"),
            P("row", "col"),
            P("row", "col"),
            P("row", "col"),
            P(),
            P(),
            P("col", "row"),
            P("row"),
            P("row", "col"),
            P("row", "col"),
            P("col", "row"),
        ),
        check_vma=False,
    )
```

```python
from functools import partial

import jax
import jax.numpy as jnp
from jax import lax
from jax.experimental import pallas as pl
from jax.experimental.pallas import tpu as pltpu
from jax.sharding import PartitionSpec as P

epsilon = 1e-06
rope_base = 1000000.0
lanes = 128
full_vmem = 67043328
chunk_limit = 262144
lag = 2
low = jnp.bfloat16
wide = jnp.float32


def dot(a, b, contract=((1,), (0,))):
    return lax.dot_general(a, b, (contract, ((), ())), preferred_element_type=wide)


def dot_t(a, b):
    return dot(a, b, ((1,), (1,)))


def t_dot(a, b):
    return dot(a, b, ((0,), (0,)))


def window(index, size):
    return pl.ds(pl.multiple_of(index * size, lanes), size)


def remote(source, target, send, receive, axis, index):
    return pltpu.make_async_remote_copy(
        src_ref=source,
        dst_ref=target,
        send_sem=send,
        recv_sem=receive,
        device_id={axis: index},
        device_id_type=pl.DeviceIdType.MESH,
    )


def greet(groups):
    barrier = pltpu.get_barrier_semaphore()
    total = 0
    for axis, size in groups:
        me = lax.axis_index(axis)
        for shift in range(1, size):
            pl.semaphore_signal(
                barrier,
                inc=1,
                device_id={axis: lax.rem(me + shift, size)},
                device_id_type=pl.DeviceIdType.MESH,
            )
            total += 1
    if total:
        pl.semaphore_wait(barrier, total)


def half_turn(values):
    size = values.shape[-1]
    turned = pltpu.roll(values, size // 2, axis=1)
    lane = lax.broadcasted_iota(jnp.int32, values.shape, 1)
    return jnp.where(lane < size // 2, -turned, turned)


class Exchange:
    def __init__(self, axis, size, send, receive, send_sem, receive_sem):
        self.axis, self.size = axis, size
        self.send, self.receive = send, receive
        self.send_sem, self.receive_sem = send_sem, receive_sem
        self.me = lax.axis_index(axis)

    def target(self, shift):
        return lax.rem(self.me + shift, self.size)

    def source(self, shift):
        return lax.rem(self.me + self.size - shift, self.size)

    def copy(self, shift):
        sent = self.send(shift)
        return remote(
            sent,
            self.receive.at[shift - 1],
            self.send_sem.at[shift - 1],
            self.receive_sem.at[shift - 1],
            self.axis,
            self.target(shift),
        )

    def start(self, shift):
        self.copy(shift).start()

    def arrive(self, shift):
        self.copy(shift).wait_recv()

    def finish(self):
        for shift in range(1, self.size):
            self.copy(shift).wait_send()


class Ranked(Exchange):
    def copy(self, shift):
        return remote(
            self.send(shift),
            self.receive.at[self.me],
            self.send_sem.at[shift - 1],
            self.receive_sem.at[shift - 1],
            self.axis,
            self.target(shift),
        )

    def total(self, rows):
        result = self.receive[0, rows]
        for member in range(1, self.size):
            result = result + self.receive[member, rows]
        return result


def each_tile(rows, body):
    tile = lanes if rows % lanes == 0 else rows

    def step(index, carry):
        body(pl.ds(pl.multiple_of(index * tile, tile), tile), index * tile, tile)
        return carry

    lax.fori_loop(0, rows // tile, step, 0)


def forward_kernel(
    rows_of,
    cols_of,
    members,
    need,
    x,
    seg_row,
    seg_col,
    inverse,
    gain1,
    wq,
    wk,
    wv,
    qn,
    kn,
    wo,
    gain2,
    wg,
    wu,
    ct,
    n1,
    fs,
    raw,
    lows,
    shares,
    trig,
    mixed,
    mid,
    ss,
    n2,
    hid,
    slope,
    ct_all,
    unit,
    pq_own,
    pq_s,
    pq_r,
    pg_own,
    pg_s,
    pg_r,
    mixed_r,
    stat_s,
    stat_r,
    ox_s,
    ox_r,
    row_send,
    row_recv,
    stat_send,
    stat_recv,
    col_send,
    col_recv,
    ct_send,
    ct_recv,
    ct_store,
):
    tokens, depth = x.shape
    width = depth * rows_of
    qw, kw, fw = wq.shape[1] // rows_of, wk.shape[1] // rows_of, wg.shape[1] // rows_of
    size = qn.shape[1]
    heads, key_heads = qw // size, kw // size
    group = heads // key_heads
    scale = size ** (-0.5)
    me = lax.axis_index("row")
    greet((("row", rows_of), ("col", cols_of), ("dp", members)))

    def row_exchange(kind, send, receive):
        return Exchange("row", rows_of, send, receive, row_send.at[kind], row_recv.at[kind])

    def stat_exchange(kind):
        return Ranked(
            "row",
            rows_of,
            lambda shift: stat_s.at[kind],
            stat_r.at[kind],
            stat_send.at[kind],
            stat_recv.at[kind],
        )

    stat1 = stat_exchange(0)

    def prepare(rows, start, tile):
        value = x[rows, :].astype(wide)
        square = jnp.broadcast_to(jnp.sum(value * value, axis=1, keepdims=True), (tile, lanes))
        stat_s[0, rows] = square
        stat_r[0, me, rows] = square
        unit[rows, :] = (value * gain1[...]).astype(low)

    each_tile(tokens, prepare)
    for shift in range(1, rows_of):
        stat1.start(shift)

    def project(index, target, slot):
        u = unit[...]
        q = dot(u, wq[:, window(index, qw)])
        k = dot(u, wk[:, window(index, kw)])
        v = dot(u, wv[:, window(index, kw)])
        kind = target.dtype
        if slot is None:
            target[:, :qw] = q.astype(kind)
            target[:, qw : qw + kw] = k.astype(kind)
            target[:, qw + kw :] = v.astype(kind)
        else:
            target[slot, :, :qw] = q.astype(kind)
            target[slot, :, qw : qw + kw] = k.astype(kind)
            target[slot, :, qw + kw :] = v.astype(kind)

    qkv = row_exchange(0, lambda shift: pq_s.at[shift - 1], pq_r)
    for shift in range(1, rows_of):
        project(qkv.target(shift), pq_s, shift - 1)
        qkv.start(shift)
    project(me, pq_own, None)

    need("ct")
    spread = Ranked("dp", members, lambda shift: ct, ct_all, ct_send, ct_recv)
    kept = pltpu.make_async_copy(ct, ct_all.at[spread.me], ct_store.at[0])
    kept.start()
    for shift in range(1, members):
        spread.start(shift)

    def tables(rows, start, tile):
        key = lax.broadcasted_iota(jnp.int32, (tile, tokens), 1)
        query = lax.broadcasted_iota(jnp.int32, (tile, tokens), 0) + start
        allowed = (seg_col[rows, :] == seg_row[...]) & (key <= query)
        count = jnp.sum(jnp.where(allowed, 1.0, 0.0), axis=1, keepdims=True) - 1.0
        angle = count * inverse[...]
        trig[0, rows, :] = jnp.cos(angle)
        trig[1, rows, :] = jnp.sin(angle)

    each_tile(tokens, tables)

    for shift in range(1, rows_of):
        stat1.arrive(shift)
        qkv.arrive(shift)

    def heads_in(rows, start, tile):
        first = lax.rsqrt(stat1.total(rows) / width + epsilon)
        fs[rows, :] = first
        first = first[:, :1]
        n1[rows, :] = (x[rows, :].astype(wide) * first * gain1[...]).astype(low)
        value = pq_own[rows, :]
        for shift in range(1, rows_of):
            value = value + pq_r[shift - 1, rows, :].astype(wide)
        value = value * first
        raw[rows, :] = value[:, : qw + kw]
        cosine, sine = trig[0, rows, :], trig[1, rows, :]
        for head in range(heads + key_heads):
            piece = value[:, head * size : (head + 1) * size]
            gain = qn[...] if head < heads else kn[...]
            norm = lax.rsqrt(jnp.mean(piece * piece, axis=1, keepdims=True) + epsilon)
            normed = piece * norm * gain
            rotated = normed * cosine + half_turn(normed) * sine
            lows[rows, head * size : (head + 1) * size] = rotated.astype(low)
        lows[rows, qw + kw :] = value[:, qw + kw :].astype(low)

    each_tile(tokens, heads_in)

    def attend(rows, start, tile):
        key = lax.broadcasted_iota(jnp.int32, (tile, tokens), 1)
        query = lax.broadcasted_iota(jnp.int32, (tile, tokens), 0) + start
        allowed = (seg_col[rows, :] == seg_row[...]) & (key <= query)
        for head in range(heads):
            pair = head // group
            keys = lows[:, qw + pair * size : qw + (pair + 1) * size]
            values = lows[:, qw + kw + pair * size : qw + kw + (pair + 1) * size]
            scores = dot_t(lows[rows, head * size : (head + 1) * size], keys) * scale
            numerators = jnp.where(allowed, jnp.exp(scores), 0.0)
            share = numerators / jnp.sum(numerators, axis=1, keepdims=True)
            shares[head, rows, :] = share
            mixed[0, rows, head * size : (head + 1) * size] = dot(
                share.astype(low), values
            ).astype(low)

    each_tile(tokens, attend)

    gather = row_exchange(2, lambda shift: mixed.at[0], mixed_r)
    for shift in range(1, rows_of):
        gather.start(shift)
    need("wo")
    ox_s[...] = dot(mixed[0], wo[window(me, qw), :])
    for shift in range(1, rows_of):
        gather.arrive(shift)
        mixed[shift] = mixed_r[shift - 1]
        ox_s[...] += dot(mixed_r[shift - 1], wo[window(gather.source(shift), qw), :])
    column = Exchange("col", cols_of, lambda shift: ox_s, ox_r, col_send, col_recv)
    for shift in range(1, cols_of):
        column.start(shift)
    for shift in range(1, cols_of):
        column.arrive(shift)

    stat2 = stat_exchange(1)

    def middle(rows, start, tile):
        value = ox_s[rows, :]
        for shift in range(1, cols_of):
            value = value + ox_r[shift - 1, rows, :]
        value = x[rows, :].astype(wide) + value
        mid[rows, :] = value
        square = jnp.broadcast_to(jnp.sum(value * value, axis=1, keepdims=True), (tile, lanes))
        stat_s[1, rows] = square
        stat_r[1, me, rows] = square
        unit[rows, :] = (value * gain2[...]).astype(low)

    each_tile(tokens, middle)
    for shift in range(1, rows_of):
        stat2.start(shift)

    need("wg", "wu")
    feed = row_exchange(3, lambda shift: pg_s.at[shift - 1], pg_r)
    for shift in range(1, rows_of):
        columns = window(feed.target(shift), fw)
        pg_s[shift - 1, :, :fw] = dot(unit[...], wg[:, columns]).astype(low)
        pg_s[shift - 1, :, fw:] = dot(unit[...], wu[:, columns]).astype(low)
        feed.start(shift)
    pg_own[:, :fw] = dot(unit[...], wg[:, window(me, fw)])
    pg_own[:, fw:] = dot(unit[...], wu[:, window(me, fw)])
    for shift in range(1, rows_of):
        stat2.arrive(shift)

    def scale_rows(rows, start, tile):
        second = lax.rsqrt(stat2.total(rows) / width + epsilon)
        ss[rows, :] = second
        n2[rows, :] = (mid[rows, :] * second[:, :1] * gain2[...]).astype(low)

    each_tile(tokens, scale_rows)
    for shift in range(1, rows_of):
        feed.arrive(shift)

    def activate(rows, start, tile):
        second = ss[rows, :1]
        gate = pg_own[rows, :fw]
        upward = pg_own[rows, fw:]
        for shift in range(1, rows_of):
            gate = gate + pg_r[shift - 1, rows, :fw].astype(wide)
            upward = upward + pg_r[shift - 1, rows, fw:].astype(wide)
        gate = gate * second
        upward = upward * second
        sigmoid = jax.nn.sigmoid(gate)
        silu = gate * sigmoid
        hid[rows, :] = (silu * upward).astype(low)
        slope[rows, :fw] = upward * sigmoid * (1.0 + gate * (1.0 - sigmoid))
        slope[rows, fw:] = silu

    each_tile(tokens, activate)
    for shift in range(1, members):
        spread.arrive(shift)
    kept.wait()
    for exchange in (stat1, qkv, gather, column, stat2, feed, spread):
        exchange.finish()


def split(rows, columns):
    count = 1
    while rows % count or (rows // count) * columns > chunk_limit:
        count += 1
    return count


class Line:
    def __init__(self, members, out, near, far, spares, sems):
        self.members, self.out, self.near, self.far = members, out, near, far
        self.spares = spares
        self.in_send, self.near_sem, self.far_sem, self.out_send, self.store_sem, self.load_sem = sems
        me = lax.axis_index("dp")
        half = members // 2
        left = me < half
        place = jnp.where(left, half - 1 - me, me - half)
        self.inner = jnp.where(left, me + 1, me - 1)
        self.outer = jnp.where(left, jnp.maximum(me - 1, 0), jnp.minimum(me + 1, members - 1))
        self.is_mid = place == 0
        self.not_mid = place > 0
        self.has_outer = place < half - 1
        self.is_end = place == half - 1
        self.chunks, self.done = [], 0

    def view(self, refs, index):
        which, row, rows, column, columns = self.chunks[index]
        if not isinstance(row, int):
            row = pl.multiple_of(row, 16)
        if not isinstance(column, int):
            column = pl.multiple_of(column, lanes)
        return refs[which].at[pl.ds(row, rows), pl.ds(column, columns)]

    def inward(self, index, target, sem):
        return remote(
            self.view(self.out, index),
            self.view(target, index),
            self.in_send.at[index],
            sem.at[index],
            "dp",
            self.inner,
        )

    def outward(self, index):
        return remote(
            self.view(self.out, index),
            self.view(self.far, index),
            self.out_send.at[index],
            self.far_sem.at[index],
            "dp",
            self.outer,
        )

    def relay(self, index):
        return remote(
            self.view(self.far, index),
            self.view(self.far, index),
            self.out_send.at[index],
            self.far_sem.at[index],
            "dp",
            self.outer,
        )

    def send_in(self, index):
        @pl.when(self.is_mid)
        def _():
            self.inward(index, self.far, self.far_sem).start()

        @pl.when(self.not_mid)
        def _():
            self.inward(index, self.near, self.near_sem).start()

    def release(self, which, row, rows, column, columns):
        if self.members == 1:
            return
        count = split(rows, columns)
        for part in range(count):
            size = rows // count
            self.chunks.append((which, row + part * size, size, column, columns))
            index = len(self.chunks) - 1

            @pl.when(self.is_end)
            def _(index=index):
                self.send_in(index)

    def spare(self, index, kind):
        _, _, rows, _, columns = self.chunks[index]
        for ref in self.spares:
            if ref.shape[1:] == (rows, columns):
                return ref.at[kind]
        raise ValueError("no spare")

    def load(self, index, kind):
        source = self.view((self.near, self.far)[kind], index)
        return pltpu.make_async_copy(source, self.spare(index, kind), self.load_sem.at[kind])

    def add(self, index, kind):
        target, other = self.view(self.out, index), self.spare(index, kind)
        rows = other.shape[0]
        tile = 32 if rows % 32 == 0 else rows

        def step(part, carry):
            spot = pl.ds(pl.multiple_of(part * tile, 16), tile)
            target[spot, :] = (target[spot, :].astype(wide) + other[spot, :].astype(wide)).astype(low)
            return carry

        lax.fori_loop(0, rows // tile, step, 0)

    def begin_total(self, index):
        @pl.when(self.is_mid)
        def _():
            self.inward(index, self.far, self.far_sem).wait_recv()
            self.load(index, 1).start()

    def store(self, index):
        return pltpu.make_async_copy(
            self.view(self.out, index), self.view(self.far, index), self.store_sem.at[index]
        )

    def end_total(self, index):
        @pl.when(self.is_mid)
        def _():
            self.load(index, 1).wait()
            self.inward(index, self.far, self.far_sem).wait_send()
            self.add(index, 1)

            @pl.when(self.has_outer)
            def _():
                self.outward(index).start()

            self.store(index).start()

    def advance(self, count):
        if self.members == 1:
            return
        for _ in range(count):
            index = self.done
            self.done += 1

            @pl.when(self.has_outer)
            def _():
                self.inward(index, self.near, self.near_sem).wait_recv()
                self.load(index, 0).start()

            if index >= lag:
                self.begin_total(index - lag)

            @pl.when(self.has_outer)
            def _():
                self.load(index, 0).wait()
                self.add(index, 0)
                self.send_in(index)

            if index >= lag:
                self.end_total(index - lag)

    def settle(self):
        total = len(self.chunks)
        self.advance(total - self.done)
        for index in range(max(total - lag, 0), total):
            self.begin_total(index)
            self.end_total(index)

        @pl.when(self.not_mid)
        def _():
            for index in range(total):
                self.inward(index, self.far, self.far_sem).wait_recv()

                @pl.when(self.has_outer)
                def _():
                    self.relay(index).start()

            for index in range(total):
                self.inward(index, self.near, self.near_sem).wait_send()

                @pl.when(self.has_outer)
                def _():
                    self.relay(index).wait_send()

        @pl.when(self.is_mid)
        def _():
            for index in range(total):
                self.store(index).wait()

                @pl.when(self.has_outer)
                def _():
                    self.outward(index).wait_send()


class Chain:
    def __init__(self, members, own, blocks, send, receive, pass_send, pass_recv, row):
        self.members, self.own, self.blocks, self.row = members, own, blocks, row
        self.send, self.receive = send, receive
        self.pass_send, self.pass_recv = pass_send, pass_recv
        self.me = lax.axis_index("dp")

    def valid(self, place):
        return (place >= 0) & (place < self.members)

    def step(self, side, hop):
        way = 1 - 2 * side
        origin = self.me - way * (hop - 1)
        spot = self.blocks.at[origin, self.row.me]
        return remote(
            self.own if hop == 1 else spot,
            spot,
            self.send.at[side, hop - 1],
            self.receive.at[side, hop - 1],
            "dp",
            self.me + way,
        )

    def incoming(self, side, hop):
        origin = self.me - (1 - 2 * side) * hop
        spot = self.blocks.at[origin, self.row.me]
        return origin, remote(
            spot,
            spot,
            self.send.at[side, hop - 1],
            self.receive.at[side, hop - 1],
            "dp",
            self.me,
        )

    def sends(self, side, hop):
        way = 1 - 2 * side
        return self.valid(self.me - way * (hop - 1)) & self.valid(self.me + way)

    def hop(self, hop):
        for side in range(2):
            if hop > 1:
                self.await_block(side, hop - 1)

            @pl.when(self.sends(side, hop))
            def _(side=side):
                self.step(side, hop).start()

    def await_block(self, side, hop):
        @pl.when(self.valid(self.me - (1 - 2 * side) * hop))
        def _():
            self.incoming(side, hop)[1].wait_recv()

    def pass_on(self, side, hop, shift):
        origin = self.me - (1 - 2 * side) * hop
        spot = self.blocks.at[origin, self.row.me]
        return remote(
            spot,
            spot,
            self.pass_send.at[side, hop - 1, shift - 1],
            self.pass_recv.at[side, hop - 1, shift - 1],
            "row",
            self.row.target(shift),
        )

    def spread(self, hop):
        for side in range(2):
            if hop == self.members - 1:
                self.await_block(side, hop)

            @pl.when(self.valid(self.me - (1 - 2 * side) * hop))
            def _(side=side):
                for shift in range(1, self.row.size):
                    self.pass_on(side, hop, shift).start()

    def finish(self):
        for hop in range(1, self.members):
            for side in range(2):

                @pl.when(self.valid(self.me - (1 - 2 * side) * hop))
                def _(side=side, hop=hop):
                    for shift in range(1, self.row.size):
                        self.pass_on(side, hop, shift).wait_recv()
                        self.pass_on(side, hop, shift).wait_send()

                @pl.when(self.sends(side, hop))
                def _(side=side, hop=hop):
                    self.step(side, hop).wait_send()


def backward_kernel(
    rows_of,
    cols_of,
    members,
    need,
    x,
    ct,
    n1,
    fs,
    raw,
    lows,
    shares,
    trig,
    mixed,
    mid,
    ss,
    n2,
    hid,
    slope,
    gain1,
    gain2,
    qn,
    kn,
    wq,
    wk,
    wv,
    wo,
    wg,
    wu,
    wd,
    bo,
    ig,
    small,
    *rest,
):
    hid_all, *rest = rest
    far, near, rest = rest[:6], rest[6:12], rest[12:]
    grads, rest = rest[:6], rest[6:]
    gq, gk, gv, go, gg, gu = grads
    (
        gub,
        ph_s,
        ph_r,
        hid_r,
    gub_r,
    n_t,
    mb,
    ml,
    pm_own,
    pm_s,
    pm_r,
    sl,
    sb,
    dqkv,
    dqkv_r,
    gains,
    stat_s,
    stat_r,
    ox_s,
    ox_r,
    row_send,
    row_recv,
    stat_send,
    stat_recv,
        col_send,
        col_recv,
        small_r,
        small_send,
        small_recv,
        in_send,
        near_sem,
        far_sem,
        out_send,
        store_sem,
        load_sem,
        hop_send,
        hop_recv,
        pass_send,
        pass_recv,
        keep_sem,
        *spares,
    ) = rest
    tokens, depth = x.shape
    width = depth * rows_of
    qw, kw, fw = wq.shape[1] // rows_of, wk.shape[1] // rows_of, wg.shape[1] // rows_of
    size = qn.shape[1]
    heads, key_heads = qw // size, kw // size
    group = heads // key_heads
    scale = size ** (-0.5)
    me = lax.axis_index("row")
    greet((("row", rows_of), ("col", cols_of), ("dp", members)))
    line = Line(
        members,
        grads,
        near,
        far,
        spares,
        (in_send, near_sem, far_sem, out_send, store_sem, load_sem),
    )

    def row_exchange(kind, send, receive):
        return Exchange("row", rows_of, send, receive, row_send.at[kind], row_recv.at[kind])

    def stat_exchange(kind):
        return Ranked(
            "row",
            rows_of,
            lambda shift: stat_s.at[kind],
            stat_r.at[kind],
            stat_send.at[kind],
            stat_recv.at[kind],
        )

    def column_exchange(kind):
        return Exchange(
            "col",
            cols_of,
            lambda shift: ox_s.at[kind],
            ox_r.at[kind],
            col_send.at[kind],
            col_recv.at[kind],
        )

    def column_sum(kind, rows):
        value = ox_s[kind, rows, :]
        for shift in range(1, cols_of):
            value = value + ox_r[kind, shift - 1, rows, :]
        return value

    hide = row_exchange(0, lambda shift: hid, hid_r)
    gates = row_exchange(1, lambda shift: gub, gub_r)
    body = pl.ds(0, tokens)
    chain = Chain(members, hid, hid_all, hop_send, hop_recv, pass_send, pass_recv, hide)
    chain.hop(1)
    back = row_exchange(4, lambda shift: ph_s.at[shift - 1], ph_r)
    for shift in range(1, rows_of):
        ph_s[shift - 1] = dot_t(ct[...], wd[window(back.target(shift), fw), :]).astype(low)
        back.start(shift)
    stage = lax.axis_index("dp")

    def keep(shift):
        piece = hid if shift == 0 else hid_r.at[shift - 1]
        return pltpu.make_async_copy(
            piece, hid_all.at[stage, hide.source(shift)], keep_sem.at[shift]
        )

    keep(0).start()
    n_t[...] = n2[...].T
    need("slope")
    if members > 2:
        chain.hop(2)
    for shift in range(1, rows_of):
        back.arrive(shift)

    def behind(rows, start, tile):
        value = dot_t(ct[rows, :], wd[window(me, fw), :])
        for shift in range(1, rows_of):
            value = value + ph_r[shift - 1, rows, :].astype(wide)
        gub[rows, :fw] = (value * slope[rows, :fw]).astype(low)
        gub[rows, fw:] = (value * slope[rows, fw:]).astype(low)

    each_tile(tokens, behind)
    for shift in range(1, rows_of):
        gates.start(shift)
    for step in range(3, members):
        chain.hop(step)
    need("wg", "wu")
    for shift in range(rows_of):
        if shift:
            line.advance(1 if shift == 1 else 2)
            gates.arrive(shift)
        piece = gub if shift == 0 else gub_r.at[shift - 1]
        index = window(gates.source(shift), fw)
        part = dot_t(piece[:, :fw], wg[:, index]) + dot_t(piece[:, fw:], wu[:, index])
        if shift == 0:
            ox_s[1, body, :] = part
        else:
            ox_s[1, body, :] += part
        gg[:, index] = dot(n_t[...], piece[:, :fw]).astype(low)
        line.release(4, 0, depth, gates.source(shift) * fw, fw)
        gu[:, index] = dot(n_t[...], piece[:, fw:]).astype(low)
        line.release(5, 0, depth, gates.source(shift) * fw, fw)
    column1 = column_exchange(1)
    for shift in range(1, cols_of):
        column1.start(shift)
    line.advance(1)
    for shift in range(1, cols_of):
        column1.arrive(shift)

    stat2 = stat_exchange(0)
    small[...] = jnp.zeros_like(small)
    gains[...] = jnp.zeros_like(gains)

    def feed_stat(rows, start, tile):
        back = column_sum(1, rows)
        unit = mid[rows, :] * ss[rows, :1]
        small[1:2, :] += jnp.sum(back * unit, axis=0, keepdims=True)
        inner = jnp.sum(back * gain2[...] * unit, axis=1, keepdims=True)
        inner = jnp.broadcast_to(inner, (tile, lanes))
        stat_s[0, rows] = inner
        stat_r[0, me, rows] = inner

    each_tile(tokens, feed_stat)
    pad = pl.ds(tokens, 8)
    stat_s[0, pad] = jnp.zeros((8, lanes), wide)
    for shift in range(1, rows_of):
        stat2.start(shift)
    need("wo", "mixed", "lows", "shares")
    line.advance(1)
    for shift in range(1, rows_of):
        stat2.arrive(shift)

    def middle_back(rows, start, tile):
        second = ss[rows, :1]
        unit = mid[rows, :] * second
        inner = stat2.total(rows)[:, :1] / width
        value = ct[rows, :].astype(wide) + second * (
            column_sum(1, rows) * gain2[...] - unit * inner
        )
        mb[rows, :] = value
        ml[rows, :] = value.astype(low)

    each_tile(tokens, middle_back)
    blend = row_exchange(2, lambda shift: pm_s.at[shift - 1], pm_r)
    for shift in range(1, rows_of):
        pm_s[shift - 1] = dot_t(ml[...], wo[window(blend.target(shift), qw), :]).astype(low)
        blend.start(shift)
    pm_own[...] = dot_t(ml[...], wo[window(me, qw), :])
    for shift in range(rows_of):
        index = window(blend.source(shift), qw)
        go[index, :] = t_dot(mixed[shift], ml[...]).astype(low)
        line.release(3, blend.source(shift) * qw, qw, 0, depth)
    line.advance(2)
    for shift in range(1, rows_of):
        blend.arrive(shift)

    def share_back(rows, start, tile):
        value = pm_own[rows, :]
        for shift in range(1, rows_of):
            value = value + pm_r[shift - 1, rows, :].astype(wide)
        incoming = value.astype(low)
        pm_s[0, rows, :] = incoming
        product = incoming.astype(wide) * mixed[0, rows, :].astype(wide)
        for head in range(heads):
            pair = head // group
            part = slice(head * size, (head + 1) * size)
            values = lows[:, qw + kw + pair * size : qw + kw + (pair + 1) * size]
            delta = jnp.sum(product[:, part], axis=1, keepdims=True)
            share = shares[head, rows, :]
            sl[head, rows, :] = share.astype(low)
            sb[head, rows, :] = (share * (dot_t(incoming[:, part], values) - delta)).astype(low)

    blend.finish()
    each_tile(tokens, share_back)
    need("n1", "raw", "trig")
    n_t[...] = n1[...].T
    line.advance(1)

    def pull(head, back, gain, row):
        raw_piece = raw[:, head * size : (head + 1) * size]
        norm = lax.rsqrt(jnp.mean(raw_piece * raw_piece, axis=1, keepdims=True) + epsilon)
        unit = raw_piece * norm
        normed_back = back * trig[0] - half_turn(back * trig[1])
        gains[row : row + 1, :] += jnp.sum(normed_back * unit, axis=0, keepdims=True)
        unit_back = normed_back * gain
        return norm * (unit_back - unit * jnp.mean(unit_back * unit, axis=1, keepdims=True))

    for pair in range(key_heads):
        keys = lows[:, qw + pair * size : qw + (pair + 1) * size]
        key_back = jnp.zeros((tokens, size), wide)
        value_back = jnp.zeros((tokens, size), wide)
        for head in range(pair * group, (pair + 1) * group):
            part = slice(head * size, (head + 1) * size)
            value_back = value_back + t_dot(sl[head], pm_s[0, :, part])
            key_back = key_back + scale * t_dot(sb[head], lows[:, part])
            query_back = scale * dot(sb[head], keys)
            dqkv[:, part] = pull(head, query_back, qn[...], 0).astype(low)
        spot = qw + pair * size
        dqkv[:, spot : spot + size] = pull(heads + pair, key_back, kn[...], 1).astype(low)
        spot = qw + kw + pair * size
        dqkv[:, spot : spot + size] = value_back.astype(low)

    deliver = row_exchange(3, lambda shift: dqkv, dqkv_r)
    for shift in range(1, rows_of):
        deliver.start(shift)
    for shift in range(1, rows_of):
        hide.start(shift)
    need("wq", "wk", "wv")
    for shift in range(rows_of):
        if shift:
            line.advance(1)
            deliver.arrive(shift)
        piece = dqkv if shift == 0 else dqkv_r.at[shift - 1]
        source = deliver.source(shift)
        part = dot_t(piece[:, :qw], wq[:, window(source, qw)])
        part = part + dot_t(piece[:, qw : qw + kw], wk[:, window(source, kw)])
        part = part + dot_t(piece[:, qw + kw :], wv[:, window(source, kw)])
        if shift == 0:
            ox_s[2, body, :] = part
        else:
            ox_s[2, body, :] += part
    ox_s[2, pad, :] = jnp.zeros((8, depth), wide)
    ox_s[2, pad, :lanes] = gains[...]
    column2 = column_exchange(2)
    for shift in range(1, cols_of):
        column2.start(shift)
    for shift in range(rows_of):
        piece = dqkv if shift == 0 else dqkv_r.at[shift - 1]
        source = deliver.source(shift)
        gq[:, window(source, qw)] = dot(n_t[...], piece[:, :qw]).astype(low)
        gk[:, window(source, kw)] = dot(n_t[...], piece[:, qw : qw + kw]).astype(low)
        gv[:, window(source, kw)] = dot(n_t[...], piece[:, qw + kw :]).astype(low)
    line.release(0, 0, depth, 0, qw * rows_of)
    line.release(1, 0, depth, 0, kw * rows_of)
    line.release(2, 0, depth, 0, kw * rows_of)
    line.advance(1)
    for shift in range(1, cols_of):
        column2.arrive(shift)
    need("x", "fs")

    stat1 = stat_exchange(1)

    def first_stat(rows, start, tile):
        back = column_sum(2, rows)
        unit = x[rows, :].astype(wide) * fs[rows, :1]
        small[0:1, :] += jnp.sum(back * unit, axis=0, keepdims=True)
        inner = jnp.sum(back * gain1[...] * unit, axis=1, keepdims=True)
        inner = jnp.broadcast_to(inner, (tile, lanes))
        stat_s[1, rows] = inner
        stat_r[1, me, rows] = inner

    each_tile(tokens, first_stat)
    summed = column_sum(2, pad)[:, :lanes]
    stat_s[1, pad] = summed
    stat_r[1, me, pad] = summed
    for shift in range(1, rows_of):
        stat1.start(shift)
    line.advance(1)
    for shift in range(1, rows_of):
        stat1.arrive(shift)

    def finish(rows, start, tile):
        first = fs[rows, :1]
        unit = x[rows, :].astype(wide) * first
        inner = stat1.total(rows)[:, :1] / width
        ig[rows, :] = mb[rows, :] + first * (column_sum(2, rows) * gain1[...] - unit * inner)

    each_tile(tokens, finish)
    small[8:16, :lanes] = stat1.total(pad)
    ranked = Ranked("dp", members, lambda shift: small, small_r, small_send, small_recv)
    if members > 1:
        small_r[lax.axis_index("dp")] = small[...]
        for shift in range(1, members):
            ranked.start(shift)
    line.advance(3)
    for shift in range(rows_of):
        if shift:
            hide.arrive(shift)
            keep(shift).start()
        piece = hid[...] if shift == 0 else hid_r[shift - 1]
        part = dot(piece, wd[window(hide.source(shift), fw), :])
        if shift == 0:
            ox_s[0, body, :] = part
        else:
            ox_s[0, body, :] += part
    column0 = column_exchange(0)
    for shift in range(1, cols_of):
        column0.start(shift)
    for step in range(1, members):
        chain.spread(step)
    line.advance(1)
    for shift in range(1, cols_of):
        column0.arrive(shift)

    def result(rows, start, tile):
        bo[rows, :] = (mid[rows, :] + column_sum(0, rows)).astype(low)

    each_tile(tokens, result)
    if members > 1:
        line.settle()
        for shift in range(1, members):
            ranked.arrive(shift)
        ranked.finish()
        summed = small_r[0]
        for member in range(1, members):
            summed = summed + small_r[member]
        small[...] = summed
    chain.finish()
    for shift in range(rows_of):
        keep(shift).wait()
    for exchange in (hide, back, gates, column0, column1, stat2, deliver, column2, stat1):
        exchange.finish()


def widen_kernel(*refs):
    count = (len(refs) - 3) // 2
    hid_all, ct_all = refs[count : count + 2]
    *out, gd = refs[count + 2 :]
    for source, target in zip(refs[:count], out):
        target[...] = source[...].astype(wide)
    total = t_dot(hid_all[0, 0], ct_all[0])
    for member in range(1, ct_all.shape[0]):
        total = total + t_dot(hid_all[member, 0], ct_all[member])
    gd[...] = total


def widen(partials, hid_all, ct_all, shape):
    members, rows_of, tokens, fw = hid_all.shape
    parts = 2 if fw % (2 * lanes) == 0 else 1
    steps = rows_of * parts

    def rows(array_shape):
        return pl.BlockSpec((array_shape[0] // steps, array_shape[1]), lambda i: (i, 0))

    specs = [rows(partial_sum.shape) for partial_sum in partials]
    return pl.pallas_call(
        widen_kernel,
        grid=(steps,),
        out_shape=tuple(
            jax.ShapeDtypeStruct(array_shape, wide)
            for array_shape in [*(partial_sum.shape for partial_sum in partials), shape]
        ),
        in_specs=specs
        + [
            pl.BlockSpec(
                (members, 1, tokens, fw // parts), lambda i: (0, i // parts, 0, i % parts)
            ),
            pl.BlockSpec(ct_all.shape, lambda i: (0, 0, 0)),
        ],
        out_specs=tuple(specs + [rows(shape)]),
        compiler_params=pltpu.CompilerParams(vmem_limit_bytes=full_vmem),
    )(*partials, hid_all, ct_all)


def vmem(shape, kind):
    return pltpu.VMEM(shape, kind)


def call(kernel, shapes, scratch, identity, arguments, late=(), outside=()):
    inside, away = pl.BlockSpec(memory_space=pltpu.VMEM), pl.BlockSpec(memory_space=pl.ANY)
    names = list(arguments)
    late = [name for name in names if name in late]

    def body(*refs):
        given = dict(zip(names, refs))
        rest = refs[len(names) :]
        copies = {}
        if late:
            holders, sem = rest[-len(late) - 1 : -1], rest[-1]
            rest = rest[: -len(late) - 1]
            for index, name in enumerate(late):
                copies[name] = pltpu.make_async_copy(given[name], holders[index], sem.at[index])
                copies[name].start()
                given[name] = holders[index]

        def need(*wanted):
            for name in wanted:
                copy = copies.pop(name, None)
                if copy is not None:
                    copy.wait()

        kernel(need, *given.values(), *rest)
        need(*list(copies))

    extra = []
    if late:
        extra = [vmem(arguments[name].shape, arguments[name].dtype) for name in late]
        extra.append(pltpu.SemaphoreType.DMA((len(late),)))
    return pl.pallas_call(
        body,
        out_shape=tuple(jax.ShapeDtypeStruct(shape, kind) for shape, kind in shapes),
        in_specs=[away if name in late else inside for name in names],
        out_specs=tuple(away if index in outside else inside for index in range(len(shapes))),
        scratch_shapes=scratch + extra,
        compiler_params=pltpu.CompilerParams(
            collective_id=identity, has_side_effects=True, vmem_limit_bytes=full_vmem
        ),
    )(*arguments.values())


def per_device(
    block_input,
    segments,
    attention_norm,
    query_weight,
    key_weight,
    value_weight,
    query_norm,
    key_norm,
    output_weight,
    feedforward_norm,
    gate_weight,
    up_weight,
    down_weight,
    cotangent,
):
    rows_of, cols_of, members = (lax.axis_size(name) for name in ("row", "col", "dp"))
    tokens, depth = block_input.shape
    size = query_norm.shape[0]
    qw, kw, fw = (
        weight.shape[1] // rows_of for weight in (query_weight, key_weight, gate_weight)
    )
    heads = qw // size
    others, beside = max(rows_of - 1, 1), max(cols_of - 1, 1)
    half = size // 2
    inverse = rope_base ** (-2.0 * jnp.arange(half, dtype=wide) / size)
    inverse = jnp.concatenate([inverse, inverse])[None, :]
    seg_row = segments.reshape(1, tokens)
    seg_col = segments.reshape(tokens, 1)
    gain1, gain2 = attention_norm[None, :], feedforward_norm[None, :]
    qn, kn = query_norm[None, :], key_norm[None, :]
    total = qw + 2 * kw
    peers = max(members - 1, 1)
    dma = pltpu.SemaphoreType.DMA

    def sems(kinds):
        return [
            dma((5, others)),
            dma((5, others)),
            dma((2, others)),
            dma((2, others)),
            dma((kinds, beside)) if kinds > 1 else dma((beside,)),
            dma((kinds, beside)) if kinds > 1 else dma((beside,)),
        ]

    saved = call(
        partial(forward_kernel, rows_of, cols_of, members),
        (
            ((tokens, depth), low),
            ((tokens, lanes), wide),
            ((tokens, qw + kw), wide),
            ((tokens, total), low),
            ((heads, tokens, tokens), wide),
            ((2, tokens, size), wide),
            ((rows_of, tokens, qw), low),
            ((tokens, depth), wide),
            ((tokens, lanes), wide),
            ((tokens, depth), low),
            ((tokens, fw), low),
            ((tokens, 2 * fw), wide),
            ((members, tokens, depth), low),
        ),
        [
            vmem((tokens, depth), low),
            vmem((tokens, total), wide),
            vmem((others, tokens, total), low),
            vmem((others, tokens, total), low),
            vmem((tokens, 2 * fw), wide),
            vmem((others, tokens, 2 * fw), low),
            vmem((others, tokens, 2 * fw), low),
            vmem((others, tokens, qw), low),
            vmem((2, tokens, lanes), wide),
            vmem((2, rows_of, tokens, lanes), wide),
            vmem((tokens, depth), wide),
            vmem((beside, tokens, depth), wide),
        ]
        + sems(1)
        + [dma((peers,)), dma((peers,)), dma((1,))],
        0,
        dict(
            x=block_input,
            seg_row=seg_row,
            seg_col=seg_col,
            inverse=inverse,
            gain1=gain1,
            wq=query_weight,
            wk=key_weight,
            wv=value_weight,
            qn=qn,
            kn=kn,
            wo=output_weight,
            gain2=gain2,
            wg=gate_weight,
            wu=up_weight,
            ct=cotangent,
        ),
        late=("wo", "wg", "wu", "ct"),
        outside=(12,),
    )
    *saved, ct_all = saved
    saved = dict(
        zip(("n1", "fs", "raw", "lows", "shares", "trig", "mixed", "mid", "ss", "n2", "hid", "slope"), saved)
    )
    weights = (query_weight, key_weight, value_weight, output_weight, gate_weight, up_weight)
    shapes = [weight.shape for weight in weights]
    pieces = {
        (depth, fw): 2 * rows_of,
        (qw, depth): rows_of,
        (depth, qw * rows_of): 1,
        (depth, kw * rows_of): 2,
    }
    slots = sum(split(*shape) * times for shape, times in pieces.items())
    spares = {(shape[0] // split(*shape), shape[1]) for shape in pieces}
    done = call(
        partial(backward_kernel, rows_of, cols_of, members),
        (
            ((tokens, depth), low),
            ((tokens, depth), wide),
            ((16, depth), wide),
            ((members, rows_of, tokens, fw), low),
            *((shape, low) for shape in shapes * 2),
        ),
        [vmem(shape, low) for shape in shapes]
        + [
            vmem((tokens, 2 * fw), low),
            vmem((others, tokens, fw), low),
            vmem((others, tokens, fw), low),
            vmem((others, tokens, fw), low),
            vmem((others, tokens, 2 * fw), low),
            vmem((depth, tokens), low),
            vmem((tokens, depth), wide),
            vmem((tokens, depth), low),
            vmem((tokens, qw), wide),
            vmem((others, tokens, qw), low),
            vmem((others, tokens, qw), low),
            vmem((heads, tokens, tokens), low),
            vmem((heads, tokens, tokens), low),
            vmem((tokens, total), low),
            vmem((others, tokens, total), low),
            vmem((8, lanes), wide),
            vmem((2, tokens + 8, lanes), wide),
            vmem((2, rows_of, tokens + 8, lanes), wide),
            vmem((3, tokens + 8, depth), wide),
            vmem((3, beside, tokens + 8, depth), wide),
        ]
        + sems(3)
        + [vmem((members, 16, depth), wide), dma((peers,)), dma((peers,))]
        + [dma((slots,))] * 5
        + [dma((2,))]
        + [dma((2, peers))] * 2
        + [dma((2, peers, others))] * 2
        + [dma((rows_of,))]
        + [vmem((2, *shape), low) for shape in sorted(spares)],
        1,
        dict(
            x=block_input,
            ct=cotangent,
            **saved,
            gain1=gain1,
            gain2=gain2,
            qn=qn,
            kn=kn,
            wq=query_weight,
            wk=key_weight,
            wv=value_weight,
            wo=output_weight,
            wg=gate_weight,
            wu=up_weight,
            wd=down_weight,
        ),
        late=("x", "n1", "fs", "raw", "lows", "shares", "trig", "mixed", "slope", "wq", "wk", "wv", "wo", "wg", "wu"),
        outside=range(3, 16),
    )
    block_output, input_gradient, small, hid_all, *partials = done[:10]
    gq, gk, gv, go, gg, gu, gd = widen(partials, hid_all, ct_all, down_weight.shape)
    return (
        block_output,
        input_gradient,
        small[0],
        gq,
        gk,
        gv,
        small[8, :size],
        small[9, :size],
        go,
        small[1],
        gg,
        gu,
        gd,
    )


def solution(mesh):
    return jax.shard_map(
        per_device,
        mesh=mesh,
        in_specs=(
            P("dp", "row"),
            P("dp", None),
            P("row"),
            P("row", "col"),
            P("row", "col"),
            P("row", "col"),
            P(),
            P(),
            P("col", "row"),
            P("row"),
            P("row", "col"),
            P("row", "col"),
            P("col", "row"),
            P("dp", "row"),
        ),
        out_specs=(
            P("dp", "row"),
            P("dp", "row"),
            P("row"),
            P("row", "col"),
            P("row", "col"),
            P("row", "col"),
            P(),
            P(),
            P("col", "row"),
            P("row"),
            P("row", "col"),
            P("row", "col"),
            P("col", "row"),
        ),
        check_vma=False,
    )
```

```python
from functools import partial

import jax
import jax.numpy as jnp
from jax import lax
from jax.experimental import pallas as pl
from jax.experimental.pallas import tpu as pltpu
from jax.sharding import PartitionSpec as P

epsilon = 1e-06
rope_base = 1000000.0
lanes = 128
full_vmem = 67043328
chunk_limit = 131072
lag = 3
pace = 2
bulk = 6
slots_left = 1000
low = jnp.bfloat16
wide = jnp.float32


def dot(a, b, contract=((1,), (0,))):
    return lax.dot_general(a, b, (contract, ((), ())), preferred_element_type=wide)


def dot_t(a, b):
    return dot(a, b, ((1,), (1,)))


def t_dot(a, b):
    return dot(a, b, ((0,), (0,)))


def window(index, size):
    return pl.ds(pl.multiple_of(index * size, lanes), size)


def remote(source, target, send, receive, axis, index):
    return pltpu.make_async_remote_copy(
        src_ref=source,
        dst_ref=target,
        send_sem=send,
        recv_sem=receive,
        device_id={axis: index},
        device_id_type=pl.DeviceIdType.MESH,
    )


def greet(groups):
    barrier = pltpu.get_barrier_semaphore()
    total = 0
    for axis, size in groups:
        me = lax.axis_index(axis)
        for shift in range(1, size):
            pl.semaphore_signal(
                barrier,
                inc=1,
                device_id={axis: lax.rem(me + shift, size)},
                device_id_type=pl.DeviceIdType.MESH,
            )
            total += 1
    if total:
        pl.semaphore_wait(barrier, total)


def half_turn(values):
    size = values.shape[-1]
    turned = pltpu.roll(values, size // 2, axis=1)
    lane = lax.broadcasted_iota(jnp.int32, values.shape, 1)
    return jnp.where(lane < size // 2, -turned, turned)


class Exchange:
    def __init__(self, axis, size, send, receive, send_sem, receive_sem):
        self.axis, self.size = axis, size
        self.send, self.receive = send, receive
        self.send_sem, self.receive_sem = send_sem, receive_sem
        self.me = lax.axis_index(axis)

    def target(self, shift):
        return lax.rem(self.me + shift, self.size)

    def source(self, shift):
        return lax.rem(self.me + self.size - shift, self.size)

    def copy(self, shift):
        sent = self.send(shift)
        return remote(
            sent,
            self.receive.at[shift - 1],
            self.send_sem.at[shift - 1],
            self.receive_sem.at[shift - 1],
            self.axis,
            self.target(shift),
        )

    def start(self, shift):
        self.copy(shift).start()

    def arrive(self, shift):
        self.copy(shift).wait_recv()

    def finish(self):
        for shift in range(1, self.size):
            self.copy(shift).wait_send()


class Ranked(Exchange):
    def copy(self, shift):
        return remote(
            self.send(shift),
            self.receive.at[self.me],
            self.send_sem.at[shift - 1],
            self.receive_sem.at[shift - 1],
            self.axis,
            self.target(shift),
        )

    def total(self, rows):
        result = self.receive[0, rows]
        for member in range(1, self.size):
            result = result + self.receive[member, rows]
        return result


class Reduce:
    def __init__(self, size, produce, send, receive, extra, send_sem, receive_sem):
        self.size, self.produce = size, produce
        self.send, self.receive, self.extra = send, receive, extra
        self.send_sem, self.receive_sem = send_sem, receive_sem
        self.halved = size == 4
        self.count = 2 if self.halved else size - 1
        me = lax.axis_index("row")
        if self.halved:
            self.half = send.shape[1] // 2
            beside = me + 1 - 2 * lax.rem(me, 2)
            across = lax.rem(me + 2, 4)
            self.members = (beside, across, lax.rem(beside + 2, 4))
        else:
            self.direct = Exchange(
                "row", size, lambda shift: send.at[shift - 1], receive, send_sem, receive_sem
            )

    def rows(self, part):
        return pl.ds(part * self.half, self.half)

    def copy(self, kind):
        slot, part, to = ((2, 0, 0), (2, 1, 1), (0, 0, 0), (1, 1, 1), (0, 1, 0), (1, 0, 1))[kind]
        source = self.send.at[slot, self.rows(part)]
        target = self.extra.at[to] if slot == 2 else self.receive.at[slot, self.rows(part)]
        return remote(
            source,
            target,
            self.send_sem.at[kind],
            self.receive_sem.at[kind],
            "row",
            self.members[to],
        )

    def start(self):
        if not self.halved:
            for shift in range(1, self.size):
                self.produce(self.direct.target(shift), shift - 1)
                self.direct.start(shift)
            return
        self.produce(self.members[2], 2)
        self.copy(0).start()
        self.copy(1).start()
        self.produce(self.members[0], 0)
        self.copy(2).start()
        self.produce(self.members[1], 1)
        self.copy(3).start()

    def relay(self):
        if not self.halved:
            return
        for kind, slot in ((0, 1), (1, 0)):
            self.copy(kind).wait_recv()
            tile = 32 if self.half % 32 == 0 else self.half

            def step(index, carry, kind=kind, slot=slot, tile=tile):
                spot = pl.ds(pl.multiple_of(index * tile, 16), tile)
                rows = pl.ds(pl.multiple_of(kind * self.half + index * tile, 16), tile)
                total = self.send[slot, rows, :].astype(wide) + self.extra[kind, spot, :].astype(
                    wide
                )
                self.send[slot, rows, :] = total.astype(low)
                return carry

            lax.fori_loop(0, self.half // tile, step, 0)
            self.copy(5 - kind).start()

    def arrive(self):
        if not self.halved:
            for shift in range(1, self.size):
                self.direct.arrive(shift)
            return
        for kind in range(2, 6):
            self.copy(kind).wait_recv()

    def finish(self):
        if not self.halved:
            self.direct.finish()
            return
        for kind in range(6):
            self.copy(kind).wait_send()


def each_tile(rows, body):
    tile = lanes if rows % lanes == 0 else rows

    def step(index, carry):
        body(pl.ds(pl.multiple_of(index * tile, tile), tile), index * tile, tile)
        return carry

    lax.fori_loop(0, rows // tile, step, 0)


def forward_kernel(
    rows_of,
    cols_of,
    members,
    need,
    x,
    seg_row,
    seg_col,
    inverse,
    gain1,
    wq,
    wk,
    wv,
    qn,
    kn,
    wo,
    gain2,
    wg,
    wu,
    ct,
    n1,
    fs,
    raw,
    lows,
    shares,
    trig,
    mixed,
    mid,
    ss,
    n2,
    hid,
    slope,
    ct_all,
    unit,
    pq_own,
    pq_s,
    pq_r,
    pq_x,
    pg_own,
    pg_s,
    pg_r,
    pg_x,
    mixed_r,
    stat_s,
    stat_r,
    ox_s,
    ox_r,
    row_send,
    row_recv,
    stat_send,
    stat_recv,
    col_send,
    col_recv,
    ct_send,
    ct_recv,
    ct_store,
    sum_send,
    sum_recv,
):
    tokens, depth = x.shape
    width = depth * rows_of
    qw, kw, fw = wq.shape[1] // rows_of, wk.shape[1] // rows_of, wg.shape[1] // rows_of
    size = qn.shape[1]
    heads, key_heads = qw // size, kw // size
    group = heads // key_heads
    scale = size ** (-0.5)
    me = lax.axis_index("row")
    greet((("row", rows_of), ("col", cols_of), ("dp", members)))

    def row_exchange(kind, send, receive):
        return Exchange("row", rows_of, send, receive, row_send.at[kind], row_recv.at[kind])

    def stat_exchange(kind):
        return Ranked(
            "row",
            rows_of,
            lambda shift: stat_s.at[kind],
            stat_r.at[kind],
            stat_send.at[kind],
            stat_recv.at[kind],
        )

    stat1 = stat_exchange(0)

    def prepare(rows, start, tile):
        value = x[rows, :].astype(wide)
        square = jnp.broadcast_to(jnp.sum(value * value, axis=1, keepdims=True), (tile, lanes))
        stat_s[0, rows] = square
        stat_r[0, me, rows] = square
        unit[rows, :] = (value * gain1[...]).astype(low)

    each_tile(tokens, prepare)
    for shift in range(1, rows_of):
        stat1.start(shift)

    def project(index, target, slot):
        u = unit[...]
        q = dot(u, wq[:, window(index, qw)])
        k = dot(u, wk[:, window(index, kw)])
        v = dot(u, wv[:, window(index, kw)])
        kind = target.dtype
        if slot is None:
            target[:, :qw] = q.astype(kind)
            target[:, qw : qw + kw] = k.astype(kind)
            target[:, qw + kw :] = v.astype(kind)
        else:
            target[slot, :, :qw] = q.astype(kind)
            target[slot, :, qw : qw + kw] = k.astype(kind)
            target[slot, :, qw + kw :] = v.astype(kind)

    qkv = Reduce(
        rows_of,
        lambda index, slot: project(index, pq_s, slot),
        pq_s,
        pq_r,
        pq_x,
        sum_send.at[0],
        sum_recv.at[0],
    )
    qkv.start()
    project(me, pq_own, None)
    qkv.relay()

    need("ct")
    spread = Ranked("dp", members, lambda shift: ct, ct_all, ct_send, ct_recv)
    kept = pltpu.make_async_copy(ct, ct_all.at[spread.me], ct_store.at[0])
    kept.start()
    for shift in range(1, members):
        spread.start(shift)

    def tables(rows, start, tile):
        key = lax.broadcasted_iota(jnp.int32, (tile, tokens), 1)
        query = lax.broadcasted_iota(jnp.int32, (tile, tokens), 0) + start
        allowed = (seg_col[rows, :] == seg_row[...]) & (key <= query)
        count = jnp.sum(jnp.where(allowed, 1.0, 0.0), axis=1, keepdims=True) - 1.0
        angle = count * inverse[...]
        trig[0, rows, :] = jnp.cos(angle)
        trig[1, rows, :] = jnp.sin(angle)

    each_tile(tokens, tables)

    for shift in range(1, rows_of):
        stat1.arrive(shift)
    qkv.arrive()

    def heads_in(rows, start, tile):
        first = lax.rsqrt(stat1.total(rows) / width + epsilon)
        fs[rows, :] = first
        first = first[:, :1]
        n1[rows, :] = (x[rows, :].astype(wide) * first * gain1[...]).astype(low)
        value = pq_own[rows, :]
        for slot in range(qkv.count):
            value = value + pq_r[slot, rows, :].astype(wide)
        value = value * first
        raw[rows, :] = value[:, : qw + kw]
        cosine, sine = trig[0, rows, :], trig[1, rows, :]
        for head in range(heads + key_heads):
            piece = value[:, head * size : (head + 1) * size]
            gain = qn[...] if head < heads else kn[...]
            norm = lax.rsqrt(jnp.mean(piece * piece, axis=1, keepdims=True) + epsilon)
            normed = piece * norm * gain
            rotated = normed * cosine + half_turn(normed) * sine
            lows[rows, head * size : (head + 1) * size] = rotated.astype(low)
        lows[rows, qw + kw :] = value[:, qw + kw :].astype(low)

    each_tile(tokens, heads_in)

    def attend(rows, start, tile):
        key = lax.broadcasted_iota(jnp.int32, (tile, tokens), 1)
        query = lax.broadcasted_iota(jnp.int32, (tile, tokens), 0) + start
        allowed = (seg_col[rows, :] == seg_row[...]) & (key <= query)
        for head in range(heads):
            pair = head // group
            keys = lows[:, qw + pair * size : qw + (pair + 1) * size]
            values = lows[:, qw + kw + pair * size : qw + kw + (pair + 1) * size]
            scores = dot_t(lows[rows, head * size : (head + 1) * size], keys) * scale
            numerators = jnp.where(allowed, jnp.exp(scores), 0.0)
            share = numerators / jnp.sum(numerators, axis=1, keepdims=True)
            shares[head, rows, :] = share
            mixed[0, rows, head * size : (head + 1) * size] = dot(
                share.astype(low), values
            ).astype(low)

    each_tile(tokens, attend)

    gather = row_exchange(2, lambda shift: mixed.at[0], mixed_r)
    for shift in range(1, rows_of):
        gather.start(shift)
    need("wo")
    ox_s[...] = dot(mixed[0], wo[window(me, qw), :])
    for shift in range(1, rows_of):
        gather.arrive(shift)
        mixed[shift] = mixed_r[shift - 1]
        ox_s[...] += dot(mixed_r[shift - 1], wo[window(gather.source(shift), qw), :])
    column = Exchange("col", cols_of, lambda shift: ox_s, ox_r, col_send, col_recv)
    for shift in range(1, cols_of):
        column.start(shift)
    for shift in range(1, cols_of):
        column.arrive(shift)

    stat2 = stat_exchange(1)

    def middle(rows, start, tile):
        value = ox_s[rows, :]
        for shift in range(1, cols_of):
            value = value + ox_r[shift - 1, rows, :]
        value = x[rows, :].astype(wide) + value
        mid[rows, :] = value
        square = jnp.broadcast_to(jnp.sum(value * value, axis=1, keepdims=True), (tile, lanes))
        stat_s[1, rows] = square
        stat_r[1, me, rows] = square
        unit[rows, :] = (value * gain2[...]).astype(low)

    each_tile(tokens, middle)
    for shift in range(1, rows_of):
        stat2.start(shift)

    need("wg", "wu")
    def widen_out(index, slot):
        columns = window(index, fw)
        pg_s[slot, :, :fw] = dot(unit[...], wg[:, columns]).astype(low)
        pg_s[slot, :, fw:] = dot(unit[...], wu[:, columns]).astype(low)

    feed = Reduce(rows_of, widen_out, pg_s, pg_r, pg_x, sum_send.at[1], sum_recv.at[1])
    feed.start()
    pg_own[:, :fw] = dot(unit[...], wg[:, window(me, fw)])
    pg_own[:, fw:] = dot(unit[...], wu[:, window(me, fw)])
    for shift in range(1, rows_of):
        stat2.arrive(shift)

    def scale_rows(rows, start, tile):
        second = lax.rsqrt(stat2.total(rows) / width + epsilon)
        ss[rows, :] = second
        n2[rows, :] = (mid[rows, :] * second[:, :1] * gain2[...]).astype(low)

    each_tile(tokens, scale_rows)
    feed.relay()
    feed.arrive()

    def activate(rows, start, tile):
        second = ss[rows, :1]
        gate = pg_own[rows, :fw]
        upward = pg_own[rows, fw:]
        for slot in range(feed.count):
            gate = gate + pg_r[slot, rows, :fw].astype(wide)
            upward = upward + pg_r[slot, rows, fw:].astype(wide)
        gate = gate * second
        upward = upward * second
        sigmoid = jax.nn.sigmoid(gate)
        silu = gate * sigmoid
        hid[rows, :] = (silu * upward).astype(low)
        slope[rows, :fw] = upward * sigmoid * (1.0 + gate * (1.0 - sigmoid))
        slope[rows, fw:] = silu

    each_tile(tokens, activate)
    for shift in range(1, members):
        spread.arrive(shift)
    kept.wait()
    for exchange in (stat1, qkv, gather, column, stat2, feed, spread):
        exchange.finish()


def split(rows, columns):
    count = 1
    while rows % count or (rows // count) * columns > chunk_limit:
        count += 1
    return count


class Line:
    def __init__(self, members, out, near, far, spares, sems):
        self.members, self.out, self.near, self.far = members, out, near, far
        self.spares = spares
        self.in_send, self.near_sem, self.far_sem, self.out_send, self.store_sem, self.load_sem = sems
        me = lax.axis_index("dp")
        half = members // 2
        left = me < half
        place = jnp.where(left, half - 1 - me, me - half)
        self.inner = jnp.where(left, me + 1, me - 1)
        self.outer = jnp.where(left, jnp.maximum(me - 1, 0), jnp.minimum(me + 1, members - 1))
        self.is_mid = place == 0
        self.not_mid = place > 0
        self.has_outer = place < half - 1
        self.is_end = place == half - 1
        self.chunks, self.done = [], 0

    def view(self, refs, index):
        which, row, rows, column, columns = self.chunks[index]
        if not isinstance(row, int):
            row = pl.multiple_of(row, 16)
        if not isinstance(column, int):
            column = pl.multiple_of(column, lanes)
        return refs[which].at[pl.ds(row, rows), pl.ds(column, columns)]

    def inward(self, index, target, sem):
        return remote(
            self.view(self.out, index),
            self.view(target, index),
            self.in_send.at[index],
            sem.at[index],
            "dp",
            self.inner,
        )

    def outward(self, index):
        return remote(
            self.view(self.out, index),
            self.view(self.far, index),
            self.out_send.at[index],
            self.far_sem.at[index],
            "dp",
            self.outer,
        )

    def relay(self, index):
        return remote(
            self.view(self.far, index),
            self.view(self.far, index),
            self.out_send.at[index],
            self.far_sem.at[index],
            "dp",
            self.outer,
        )

    def send_in(self, index):
        @pl.when(self.is_mid)
        def _():
            self.inward(index, self.far, self.far_sem).start()

        @pl.when(self.not_mid)
        def _():
            self.inward(index, self.near, self.near_sem).start()

    def release(self, which, row, rows, column, columns):
        if self.members == 1:
            return
        count = split(rows, columns)
        for part in range(count):
            size = rows // count
            self.chunks.append((which, row + part * size, size, column, columns))
            index = len(self.chunks) - 1

            @pl.when(self.is_end)
            def _(index=index):
                self.send_in(index)

    def spare(self, index, kind):
        _, _, rows, _, columns = self.chunks[index]
        for ref in self.spares:
            if ref.shape[1:] == (rows, columns):
                return ref.at[kind]
        raise ValueError("no spare")

    def load(self, index, kind):
        source = self.view((self.near, self.far)[kind], index)
        return pltpu.make_async_copy(source, self.spare(index, kind), self.load_sem.at[kind])

    def add(self, index, kind):
        target, other = self.view(self.out, index), self.spare(index, kind)
        rows = other.shape[0]
        tile = 32 if rows % 32 == 0 else rows

        def step(part, carry):
            spot = pl.ds(pl.multiple_of(part * tile, 16), tile)
            target[spot, :] = (target[spot, :].astype(wide) + other[spot, :].astype(wide)).astype(low)
            return carry

        lax.fori_loop(0, rows // tile, step, 0)

    def begin_total(self, index):
        @pl.when(self.is_mid)
        def _():
            self.inward(index, self.far, self.far_sem).wait_recv()
            self.load(index, 1).start()

    def store(self, index):
        return pltpu.make_async_copy(
            self.view(self.out, index), self.view(self.far, index), self.store_sem.at[index]
        )

    def end_total(self, index):
        @pl.when(self.is_mid)
        def _():
            self.load(index, 1).wait()
            self.inward(index, self.far, self.far_sem).wait_send()
            self.add(index, 1)

            @pl.when(self.has_outer)
            def _():
                self.outward(index).start()

            self.store(index).start()

    def advance(self, count):
        if self.members == 1:
            return
        for _ in range(count):
            if self.done == len(self.chunks):
                return
            index = self.done
            self.done += 1

            @pl.when(self.has_outer)
            def _():
                self.inward(index, self.near, self.near_sem).wait_recv()
                self.load(index, 0).start()

            if index >= lag:
                self.begin_total(index - lag)

            @pl.when(self.has_outer)
            def _():
                self.load(index, 0).wait()
                self.add(index, 0)
                self.send_in(index)

            if index >= lag:
                self.end_total(index - lag)

    def settle(self):
        total = len(self.chunks)
        self.advance(total - self.done)
        for index in range(max(total - lag, 0), total):
            self.begin_total(index)
            self.end_total(index)

        @pl.when(self.not_mid)
        def _():
            for index in range(total):
                self.inward(index, self.far, self.far_sem).wait_recv()

                @pl.when(self.has_outer)
                def _():
                    self.relay(index).start()

            for index in range(total):
                self.inward(index, self.near, self.near_sem).wait_send()

                @pl.when(self.has_outer)
                def _():
                    self.relay(index).wait_send()

        @pl.when(self.is_mid)
        def _():
            for index in range(total):
                self.store(index).wait()

                @pl.when(self.has_outer)
                def _():
                    self.outward(index).wait_send()


class Chain:
    def __init__(self, members, own, blocks, send, receive, pass_send, pass_recv, row):
        self.members, self.own, self.blocks, self.row = members, own, blocks, row
        self.send, self.receive = send, receive
        self.pass_send, self.pass_recv = pass_send, pass_recv
        self.me = lax.axis_index("dp")

    def valid(self, place):
        return (place >= 0) & (place < self.members)

    def step(self, side, hop):
        way = 1 - 2 * side
        origin = self.me - way * (hop - 1)
        spot = self.blocks.at[origin, self.row.me]
        return remote(
            self.own if hop == 1 else spot,
            spot,
            self.send.at[side, hop - 1],
            self.receive.at[side, hop - 1],
            "dp",
            self.me + way,
        )

    def incoming(self, side, hop):
        origin = self.me - (1 - 2 * side) * hop
        spot = self.blocks.at[origin, self.row.me]
        return origin, remote(
            spot,
            spot,
            self.send.at[side, hop - 1],
            self.receive.at[side, hop - 1],
            "dp",
            self.me,
        )

    def sends(self, side, hop):
        way = 1 - 2 * side
        return self.valid(self.me - way * (hop - 1)) & self.valid(self.me + way)

    def hop(self, hop):
        for side in range(2):
            if hop > 1:
                self.await_block(side, hop - 1)

            @pl.when(self.sends(side, hop))
            def _(side=side):
                self.step(side, hop).start()

    def await_block(self, side, hop):
        @pl.when(self.valid(self.me - (1 - 2 * side) * hop))
        def _():
            self.incoming(side, hop)[1].wait_recv()

    def pass_on(self, side, hop, shift):
        origin = self.me - (1 - 2 * side) * hop
        spot = self.blocks.at[origin, self.row.me]
        return remote(
            spot,
            spot,
            self.pass_send.at[side, hop - 1, shift - 1],
            self.pass_recv.at[side, hop - 1, shift - 1],
            "row",
            self.row.target(shift),
        )

    def spread(self, hop):
        for side in range(2):
            if hop == self.members - 1:
                self.await_block(side, hop)

            @pl.when(self.valid(self.me - (1 - 2 * side) * hop))
            def _(side=side):
                for shift in range(1, self.row.size):
                    self.pass_on(side, hop, shift).start()

    def finish(self):
        for hop in range(1, self.members):
            for side in range(2):

                @pl.when(self.valid(self.me - (1 - 2 * side) * hop))
                def _(side=side, hop=hop):
                    for shift in range(1, self.row.size):
                        self.pass_on(side, hop, shift).wait_recv()
                        self.pass_on(side, hop, shift).wait_send()

                @pl.when(self.sends(side, hop))
                def _(side=side, hop=hop):
                    self.step(side, hop).wait_send()


def backward_kernel(
    rows_of,
    cols_of,
    members,
    need,
    x,
    ct,
    n1,
    fs,
    raw,
    lows,
    shares,
    trig,
    mixed,
    mid,
    ss,
    n2,
    hid,
    slope,
    gain1,
    gain2,
    qn,
    kn,
    wq,
    wk,
    wv,
    wo,
    wg,
    wu,
    wd,
    bo,
    ig,
    small,
    *rest,
):
    hid_all, *rest = rest
    far, near, rest = rest[:6], rest[6:12], rest[12:]
    grads, rest = rest[:6], rest[6:]
    gq, gk, gv, go, gg, gu = grads
    (
        gub,
        ph_s,
        ph_r,
        hid_r,
    gub_r,
    n_t,
    mb,
    ml,
    pm_own,
    pm_s,
    pm_r,
    sl,
    sb,
    dqkv,
    dqkv_r,
    gains,
    stat_s,
    stat_r,
    ox_s,
    ox_r,
    row_send,
    row_recv,
    stat_send,
    stat_recv,
        col_send,
        col_recv,
        small_r,
        small_send,
        small_recv,
        in_send,
        near_sem,
        far_sem,
        out_send,
        store_sem,
        load_sem,
        hop_send,
        hop_recv,
        pass_send,
        pass_recv,
        keep_sem,
        *spares,
    ) = rest
    tokens, depth = x.shape
    width = depth * rows_of
    qw, kw, fw = wq.shape[1] // rows_of, wk.shape[1] // rows_of, wg.shape[1] // rows_of
    size = qn.shape[1]
    heads, key_heads = qw // size, kw // size
    group = heads // key_heads
    scale = size ** (-0.5)
    me = lax.axis_index("row")
    greet((("row", rows_of), ("col", cols_of), ("dp", members)))
    line = Line(
        members,
        grads,
        near,
        far,
        spares,
        (in_send, near_sem, far_sem, out_send, store_sem, load_sem),
    )

    def row_exchange(kind, send, receive):
        return Exchange("row", rows_of, send, receive, row_send.at[kind], row_recv.at[kind])

    def stat_exchange(kind):
        return Ranked(
            "row",
            rows_of,
            lambda shift: stat_s.at[kind],
            stat_r.at[kind],
            stat_send.at[kind],
            stat_recv.at[kind],
        )

    def column_exchange(kind):
        return Exchange(
            "col",
            cols_of,
            lambda shift: ox_s.at[kind],
            ox_r.at[kind],
            col_send.at[kind],
            col_recv.at[kind],
        )

    def column_sum(kind, rows):
        value = ox_s[kind, rows, :]
        for shift in range(1, cols_of):
            value = value + ox_r[kind, shift - 1, rows, :]
        return value

    hide = row_exchange(0, lambda shift: hid, hid_r)
    gates = row_exchange(1, lambda shift: gub, gub_r)
    body = pl.ds(0, tokens)
    chain = Chain(members, hid, hid_all, hop_send, hop_recv, pass_send, pass_recv, hide)
    chain.hop(1)
    back = row_exchange(4, lambda shift: ph_s.at[shift - 1], ph_r)
    for shift in range(1, rows_of):
        ph_s[shift - 1] = dot_t(ct[...], wd[window(back.target(shift), fw), :]).astype(low)
        back.start(shift)
    stage = lax.axis_index("dp")

    def keep(shift):
        piece = hid if shift == 0 else hid_r.at[shift - 1]
        return pltpu.make_async_copy(
            piece, hid_all.at[stage, hide.source(shift)], keep_sem.at[shift]
        )

    keep(0).start()
    n_t[...] = n2[...].T
    need("slope")
    if members > 2:
        chain.hop(2)
    for shift in range(1, rows_of):
        back.arrive(shift)

    def behind(rows, start, tile):
        value = dot_t(ct[rows, :], wd[window(me, fw), :])
        for shift in range(1, rows_of):
            value = value + ph_r[shift - 1, rows, :].astype(wide)
        gub[rows, :fw] = (value * slope[rows, :fw]).astype(low)
        gub[rows, fw:] = (value * slope[rows, fw:]).astype(low)

    each_tile(tokens, behind)
    for shift in range(1, rows_of):
        gates.start(shift)
    for step in range(3, members):
        chain.hop(step)
    need("wg", "wu")
    for shift in range(rows_of):
        if shift:
            line.advance(pace * (1 if shift == 1 else 2))
            gates.arrive(shift)
        piece = gub if shift == 0 else gub_r.at[shift - 1]
        index = window(gates.source(shift), fw)
        part = dot_t(piece[:, :fw], wg[:, index]) + dot_t(piece[:, fw:], wu[:, index])
        if shift == 0:
            ox_s[1, body, :] = part
        else:
            ox_s[1, body, :] += part
        gg[:, index] = dot(n_t[...], piece[:, :fw]).astype(low)
        line.release(4, 0, depth, gates.source(shift) * fw, fw)
        gu[:, index] = dot(n_t[...], piece[:, fw:]).astype(low)
        line.release(5, 0, depth, gates.source(shift) * fw, fw)
    column1 = column_exchange(1)
    for shift in range(1, cols_of):
        column1.start(shift)
    line.advance(1 * pace)
    for shift in range(1, cols_of):
        column1.arrive(shift)

    stat2 = stat_exchange(0)
    small[...] = jnp.zeros_like(small)
    gains[...] = jnp.zeros_like(gains)

    def feed_stat(rows, start, tile):
        back = column_sum(1, rows)
        unit = mid[rows, :] * ss[rows, :1]
        small[1:2, :] += jnp.sum(back * unit, axis=0, keepdims=True)
        inner = jnp.sum(back * gain2[...] * unit, axis=1, keepdims=True)
        inner = jnp.broadcast_to(inner, (tile, lanes))
        stat_s[0, rows] = inner
        stat_r[0, me, rows] = inner

    each_tile(tokens, feed_stat)
    pad = pl.ds(tokens, 8)
    stat_s[0, pad] = jnp.zeros((8, lanes), wide)
    for shift in range(1, rows_of):
        stat2.start(shift)
    need("wo", "mixed", "lows", "shares")
    line.advance(1 * pace)
    for shift in range(1, rows_of):
        stat2.arrive(shift)

    def middle_back(rows, start, tile):
        second = ss[rows, :1]
        unit = mid[rows, :] * second
        inner = stat2.total(rows)[:, :1] / width
        value = ct[rows, :].astype(wide) + second * (
            column_sum(1, rows) * gain2[...] - unit * inner
        )
        mb[rows, :] = value
        ml[rows, :] = value.astype(low)

    each_tile(tokens, middle_back)
    blend = row_exchange(2, lambda shift: pm_s.at[shift - 1], pm_r)
    for shift in range(1, rows_of):
        pm_s[shift - 1] = dot_t(ml[...], wo[window(blend.target(shift), qw), :]).astype(low)
        blend.start(shift)
    pm_own[...] = dot_t(ml[...], wo[window(me, qw), :])
    for shift in range(rows_of):
        index = window(blend.source(shift), qw)
        go[index, :] = t_dot(mixed[shift], ml[...]).astype(low)
        line.release(3, blend.source(shift) * qw, qw, 0, depth)
    line.advance(2 * pace)
    for shift in range(1, rows_of):
        blend.arrive(shift)

    def share_back(rows, start, tile):
        value = pm_own[rows, :]
        for shift in range(1, rows_of):
            value = value + pm_r[shift - 1, rows, :].astype(wide)
        incoming = value.astype(low)
        pm_s[0, rows, :] = incoming
        product = incoming.astype(wide) * mixed[0, rows, :].astype(wide)
        for head in range(heads):
            pair = head // group
            part = slice(head * size, (head + 1) * size)
            values = lows[:, qw + kw + pair * size : qw + kw + (pair + 1) * size]
            delta = jnp.sum(product[:, part], axis=1, keepdims=True)
            share = shares[head, rows, :]
            sl[head, rows, :] = share.astype(low)
            sb[head, rows, :] = (share * (dot_t(incoming[:, part], values) - delta)).astype(low)

    blend.finish()
    each_tile(tokens, share_back)
    need("n1", "raw", "trig")
    n_t[...] = n1[...].T
    line.advance(1 * pace)

    def pull(head, back, gain, row):
        raw_piece = raw[:, head * size : (head + 1) * size]
        norm = lax.rsqrt(jnp.mean(raw_piece * raw_piece, axis=1, keepdims=True) + epsilon)
        unit = raw_piece * norm
        normed_back = back * trig[0] - half_turn(back * trig[1])
        gains[row : row + 1, :] += jnp.sum(normed_back * unit, axis=0, keepdims=True)
        unit_back = normed_back * gain
        return norm * (unit_back - unit * jnp.mean(unit_back * unit, axis=1, keepdims=True))

    for pair in range(key_heads):
        keys = lows[:, qw + pair * size : qw + (pair + 1) * size]
        key_back = jnp.zeros((tokens, size), wide)
        value_back = jnp.zeros((tokens, size), wide)
        for head in range(pair * group, (pair + 1) * group):
            part = slice(head * size, (head + 1) * size)
            value_back = value_back + t_dot(sl[head], pm_s[0, :, part])
            key_back = key_back + scale * t_dot(sb[head], lows[:, part])
            query_back = scale * dot(sb[head], keys)
            dqkv[:, part] = pull(head, query_back, qn[...], 0).astype(low)
        spot = qw + pair * size
        dqkv[:, spot : spot + size] = pull(heads + pair, key_back, kn[...], 1).astype(low)
        spot = qw + kw + pair * size
        dqkv[:, spot : spot + size] = value_back.astype(low)

    deliver = row_exchange(3, lambda shift: dqkv, dqkv_r)
    for shift in range(1, rows_of):
        deliver.start(shift)
    for shift in range(1, rows_of):
        hide.start(shift)
    if members > 1:
        chain.spread(1)
    need("wq", "wk", "wv")
    for shift in range(rows_of):
        if shift:
            line.advance(1 * pace)
            deliver.arrive(shift)
        piece = dqkv if shift == 0 else dqkv_r.at[shift - 1]
        source = deliver.source(shift)
        part = dot_t(piece[:, :qw], wq[:, window(source, qw)])
        part = part + dot_t(piece[:, qw : qw + kw], wk[:, window(source, kw)])
        part = part + dot_t(piece[:, qw + kw :], wv[:, window(source, kw)])
        if shift == 0:
            ox_s[2, body, :] = part
        else:
            ox_s[2, body, :] += part
    ox_s[2, pad, :] = jnp.zeros((8, depth), wide)
    ox_s[2, pad, :lanes] = gains[...]
    column2 = column_exchange(2)
    for shift in range(1, cols_of):
        column2.start(shift)
    for shift in range(rows_of):
        piece = dqkv if shift == 0 else dqkv_r.at[shift - 1]
        source = deliver.source(shift)
        gq[:, window(source, qw)] = dot(n_t[...], piece[:, :qw]).astype(low)
        gk[:, window(source, kw)] = dot(n_t[...], piece[:, qw : qw + kw]).astype(low)
        gv[:, window(source, kw)] = dot(n_t[...], piece[:, qw + kw :]).astype(low)
    line.release(0, 0, depth, 0, qw * rows_of)
    line.release(1, 0, depth, 0, kw * rows_of)
    line.release(2, 0, depth, 0, kw * rows_of)
    line.advance(1 * pace)
    for shift in range(1, cols_of):
        column2.arrive(shift)
    need("x", "fs")

    stat1 = stat_exchange(1)

    def first_stat(rows, start, tile):
        back = column_sum(2, rows)
        unit = x[rows, :].astype(wide) * fs[rows, :1]
        small[0:1, :] += jnp.sum(back * unit, axis=0, keepdims=True)
        inner = jnp.sum(back * gain1[...] * unit, axis=1, keepdims=True)
        inner = jnp.broadcast_to(inner, (tile, lanes))
        stat_s[1, rows] = inner
        stat_r[1, me, rows] = inner

    each_tile(tokens, first_stat)
    summed = column_sum(2, pad)[:, :lanes]
    stat_s[1, pad] = summed
    stat_r[1, me, pad] = summed
    for shift in range(1, rows_of):
        stat1.start(shift)
    for step in range(2, members):
        chain.spread(step)
    line.advance(bulk * pace)
    for shift in range(rows_of):
        if shift:
            hide.arrive(shift)
            keep(shift).start()
        piece = hid[...] if shift == 0 else hid_r[shift - 1]
        part = dot(piece, wd[window(hide.source(shift), fw), :])
        if shift == 0:
            ox_s[0, body, :] = part
        else:
            ox_s[0, body, :] += part
    column0 = column_exchange(0)
    for shift in range(1, cols_of):
        column0.start(shift)
    for shift in range(1, cols_of):
        column0.arrive(shift)

    def result(rows, start, tile):
        bo[rows, :] = (mid[rows, :] + column_sum(0, rows)).astype(low)

    each_tile(tokens, result)
    line.advance(slots_left)
    for shift in range(1, rows_of):
        stat1.arrive(shift)

    def finish(rows, start, tile):
        first = fs[rows, :1]
        unit = x[rows, :].astype(wide) * first
        inner = stat1.total(rows)[:, :1] / width
        ig[rows, :] = mb[rows, :] + first * (column_sum(2, rows) * gain1[...] - unit * inner)

    each_tile(tokens, finish)
    small[8:16, :lanes] = stat1.total(pad)
    ranked = Ranked("dp", members, lambda shift: small, small_r, small_send, small_recv)
    if members > 1:
        small_r[lax.axis_index("dp")] = small[...]
        for shift in range(1, members):
            ranked.start(shift)
    if members > 1:
        line.settle()
        for shift in range(1, members):
            ranked.arrive(shift)
        ranked.finish()
        summed = small_r[0]
        for member in range(1, members):
            summed = summed + small_r[member]
        small[...] = summed
    chain.finish()
    for shift in range(rows_of):
        keep(shift).wait()
    for exchange in (hide, back, gates, column0, column1, stat2, deliver, column2, stat1):
        exchange.finish()


def widen_kernel(*refs):
    count = (len(refs) - 3) // 2
    hid_all, ct_all = refs[count : count + 2]
    *out, gd = refs[count + 2 :]
    for source, target in zip(refs[:count], out):
        target[...] = source[...].astype(target.dtype)
    total = t_dot(hid_all[0, 0], ct_all[0])
    for member in range(1, ct_all.shape[0]):
        total = total + t_dot(hid_all[member, 0], ct_all[member])
    gd[...] = total


def widen(arrays, kinds, hid_all, ct_all, shape):
    members, rows_of, tokens, fw = hid_all.shape
    parts = 2 if fw % (2 * lanes) == 0 else 1
    steps = rows_of * parts

    def rows(array_shape):
        return pl.BlockSpec((array_shape[0] // steps, array_shape[1]), lambda i: (i, 0))

    specs = [rows(array.shape) for array in arrays]
    shapes = [array.shape for array in arrays] + [shape]
    return pl.pallas_call(
        widen_kernel,
        grid=(steps,),
        out_shape=tuple(map(jax.ShapeDtypeStruct, shapes, kinds)),
        in_specs=specs
        + [
            pl.BlockSpec(
                (members, 1, tokens, fw // parts), lambda i: (0, i // parts, 0, i % parts)
            ),
            pl.BlockSpec(ct_all.shape, lambda i: (0, 0, 0)),
        ],
        out_specs=tuple(specs + [rows(shape)]),
        compiler_params=pltpu.CompilerParams(vmem_limit_bytes=full_vmem),
    )(*arrays, hid_all, ct_all)


def vmem(shape, kind):
    return pltpu.VMEM(shape, kind)


def call(kernel, shapes, scratch, identity, arguments, late=(), outside=()):
    inside, away = pl.BlockSpec(memory_space=pltpu.VMEM), pl.BlockSpec(memory_space=pl.ANY)
    names = list(arguments)
    late = [name for name in names if name in late]

    def body(*refs):
        given = dict(zip(names, refs))
        rest = refs[len(names) :]
        copies = {}
        if late:
            holders, sem = rest[-len(late) - 1 : -1], rest[-1]
            rest = rest[: -len(late) - 1]
            for index, name in enumerate(late):
                copies[name] = pltpu.make_async_copy(given[name], holders[index], sem.at[index])
                copies[name].start()
                given[name] = holders[index]

        def need(*wanted):
            for name in wanted:
                copy = copies.pop(name, None)
                if copy is not None:
                    copy.wait()

        kernel(need, *given.values(), *rest)
        need(*list(copies))

    extra = []
    if late:
        extra = [vmem(arguments[name].shape, arguments[name].dtype) for name in late]
        extra.append(pltpu.SemaphoreType.DMA((len(late),)))
    return pl.pallas_call(
        body,
        out_shape=tuple(jax.ShapeDtypeStruct(shape, kind) for shape, kind in shapes),
        in_specs=[away if name in late else inside for name in names],
        out_specs=tuple(away if index in outside else inside for index in range(len(shapes))),
        scratch_shapes=scratch + extra,
        compiler_params=pltpu.CompilerParams(
            collective_id=identity, has_side_effects=True, vmem_limit_bytes=full_vmem
        ),
    )(*arguments.values())


def per_device(
    block_input,
    segments,
    attention_norm,
    query_weight,
    key_weight,
    value_weight,
    query_norm,
    key_norm,
    output_weight,
    feedforward_norm,
    gate_weight,
    up_weight,
    down_weight,
    cotangent,
):
    rows_of, cols_of, members = (lax.axis_size(name) for name in ("row", "col", "dp"))
    tokens, depth = block_input.shape
    size = query_norm.shape[0]
    qw, kw, fw = (
        weight.shape[1] // rows_of for weight in (query_weight, key_weight, gate_weight)
    )
    heads = qw // size
    others, beside = max(rows_of - 1, 1), max(cols_of - 1, 1)
    half = size // 2
    inverse = rope_base ** (-2.0 * jnp.arange(half, dtype=wide) / size)
    inverse = jnp.concatenate([inverse, inverse])[None, :]
    seg_row = segments.reshape(1, tokens)
    seg_col = segments.reshape(tokens, 1)
    gain1, gain2 = attention_norm[None, :], feedforward_norm[None, :]
    qn, kn = query_norm[None, :], key_norm[None, :]
    total = qw + 2 * kw
    peers = max(members - 1, 1)
    dma = pltpu.SemaphoreType.DMA

    def sems(kinds):
        return [
            dma((5, others)),
            dma((5, others)),
            dma((2, others)),
            dma((2, others)),
            dma((kinds, beside)) if kinds > 1 else dma((beside,)),
            dma((kinds, beside)) if kinds > 1 else dma((beside,)),
        ]

    saved = call(
        partial(forward_kernel, rows_of, cols_of, members),
        (
            ((tokens, depth), low),
            ((tokens, lanes), wide),
            ((tokens, qw + kw), wide),
            ((tokens, total), low),
            ((heads, tokens, tokens), wide),
            ((2, tokens, size), wide),
            ((rows_of, tokens, qw), low),
            ((tokens, depth), wide),
            ((tokens, lanes), wide),
            ((tokens, depth), low),
            ((tokens, fw), low),
            ((tokens, 2 * fw), wide),
            ((members, tokens, depth), low),
        ),
        [
            vmem((tokens, depth), low),
            vmem((tokens, total), wide),
            vmem((others, tokens, total), low),
            vmem((others, tokens, total), low),
            vmem((2, tokens // 2, total), low),
            vmem((tokens, 2 * fw), wide),
            vmem((others, tokens, 2 * fw), low),
            vmem((others, tokens, 2 * fw), low),
            vmem((2, tokens // 2, 2 * fw), low),
            vmem((others, tokens, qw), low),
            vmem((2, tokens, lanes), wide),
            vmem((2, rows_of, tokens, lanes), wide),
            vmem((tokens, depth), wide),
            vmem((beside, tokens, depth), wide),
        ]
        + sems(1)
        + [dma((peers,)), dma((peers,)), dma((1,))]
        + [dma((2, max(6, others)))] * 2,
        0,
        dict(
            x=block_input,
            seg_row=seg_row,
            seg_col=seg_col,
            inverse=inverse,
            gain1=gain1,
            wq=query_weight,
            wk=key_weight,
            wv=value_weight,
            qn=qn,
            kn=kn,
            wo=output_weight,
            gain2=gain2,
            wg=gate_weight,
            wu=up_weight,
            ct=cotangent,
        ),
        late=("wo", "wg", "wu", "ct"),
        outside=(12,),
    )
    *saved, ct_all = saved
    saved = dict(
        zip(("n1", "fs", "raw", "lows", "shares", "trig", "mixed", "mid", "ss", "n2", "hid", "slope"), saved)
    )
    weights = (query_weight, key_weight, value_weight, output_weight, gate_weight, up_weight)
    shapes = [weight.shape for weight in weights]
    pieces = {
        (depth, fw): 2 * rows_of,
        (qw, depth): rows_of,
        (depth, qw * rows_of): 1,
        (depth, kw * rows_of): 2,
    }
    slots = sum(split(*shape) * times for shape, times in pieces.items())
    spares = {(shape[0] // split(*shape), shape[1]) for shape in pieces}
    done = call(
        partial(backward_kernel, rows_of, cols_of, members),
        (
            ((tokens, depth), low),
            ((tokens, depth), wide),
            ((16, depth), wide),
            ((members, rows_of, tokens, fw), low),
            *((shape, low) for shape in shapes * 2),
        ),
        [vmem(shape, low) for shape in shapes]
        + [
            vmem((tokens, 2 * fw), low),
            vmem((others, tokens, fw), low),
            vmem((others, tokens, fw), low),
            vmem((others, tokens, fw), low),
            vmem((others, tokens, 2 * fw), low),
            vmem((depth, tokens), low),
            vmem((tokens, depth), wide),
            vmem((tokens, depth), low),
            vmem((tokens, qw), wide),
            vmem((others, tokens, qw), low),
            vmem((others, tokens, qw), low),
            vmem((heads, tokens, tokens), low),
            vmem((heads, tokens, tokens), low),
            vmem((tokens, total), low),
            vmem((others, tokens, total), low),
            vmem((8, lanes), wide),
            vmem((2, tokens + 8, lanes), wide),
            vmem((2, rows_of, tokens + 8, lanes), wide),
            vmem((3, tokens + 8, depth), wide),
            vmem((3, beside, tokens + 8, depth), wide),
        ]
        + sems(3)
        + [vmem((members, 16, depth), wide), dma((peers,)), dma((peers,))]
        + [dma((slots,))] * 5
        + [dma((2,))]
        + [dma((2, peers))] * 2
        + [dma((2, peers, others))] * 2
        + [dma((rows_of,))]
        + [vmem((2, *shape), low) for shape in sorted(spares)],
        1,
        dict(
            x=block_input,
            ct=cotangent,
            **saved,
            gain1=gain1,
            gain2=gain2,
            qn=qn,
            kn=kn,
            wq=query_weight,
            wk=key_weight,
            wv=value_weight,
            wo=output_weight,
            wg=gate_weight,
            wu=up_weight,
            wd=down_weight,
        ),
        late=("x", "n1", "fs", "raw", "lows", "shares", "trig", "mixed", "slope", "wq", "wk", "wv", "wo", "wg", "wu"),
        outside=range(3, 16),
    )
    block_output, input_gradient, small, hid_all, *partials = done[:10]
    block_output, input_gradient, gq, gk, gv, go, gg, gu, gd = widen(
        (block_output, input_gradient, *partials),
        [low] + [wide] * 8,
        hid_all,
        ct_all,
        down_weight.shape,
    )
    return (
        block_output,
        input_gradient,
        small[0],
        gq,
        gk,
        gv,
        small[8, :size],
        small[9, :size],
        go,
        small[1],
        gg,
        gu,
        gd,
    )


def solution(mesh):
    return jax.shard_map(
        per_device,
        mesh=mesh,
        in_specs=(
            P("dp", "row"),
            P("dp", None),
            P("row"),
            P("row", "col"),
            P("row", "col"),
            P("row", "col"),
            P(),
            P(),
            P("col", "row"),
            P("row"),
            P("row", "col"),
            P("row", "col"),
            P("col", "row"),
            P("dp", "row"),
        ),
        out_specs=(
            P("dp", "row"),
            P("dp", "row"),
            P("row"),
            P("row", "col"),
            P("row", "col"),
            P("row", "col"),
            P(),
            P(),
            P("col", "row"),
            P("row"),
            P("row", "col"),
            P("row", "col"),
            P("col", "row"),
        ),
        check_vma=False,
    )
```

```python
from functools import partial

import jax
import jax.numpy as jnp
import numpy as np
from jax import lax
from jax.experimental import pallas as pl
from jax.experimental.pallas import tpu as pltpu
from jax.sharding import PartitionSpec as P

epsilon = 1e-06
rope_base = 1000000.0
lanes = 128
full_vmem = 67043328
chunk_limit = 131072
lag = 3
pace = 2
bulk = 6
slots_left = 1000
low = jnp.bfloat16
wide = jnp.float32


def dot(a, b, contract=((1,), (0,))):
    return lax.dot_general(a, b, (contract, ((), ())), preferred_element_type=wide)


def dot_t(a, b):
    return dot(a, b, ((1,), (1,)))


def t_dot(a, b):
    return dot(a, b, ((0,), (0,)))


def window(index, size):
    return pl.ds(pl.multiple_of(index * size, lanes), size)


def remote(source, target, send, receive, axis, index):
    return pltpu.make_async_remote_copy(
        src_ref=source,
        dst_ref=target,
        send_sem=send,
        recv_sem=receive,
        device_id={axis: index},
        device_id_type=pl.DeviceIdType.MESH,
    )


def greet(groups):
    barrier = pltpu.get_barrier_semaphore()
    total = 0
    for axis, size in groups:
        me = lax.axis_index(axis)
        for shift in range(1, size):
            pl.semaphore_signal(
                barrier,
                inc=1,
                device_id={axis: lax.rem(me + shift, size)},
                device_id_type=pl.DeviceIdType.MESH,
            )
            total += 1
    if total:
        pl.semaphore_wait(barrier, total)


def half_turn(values):
    size = values.shape[-1]
    turned = pltpu.roll(values, size // 2, axis=1)
    lane = lax.broadcasted_iota(jnp.int32, values.shape, 1)
    return jnp.where(lane < size // 2, -turned, turned)


class Exchange:
    def __init__(self, axis, size, send, receive, send_sem, receive_sem):
        self.axis, self.size = axis, size
        self.send, self.receive = send, receive
        self.send_sem, self.receive_sem = send_sem, receive_sem
        self.me = lax.axis_index(axis)

    def target(self, shift):
        return lax.rem(self.me + shift, self.size)

    def source(self, shift):
        return lax.rem(self.me + self.size - shift, self.size)

    def copy(self, shift):
        sent = self.send(shift)
        return remote(
            sent,
            self.receive.at[shift - 1],
            self.send_sem.at[shift - 1],
            self.receive_sem.at[shift - 1],
            self.axis,
            self.target(shift),
        )

    def start(self, shift):
        self.copy(shift).start()

    def arrive(self, shift):
        self.copy(shift).wait_recv()

    def finish(self):
        for shift in range(1, self.size):
            self.copy(shift).wait_send()


class Ranked(Exchange):
    def copy(self, shift):
        return remote(
            self.send(shift),
            self.receive.at[self.me],
            self.send_sem.at[shift - 1],
            self.receive_sem.at[shift - 1],
            self.axis,
            self.target(shift),
        )

    def total(self, rows):
        result = self.receive[0, rows]
        for member in range(1, self.size):
            result = result + self.receive[member, rows]
        return result


class Reduce:
    def __init__(self, size, produce, send, receive, extra, send_sem, receive_sem):
        self.size, self.produce = size, produce
        self.send, self.receive, self.extra = send, receive, extra
        self.send_sem, self.receive_sem = send_sem, receive_sem
        self.halved = size == 4
        self.count = 2 if self.halved else size - 1
        me = lax.axis_index("row")
        if self.halved:
            self.half = send.shape[1] // 2
            beside = me + 1 - 2 * lax.rem(me, 2)
            across = lax.rem(me + 2, 4)
            self.members = (beside, across, lax.rem(beside + 2, 4))
        else:
            self.direct = Exchange(
                "row", size, lambda shift: send.at[shift - 1], receive, send_sem, receive_sem
            )

    def rows(self, part):
        return pl.ds(part * self.half, self.half)

    def copy(self, kind):
        slot, part, to = ((2, 0, 0), (2, 1, 1), (0, 0, 0), (1, 1, 1), (0, 1, 0), (1, 0, 1))[kind]
        source = self.send.at[slot, self.rows(part)]
        target = self.extra.at[to] if slot == 2 else self.receive.at[slot, self.rows(part)]
        return remote(
            source,
            target,
            self.send_sem.at[kind],
            self.receive_sem.at[kind],
            "row",
            self.members[to],
        )

    def start(self):
        if not self.halved:
            for shift in range(1, self.size):
                self.produce(self.direct.target(shift), shift - 1)
                self.direct.start(shift)
            return
        self.produce(self.members[2], 2)
        self.copy(0).start()
        self.copy(1).start()
        self.produce(self.members[0], 0)
        self.copy(2).start()
        self.produce(self.members[1], 1)
        self.copy(3).start()

    def relay(self):
        if not self.halved:
            return
        for kind, slot in ((0, 1), (1, 0)):
            self.copy(kind).wait_recv()
            tile = 32 if self.half % 32 == 0 else self.half

            def step(index, carry, kind=kind, slot=slot, tile=tile):
                spot = pl.ds(pl.multiple_of(index * tile, 16), tile)
                rows = pl.ds(pl.multiple_of(kind * self.half + index * tile, 16), tile)
                total = self.send[slot, rows, :].astype(wide) + self.extra[kind, spot, :].astype(
                    wide
                )
                self.send[slot, rows, :] = total.astype(low)
                return carry

            lax.fori_loop(0, self.half // tile, step, 0)
            self.copy(5 - kind).start()

    def arrive(self):
        if not self.halved:
            for shift in range(1, self.size):
                self.direct.arrive(shift)
            return
        for kind in range(2, 6):
            self.copy(kind).wait_recv()

    def finish(self):
        if not self.halved:
            self.direct.finish()
            return
        for kind in range(6):
            self.copy(kind).wait_send()


def each_tile(rows, body):
    tile = lanes if rows % lanes == 0 else rows

    def step(index, carry):
        body(pl.ds(pl.multiple_of(index * tile, tile), tile), index * tile, tile)
        return carry

    lax.fori_loop(0, rows // tile, step, 0)


def forward_kernel(
    rows_of,
    cols_of,
    members,
    need,
    x,
    seg_row,
    inverse,
    gain1,
    wq,
    wk,
    wv,
    qn,
    kn,
    wo,
    gain2,
    wg,
    wu,
    ct,
    wd,
    n1,
    fs,
    raw,
    lows,
    shares,
    trig,
    mixed,
    mid,
    ss,
    n2,
    hid,
    gub,
    ct_all,
    seg_col,
    unit,
    pq_own,
    pq_s,
    pq_r,
    pq_x,
    ph_own,
    ph_s,
    ph_r,
    ph_x,
    pg_own,
    pg_s,
    pg_r,
    pg_x,
    mixed_r,
    stat_s,
    stat_r,
    ox_s,
    ox_r,
    row_send,
    row_recv,
    stat_send,
    stat_recv,
    col_send,
    col_recv,
    ct_send,
    ct_recv,
    ct_store,
    sum_send,
    sum_recv,
):
    tokens, depth = x.shape
    width = depth * rows_of
    qw, kw, fw = wq.shape[1] // rows_of, wk.shape[1] // rows_of, wg.shape[1] // rows_of
    size = qn.shape[1]
    heads, key_heads = qw // size, kw // size
    group = heads // key_heads
    scale = size ** (-0.5)
    me = lax.axis_index("row")
    greet((("row", rows_of), ("col", cols_of), ("dp", members)))

    def row_exchange(kind, send, receive):
        return Exchange("row", rows_of, send, receive, row_send.at[kind], row_recv.at[kind])

    def stat_exchange(kind):
        return Ranked(
            "row",
            rows_of,
            lambda shift: stat_s.at[kind],
            stat_r.at[kind],
            stat_send.at[kind],
            stat_recv.at[kind],
        )

    stat1 = stat_exchange(0)

    def prepare(rows, start, tile):
        value = x[rows, :].astype(wide)
        square = jnp.broadcast_to(jnp.sum(value * value, axis=1, keepdims=True), (tile, lanes))
        stat_s[0, rows] = square
        stat_r[0, me, rows] = square
        unit[rows, :] = (value * gain1[...]).astype(low)

    each_tile(tokens, prepare)
    for shift in range(1, rows_of):
        stat1.start(shift)

    def project(index, target, slot):
        u = unit[...]
        q = dot(u, wq[:, window(index, qw)])
        k = dot(u, wk[:, window(index, kw)])
        v = dot(u, wv[:, window(index, kw)])
        kind = target.dtype
        if slot is None:
            target[:, :qw] = q.astype(kind)
            target[:, qw : qw + kw] = k.astype(kind)
            target[:, qw + kw :] = v.astype(kind)
        else:
            target[slot, :, :qw] = q.astype(kind)
            target[slot, :, qw : qw + kw] = k.astype(kind)
            target[slot, :, qw + kw :] = v.astype(kind)

    qkv = Reduce(
        rows_of,
        lambda index, slot: project(index, pq_s, slot),
        pq_s,
        pq_r,
        pq_x,
        sum_send.at[0],
        sum_recv.at[0],
    )
    qkv.start()
    project(me, pq_own, None)
    qkv.relay()
    need("ct", "wd")

    def behind_out(index, slot):
        ph_s[slot] = dot_t(ct[...], wd[window(index, fw), :]).astype(low)

    back = Reduce(rows_of, behind_out, ph_s, ph_r, ph_x, sum_send.at[2], sum_recv.at[2])
    back.start()
    ph_own[...] = dot_t(ct[...], wd[window(me, fw), :])
    spread = Ranked("dp", members, lambda shift: ct, ct_all, ct_send, ct_recv)
    kept = pltpu.make_async_copy(ct, ct_all.at[spread.me], ct_store.at[0])
    kept.start()
    for shift in range(1, members):
        spread.start(shift)

    line = seg_row[...].astype(wide)
    seg_col[...] = jnp.broadcast_to(line, (lanes, tokens)).T

    def tables(rows, start, tile):
        key = lax.broadcasted_iota(jnp.int32, (tile, tokens), 1)
        query = lax.broadcasted_iota(jnp.int32, (tile, tokens), 0) + start
        allowed = (seg_col[rows, :1] == seg_row[...].astype(wide)) & (key <= query)
        count = jnp.sum(jnp.where(allowed, 1.0, 0.0), axis=1, keepdims=True) - 1.0
        angle = count * inverse[...]
        trig[0, rows, :] = jnp.cos(angle)
        trig[1, rows, :] = jnp.sin(angle)

    each_tile(tokens, tables)

    for shift in range(1, rows_of):
        stat1.arrive(shift)
    qkv.arrive()

    def heads_in(rows, start, tile):
        first = lax.rsqrt(stat1.total(rows) / width + epsilon)
        fs[rows, :] = first
        first = first[:, :1]
        n1[rows, :] = (x[rows, :].astype(wide) * first * gain1[...]).astype(low)
        value = pq_own[rows, :]
        for slot in range(qkv.count):
            value = value + pq_r[slot, rows, :].astype(wide)
        value = value * first
        raw[rows, :] = value[:, : qw + kw]
        cosine, sine = trig[0, rows, :], trig[1, rows, :]
        for head in range(heads + key_heads):
            piece = value[:, head * size : (head + 1) * size]
            gain = qn[...] if head < heads else kn[...]
            norm = lax.rsqrt(jnp.mean(piece * piece, axis=1, keepdims=True) + epsilon)
            normed = piece * norm * gain
            rotated = normed * cosine + half_turn(normed) * sine
            lows[rows, head * size : (head + 1) * size] = rotated.astype(low)
        lows[rows, qw + kw :] = value[:, qw + kw :].astype(low)

    each_tile(tokens, heads_in)

    def attend(rows, start, tile):
        key = lax.broadcasted_iota(jnp.int32, (tile, tokens), 1)
        query = lax.broadcasted_iota(jnp.int32, (tile, tokens), 0) + start
        allowed = (seg_col[rows, :1] == seg_row[...].astype(wide)) & (key <= query)
        for head in range(heads):
            pair = head // group
            keys = lows[:, qw + pair * size : qw + (pair + 1) * size]
            values = lows[:, qw + kw + pair * size : qw + kw + (pair + 1) * size]
            scores = dot_t(lows[rows, head * size : (head + 1) * size], keys) * scale
            numerators = jnp.where(allowed, jnp.exp(scores), 0.0)
            share = numerators / jnp.sum(numerators, axis=1, keepdims=True)
            shares[head, rows, :] = share
            mixed[0, rows, head * size : (head + 1) * size] = dot(
                share.astype(low), values
            ).astype(low)

    each_tile(tokens, attend)

    gather = row_exchange(2, lambda shift: mixed.at[0], mixed_r)
    for shift in range(1, rows_of):
        gather.start(shift)
    need("wo")
    ox_s[...] = dot(mixed[0], wo[window(me, qw), :])
    back.relay()
    for shift in range(1, rows_of):
        gather.arrive(shift)
        mixed[shift] = mixed_r[shift - 1]
        ox_s[...] += dot(mixed_r[shift - 1], wo[window(gather.source(shift), qw), :])
    column = Exchange("col", cols_of, lambda shift: ox_s, ox_r, col_send, col_recv)
    for shift in range(1, cols_of):
        column.start(shift)
    for shift in range(1, cols_of):
        column.arrive(shift)

    stat2 = stat_exchange(1)

    def middle(rows, start, tile):
        value = ox_s[rows, :]
        for shift in range(1, cols_of):
            value = value + ox_r[shift - 1, rows, :]
        value = x[rows, :].astype(wide) + value
        mid[rows, :] = value
        square = jnp.broadcast_to(jnp.sum(value * value, axis=1, keepdims=True), (tile, lanes))
        stat_s[1, rows] = square
        stat_r[1, me, rows] = square
        unit[rows, :] = (value * gain2[...]).astype(low)

    each_tile(tokens, middle)
    for shift in range(1, rows_of):
        stat2.start(shift)

    need("wg", "wu")
    def widen_out(index, slot):
        columns = window(index, fw)
        pg_s[slot, :, :fw] = dot(unit[...], wg[:, columns]).astype(low)
        pg_s[slot, :, fw:] = dot(unit[...], wu[:, columns]).astype(low)

    feed = Reduce(rows_of, widen_out, pg_s, pg_r, pg_x, sum_send.at[1], sum_recv.at[1])
    feed.start()
    pg_own[:, :fw] = dot(unit[...], wg[:, window(me, fw)])
    pg_own[:, fw:] = dot(unit[...], wu[:, window(me, fw)])
    for shift in range(1, rows_of):
        stat2.arrive(shift)

    def scale_rows(rows, start, tile):
        second = lax.rsqrt(stat2.total(rows) / width + epsilon)
        ss[rows, :] = second
        n2[rows, :] = (mid[rows, :] * second[:, :1] * gain2[...]).astype(low)

    each_tile(tokens, scale_rows)
    feed.relay()
    feed.arrive()
    back.arrive()

    def activate(rows, start, tile):
        second = ss[rows, :1]
        gate = pg_own[rows, :fw]
        upward = pg_own[rows, fw:]
        for slot in range(feed.count):
            gate = gate + pg_r[slot, rows, :fw].astype(wide)
            upward = upward + pg_r[slot, rows, fw:].astype(wide)
        gate = gate * second
        upward = upward * second
        sigmoid = jax.nn.sigmoid(gate)
        silu = gate * sigmoid
        hid[rows, :] = (silu * upward).astype(low)
        behind = ph_own[rows, :]
        for slot in range(back.count):
            behind = behind + ph_r[slot, rows, :].astype(wide)
        gub[rows, :fw] = (behind * upward * sigmoid * (1.0 + gate * (1.0 - sigmoid))).astype(low)
        gub[rows, fw:] = (behind * silu).astype(low)

    each_tile(tokens, activate)
    for shift in range(1, members):
        spread.arrive(shift)
    kept.wait()
    for exchange in (stat1, qkv, back, gather, column, stat2, feed, spread):
        exchange.finish()


def split(rows, columns):
    count = 1
    while rows % count or (rows // count) * columns > chunk_limit:
        count += 1
    return count


class Line:
    def __init__(self, members, out, near, far, spares, sems):
        self.members, self.out, self.near, self.far = members, out, near, far
        self.spares = spares
        self.in_send, self.near_sem, self.far_sem, self.out_send, self.store_sem, self.load_sem = sems
        me = lax.axis_index("dp")
        half = members // 2
        left = me < half
        place = jnp.where(left, half - 1 - me, me - half)
        self.inner = jnp.where(left, me + 1, me - 1)
        self.outer = jnp.where(left, jnp.maximum(me - 1, 0), jnp.minimum(me + 1, members - 1))
        self.is_mid = place == 0
        self.not_mid = place > 0
        self.has_outer = place < half - 1
        self.is_end = place == half - 1
        self.chunks, self.done = [], 0

    def view(self, refs, index):
        which, row, rows, column, columns = self.chunks[index]
        if not isinstance(row, int):
            row = pl.multiple_of(row, 16)
        if not isinstance(column, int):
            column = pl.multiple_of(column, lanes)
        return refs[which].at[pl.ds(row, rows), pl.ds(column, columns)]

    def inward(self, index, target, sem):
        return remote(
            self.view(self.out, index),
            self.view(target, index),
            self.in_send.at[index],
            sem.at[index],
            "dp",
            self.inner,
        )

    def outward(self, index):
        return remote(
            self.view(self.out, index),
            self.view(self.far, index),
            self.out_send.at[index],
            self.far_sem.at[index],
            "dp",
            self.outer,
        )

    def relay(self, index):
        return remote(
            self.view(self.far, index),
            self.view(self.far, index),
            self.out_send.at[index],
            self.far_sem.at[index],
            "dp",
            self.outer,
        )

    def send_in(self, index):
        @pl.when(self.is_mid)
        def _():
            self.inward(index, self.far, self.far_sem).start()

        @pl.when(self.not_mid)
        def _():
            self.inward(index, self.near, self.near_sem).start()

    def release(self, which, row, rows, column, columns):
        if self.members == 1:
            return
        count = split(rows, columns)
        for part in range(count):
            size = rows // count
            self.chunks.append((which, row + part * size, size, column, columns))
            index = len(self.chunks) - 1

            @pl.when(self.is_end)
            def _(index=index):
                self.send_in(index)

    def spare(self, index, kind):
        _, _, rows, _, columns = self.chunks[index]
        for ref in self.spares:
            if ref.shape[1:] == (rows, columns):
                return ref.at[kind]
        raise ValueError("no spare")

    def load(self, index, kind):
        source = self.view((self.near, self.far)[kind], index)
        return pltpu.make_async_copy(source, self.spare(index, kind), self.load_sem.at[kind])

    def add(self, index, kind):
        target, other = self.view(self.out, index), self.spare(index, kind)
        rows = other.shape[0]
        tile = 32 if rows % 32 == 0 else rows

        def step(part, carry):
            spot = pl.ds(pl.multiple_of(part * tile, 16), tile)
            target[spot, :] = (target[spot, :].astype(wide) + other[spot, :].astype(wide)).astype(low)
            return carry

        lax.fori_loop(0, rows // tile, step, 0)

    def begin_total(self, index):
        @pl.when(self.is_mid)
        def _():
            self.inward(index, self.far, self.far_sem).wait_recv()
            self.load(index, 1).start()

    def store(self, index):
        return pltpu.make_async_copy(
            self.view(self.out, index), self.view(self.far, index), self.store_sem.at[index]
        )

    def end_total(self, index):
        @pl.when(self.is_mid)
        def _():
            self.load(index, 1).wait()
            self.inward(index, self.far, self.far_sem).wait_send()
            self.add(index, 1)

            @pl.when(self.has_outer)
            def _():
                self.outward(index).start()

            self.store(index).start()

    def advance(self, count):
        if self.members == 1:
            return
        for _ in range(count):
            if self.done == len(self.chunks):
                return
            index = self.done
            self.done += 1

            @pl.when(self.has_outer)
            def _():
                self.inward(index, self.near, self.near_sem).wait_recv()
                self.load(index, 0).start()

            if index >= lag:
                self.begin_total(index - lag)

            @pl.when(self.has_outer)
            def _():
                self.load(index, 0).wait()
                self.add(index, 0)
                self.send_in(index)

            if index >= lag:
                self.end_total(index - lag)

    def settle(self):
        total = len(self.chunks)
        self.advance(total - self.done)
        for index in range(max(total - lag, 0), total):
            self.begin_total(index)
            self.end_total(index)

        @pl.when(self.not_mid)
        def _():
            for index in range(total):
                self.inward(index, self.far, self.far_sem).wait_recv()

                @pl.when(self.has_outer)
                def _():
                    self.relay(index).start()

            for index in range(total):
                self.inward(index, self.near, self.near_sem).wait_send()

                @pl.when(self.has_outer)
                def _():
                    self.relay(index).wait_send()

        @pl.when(self.is_mid)
        def _():
            for index in range(total):
                self.store(index).wait()

                @pl.when(self.has_outer)
                def _():
                    self.outward(index).wait_send()


class Chain:
    def __init__(self, members, own, blocks, send, receive, pass_send, pass_recv, row):
        self.members, self.own, self.blocks, self.row = members, own, blocks, row
        self.send, self.receive = send, receive
        self.pass_send, self.pass_recv = pass_send, pass_recv
        self.me = lax.axis_index("dp")

    def valid(self, place):
        return (place >= 0) & (place < self.members)

    def step(self, side, hop):
        way = 1 - 2 * side
        origin = self.me - way * (hop - 1)
        spot = self.blocks.at[origin, self.row.me]
        return remote(
            self.own if hop == 1 else spot,
            spot,
            self.send.at[side, hop - 1],
            self.receive.at[side, hop - 1],
            "dp",
            self.me + way,
        )

    def incoming(self, side, hop):
        origin = self.me - (1 - 2 * side) * hop
        spot = self.blocks.at[origin, self.row.me]
        return origin, remote(
            spot,
            spot,
            self.send.at[side, hop - 1],
            self.receive.at[side, hop - 1],
            "dp",
            self.me,
        )

    def sends(self, side, hop):
        way = 1 - 2 * side
        return self.valid(self.me - way * (hop - 1)) & self.valid(self.me + way)

    def hop(self, hop):
        for side in range(2):
            if hop > 1:
                self.await_block(side, hop - 1)

            @pl.when(self.sends(side, hop))
            def _(side=side):
                self.step(side, hop).start()

    def await_block(self, side, hop):
        @pl.when(self.valid(self.me - (1 - 2 * side) * hop))
        def _():
            self.incoming(side, hop)[1].wait_recv()

    def pass_on(self, side, hop, shift):
        origin = self.me - (1 - 2 * side) * hop
        spot = self.blocks.at[origin, self.row.me]
        return remote(
            spot,
            spot,
            self.pass_send.at[side, hop - 1, shift - 1],
            self.pass_recv.at[side, hop - 1, shift - 1],
            "row",
            self.row.target(shift),
        )

    def spread(self, hop):
        for side in range(2):
            if hop == self.members - 1:
                self.await_block(side, hop)

            @pl.when(self.valid(self.me - (1 - 2 * side) * hop))
            def _(side=side):
                for shift in range(1, self.row.size):
                    self.pass_on(side, hop, shift).start()

    def finish(self):
        for hop in range(1, self.members):
            for side in range(2):

                @pl.when(self.valid(self.me - (1 - 2 * side) * hop))
                def _(side=side, hop=hop):
                    for shift in range(1, self.row.size):
                        self.pass_on(side, hop, shift).wait_recv()
                        self.pass_on(side, hop, shift).wait_send()

                @pl.when(self.sends(side, hop))
                def _(side=side, hop=hop):
                    self.step(side, hop).wait_send()


def backward_kernel(
    rows_of,
    cols_of,
    members,
    need,
    x,
    ct,
    n1,
    fs,
    raw,
    lows,
    shares,
    trig,
    mixed,
    mid,
    ss,
    n2,
    hid,
    gub,
    gain1,
    gain2,
    qn,
    kn,
    wq,
    wk,
    wv,
    wo,
    wg,
    wu,
    wd,
    bo,
    ig,
    small,
    *rest,
):
    hid_all, *rest = rest
    far, near, rest = rest[:6], rest[6:12], rest[12:]
    grads, rest = rest[:6], rest[6:]
    gq, gk, gv, go, gg, gu = grads
    (
        hid_r,
    gub_r,
    n_t,
    mb,
    ml,
    pm_own,
    pm_s,
    pm_r,
    sl,
    sb,
    dqkv,
    dqkv_r,
    gains,
    stat_s,
    stat_r,
    ox_s,
    ox_r,
    row_send,
    row_recv,
    stat_send,
    stat_recv,
        col_send,
        col_recv,
        small_r,
        small_send,
        small_recv,
        in_send,
        near_sem,
        far_sem,
        out_send,
        store_sem,
        load_sem,
        hop_send,
        hop_recv,
        pass_send,
        pass_recv,
        keep_sem,
        *spares,
    ) = rest
    tokens, depth = x.shape
    width = depth * rows_of
    qw, kw, fw = wq.shape[1] // rows_of, wk.shape[1] // rows_of, wg.shape[1] // rows_of
    size = qn.shape[1]
    heads, key_heads = qw // size, kw // size
    group = heads // key_heads
    scale = size ** (-0.5)
    me = lax.axis_index("row")
    greet((("row", rows_of), ("col", cols_of), ("dp", members)))
    line = Line(
        members,
        grads,
        near,
        far,
        spares,
        (in_send, near_sem, far_sem, out_send, store_sem, load_sem),
    )

    def row_exchange(kind, send, receive):
        return Exchange("row", rows_of, send, receive, row_send.at[kind], row_recv.at[kind])

    def stat_exchange(kind):
        return Ranked(
            "row",
            rows_of,
            lambda shift: stat_s.at[kind],
            stat_r.at[kind],
            stat_send.at[kind],
            stat_recv.at[kind],
        )

    def column_exchange(kind):
        return Exchange(
            "col",
            cols_of,
            lambda shift: ox_s.at[kind],
            ox_r.at[kind],
            col_send.at[kind],
            col_recv.at[kind],
        )

    def column_sum(kind, rows):
        value = ox_s[kind, rows, :]
        for shift in range(1, cols_of):
            value = value + ox_r[kind, shift - 1, rows, :]
        return value

    hide = row_exchange(0, lambda shift: hid, hid_r)
    gates = row_exchange(1, lambda shift: gub, gub_r)
    body = pl.ds(0, tokens)
    chain = Chain(members, hid, hid_all, hop_send, hop_recv, pass_send, pass_recv, hide)
    chain.hop(1)
    for shift in range(1, rows_of):
        gates.start(shift)
    stage = lax.axis_index("dp")

    def keep(shift):
        piece = hid if shift == 0 else hid_r.at[shift - 1]
        return pltpu.make_async_copy(
            piece, hid_all.at[stage, hide.source(shift)], keep_sem.at[shift]
        )

    keep(0).start()
    n_t[...] = n2[...].T
    need("wg", "wu")
    for shift in range(rows_of):
        if shift:
            line.advance(pace * (1 if shift == 1 else 2))
            if shift + 1 < members:
                chain.hop(shift + 1)
            gates.arrive(shift)
        piece = gub if shift == 0 else gub_r.at[shift - 1]
        index = window(gates.source(shift), fw)
        part = dot_t(piece[:, :fw], wg[:, index]) + dot_t(piece[:, fw:], wu[:, index])
        if shift == 0:
            ox_s[1, body, :] = part
        else:
            ox_s[1, body, :] += part
        gg[:, index] = dot(n_t[...], piece[:, :fw]).astype(low)
        line.release(4, 0, depth, gates.source(shift) * fw, fw)
        gu[:, index] = dot(n_t[...], piece[:, fw:]).astype(low)
        line.release(5, 0, depth, gates.source(shift) * fw, fw)
    for step in range(rows_of + 1, members):
        chain.hop(step)
    need("mid", "ss")
    column1 = column_exchange(1)
    for shift in range(1, cols_of):
        column1.start(shift)
    line.advance(1 * pace)
    for shift in range(1, cols_of):
        column1.arrive(shift)

    stat2 = stat_exchange(0)
    small[...] = jnp.zeros_like(small)
    gains[...] = jnp.zeros_like(gains)

    def feed_stat(rows, start, tile):
        back = column_sum(1, rows)
        unit = mid[rows, :] * ss[rows, :1]
        small[1:2, :] += jnp.sum(back * unit, axis=0, keepdims=True)
        inner = jnp.sum(back * gain2[...] * unit, axis=1, keepdims=True)
        inner = jnp.broadcast_to(inner, (tile, lanes))
        stat_s[0, rows] = inner
        stat_r[0, me, rows] = inner

    each_tile(tokens, feed_stat)
    pad = pl.ds(tokens, 8)
    stat_s[0, pad] = jnp.zeros((8, lanes), wide)
    for shift in range(1, rows_of):
        stat2.start(shift)
    need("wo", "mixed", "lows", "shares", "ct")
    line.advance(1 * pace)
    for shift in range(1, rows_of):
        stat2.arrive(shift)

    def middle_back(rows, start, tile):
        second = ss[rows, :1]
        unit = mid[rows, :] * second
        inner = stat2.total(rows)[:, :1] / width
        value = ct[rows, :].astype(wide) + second * (
            column_sum(1, rows) * gain2[...] - unit * inner
        )
        mb[rows, :] = value
        ml[rows, :] = value.astype(low)

    each_tile(tokens, middle_back)
    blend = row_exchange(2, lambda shift: pm_s.at[shift - 1], pm_r)
    for shift in range(1, rows_of):
        pm_s[shift - 1] = dot_t(ml[...], wo[window(blend.target(shift), qw), :]).astype(low)
        blend.start(shift)
    pm_own[...] = dot_t(ml[...], wo[window(me, qw), :])
    for shift in range(rows_of):
        index = window(blend.source(shift), qw)
        go[index, :] = t_dot(mixed[shift], ml[...]).astype(low)
        line.release(3, blend.source(shift) * qw, qw, 0, depth)
    line.advance(2 * pace)
    for shift in range(1, rows_of):
        blend.arrive(shift)

    def share_back(rows, start, tile):
        value = pm_own[rows, :]
        for shift in range(1, rows_of):
            value = value + pm_r[shift - 1, rows, :].astype(wide)
        incoming = value.astype(low)
        pm_s[0, rows, :] = incoming
        product = incoming.astype(wide) * mixed[0, rows, :].astype(wide)
        for head in range(heads):
            pair = head // group
            part = slice(head * size, (head + 1) * size)
            values = lows[:, qw + kw + pair * size : qw + kw + (pair + 1) * size]
            delta = jnp.sum(product[:, part], axis=1, keepdims=True)
            share = shares[head, rows, :]
            sl[head, rows, :] = share.astype(low)
            sb[head, rows, :] = (share * (dot_t(incoming[:, part], values) - delta)).astype(low)

    blend.finish()
    each_tile(tokens, share_back)
    need("n1", "raw", "trig")
    n_t[...] = n1[...].T
    line.advance(1 * pace)

    def pull(head, back, gain, row):
        raw_piece = raw[:, head * size : (head + 1) * size]
        norm = lax.rsqrt(jnp.mean(raw_piece * raw_piece, axis=1, keepdims=True) + epsilon)
        unit = raw_piece * norm
        normed_back = back * trig[0] - half_turn(back * trig[1])
        gains[row : row + 1, :] += jnp.sum(normed_back * unit, axis=0, keepdims=True)
        unit_back = normed_back * gain
        return norm * (unit_back - unit * jnp.mean(unit_back * unit, axis=1, keepdims=True))

    for pair in range(key_heads):
        keys = lows[:, qw + pair * size : qw + (pair + 1) * size]
        key_back = jnp.zeros((tokens, size), wide)
        value_back = jnp.zeros((tokens, size), wide)
        for head in range(pair * group, (pair + 1) * group):
            part = slice(head * size, (head + 1) * size)
            value_back = value_back + t_dot(sl[head], pm_s[0, :, part])
            key_back = key_back + scale * t_dot(sb[head], lows[:, part])
            query_back = scale * dot(sb[head], keys)
            dqkv[:, part] = pull(head, query_back, qn[...], 0).astype(low)
        spot = qw + pair * size
        dqkv[:, spot : spot + size] = pull(heads + pair, key_back, kn[...], 1).astype(low)
        spot = qw + kw + pair * size
        dqkv[:, spot : spot + size] = value_back.astype(low)

    deliver = row_exchange(3, lambda shift: dqkv, dqkv_r)
    for shift in range(1, rows_of):
        deliver.start(shift)
    for shift in range(1, rows_of):
        hide.start(shift)
    if members > 1:
        chain.spread(1)
    need("wq", "wk", "wv")
    for shift in range(rows_of):
        if shift:
            line.advance(1 * pace)
            deliver.arrive(shift)
        piece = dqkv if shift == 0 else dqkv_r.at[shift - 1]
        source = deliver.source(shift)
        part = dot_t(piece[:, :qw], wq[:, window(source, qw)])
        part = part + dot_t(piece[:, qw : qw + kw], wk[:, window(source, kw)])
        part = part + dot_t(piece[:, qw + kw :], wv[:, window(source, kw)])
        if shift == 0:
            ox_s[2, body, :] = part
        else:
            ox_s[2, body, :] += part
    ox_s[2, pad, :] = jnp.zeros((8, depth), wide)
    ox_s[2, pad, :lanes] = gains[...]
    column2 = column_exchange(2)
    for shift in range(1, cols_of):
        column2.start(shift)
    for shift in range(rows_of):
        piece = dqkv if shift == 0 else dqkv_r.at[shift - 1]
        source = deliver.source(shift)
        gq[:, window(source, qw)] = dot(n_t[...], piece[:, :qw]).astype(low)
        gk[:, window(source, kw)] = dot(n_t[...], piece[:, qw : qw + kw]).astype(low)
        gv[:, window(source, kw)] = dot(n_t[...], piece[:, qw + kw :]).astype(low)
    line.release(0, 0, depth, 0, qw * rows_of)
    line.release(1, 0, depth, 0, kw * rows_of)
    line.release(2, 0, depth, 0, kw * rows_of)
    line.advance(1 * pace)
    for shift in range(1, cols_of):
        column2.arrive(shift)
    need("x", "fs")

    stat1 = stat_exchange(1)

    def first_stat(rows, start, tile):
        back = column_sum(2, rows)
        unit = x[rows, :].astype(wide) * fs[rows, :1]
        small[0:1, :] += jnp.sum(back * unit, axis=0, keepdims=True)
        inner = jnp.sum(back * gain1[...] * unit, axis=1, keepdims=True)
        inner = jnp.broadcast_to(inner, (tile, lanes))
        stat_s[1, rows] = inner
        stat_r[1, me, rows] = inner

    each_tile(tokens, first_stat)
    summed = column_sum(2, pad)[:, :lanes]
    stat_s[1, pad] = summed
    stat_r[1, me, pad] = summed
    for shift in range(1, rows_of):
        stat1.start(shift)
    for step in range(2, members):
        chain.spread(step)
    line.advance(bulk * pace)
    need("wd")
    for shift in range(rows_of):
        if shift:
            hide.arrive(shift)
            keep(shift).start()
        piece = hid[...] if shift == 0 else hid_r[shift - 1]
        part = dot(piece, wd[window(hide.source(shift), fw), :])
        if shift == 0:
            ox_s[0, body, :] = part
        else:
            ox_s[0, body, :] += part
    column0 = column_exchange(0)
    for shift in range(1, cols_of):
        column0.start(shift)
    for shift in range(1, cols_of):
        column0.arrive(shift)

    def result(rows, start, tile):
        bo[rows, :] = (mid[rows, :] + column_sum(0, rows)).astype(low)

    each_tile(tokens, result)
    line.advance(slots_left)
    for shift in range(1, rows_of):
        stat1.arrive(shift)

    def finish(rows, start, tile):
        first = fs[rows, :1]
        unit = x[rows, :].astype(wide) * first
        inner = stat1.total(rows)[:, :1] / width
        ig[rows, :] = mb[rows, :] + first * (column_sum(2, rows) * gain1[...] - unit * inner)

    each_tile(tokens, finish)
    small[8:16, :lanes] = stat1.total(pad)
    ranked = Ranked("dp", members, lambda shift: small, small_r, small_send, small_recv)
    if members > 1:
        small_r[lax.axis_index("dp")] = small[...]
        for shift in range(1, members):
            ranked.start(shift)
    if members > 1:
        line.settle()
        for shift in range(1, members):
            ranked.arrive(shift)
        ranked.finish()
        summed = small_r[0]
        for member in range(1, members):
            summed = summed + small_r[member]
        small[...] = summed
    chain.finish()
    for shift in range(rows_of):
        keep(shift).wait()
    for exchange in (hide, gates, column0, column1, stat2, deliver, column2, stat1):
        exchange.finish()


def widen_kernel(*refs):
    count = (len(refs) - 8) // 2
    hid_all, ct_all, small = refs[count : count + 3]
    *out, gd, gain1, gain2, gain_q, gain_k = refs[count + 3 :]
    gain1[...] = small[0:1, :]
    gain2[...] = small[1:2, :]
    gain_q[...] = small[8:9, : gain_q.shape[1]]
    gain_k[...] = small[9:10, : gain_k.shape[1]]
    for source, target in zip(refs[:count], out):
        target[...] = source[...].astype(target.dtype)
    total = t_dot(hid_all[0, 0], ct_all[0])
    for member in range(1, ct_all.shape[0]):
        total = total + t_dot(hid_all[member, 0], ct_all[member])
    gd[...] = total


def widen(arrays, kinds, hid_all, ct_all, small, shape, size):
    members, rows_of, tokens, fw = hid_all.shape
    parts = 2 if fw % (2 * lanes) == 0 else 1
    steps = rows_of * parts

    def rows(array_shape):
        return pl.BlockSpec((array_shape[0] // steps, array_shape[1]), lambda i: (i, 0))

    specs = [rows(array.shape) for array in arrays]
    vectors = [(1, small.shape[1])] * 2 + [(1, size)] * 2
    shapes = [array.shape for array in arrays] + [shape] + vectors

    def whole(array_shape):
        return pl.BlockSpec(array_shape, lambda i: (0,) * len(array_shape))

    return pl.pallas_call(
        widen_kernel,
        grid=(steps,),
        out_shape=tuple(map(jax.ShapeDtypeStruct, shapes, kinds)),
        in_specs=specs
        + [
            pl.BlockSpec(
                (members, 1, tokens, fw // parts), lambda i: (0, i // parts, 0, i % parts)
            ),
            whole(ct_all.shape),
            whole(small.shape),
        ],
        out_specs=tuple(specs + [rows(shape)] + [whole(vector) for vector in vectors]),
        compiler_params=pltpu.CompilerParams(vmem_limit_bytes=full_vmem),
    )(*arrays, hid_all, ct_all, small)


def vmem(shape, kind):
    return pltpu.VMEM(shape, kind)


def call(kernel, shapes, scratch, identity, arguments, late=(), outside=()):
    inside, away = pl.BlockSpec(memory_space=pltpu.VMEM), pl.BlockSpec(memory_space=pl.ANY)
    names = list(arguments)
    late = [name for name in names if name in late]

    def body(*refs):
        given = dict(zip(names, refs))
        rest = refs[len(names) :]
        copies = {}
        if late:
            holders, sem = rest[-len(late) - 1 : -1], rest[-1]
            rest = rest[: -len(late) - 1]
            for index, name in enumerate(late):
                copies[name] = pltpu.make_async_copy(given[name], holders[index], sem.at[index])
                copies[name].start()
                given[name] = holders[index]

        def need(*wanted):
            for name in wanted:
                copy = copies.pop(name, None)
                if copy is not None:
                    copy.wait()

        kernel(need, *given.values(), *rest)
        need(*list(copies))

    extra = []
    if late:
        extra = [vmem(arguments[name].shape, arguments[name].dtype) for name in late]
        extra.append(pltpu.SemaphoreType.DMA((len(late),)))
    return pl.pallas_call(
        body,
        out_shape=tuple(jax.ShapeDtypeStruct(shape, kind) for shape, kind in shapes),
        in_specs=[away if name in late else inside for name in names],
        out_specs=tuple(away if index in outside else inside for index in range(len(shapes))),
        scratch_shapes=scratch + extra,
        compiler_params=pltpu.CompilerParams(
            collective_id=identity, has_side_effects=True, vmem_limit_bytes=full_vmem
        ),
    )(*arguments.values())


def per_device(
    block_input,
    segments,
    attention_norm,
    query_weight,
    key_weight,
    value_weight,
    query_norm,
    key_norm,
    output_weight,
    feedforward_norm,
    gate_weight,
    up_weight,
    down_weight,
    cotangent,
):
    rows_of, cols_of, members = (lax.axis_size(name) for name in ("row", "col", "dp"))
    tokens, depth = block_input.shape
    size = query_norm.shape[0]
    qw, kw, fw = (
        weight.shape[1] // rows_of for weight in (query_weight, key_weight, gate_weight)
    )
    heads = qw // size
    others, beside = max(rows_of - 1, 1), max(cols_of - 1, 1)
    half = size // 2
    inverse = rope_base ** (-2.0 * np.arange(half) / size)
    inverse = jnp.asarray(np.concatenate([inverse, inverse])[None, :], wide)
    seg_row = segments.reshape(1, tokens)
    gain1, gain2 = attention_norm[None, :], feedforward_norm[None, :]
    qn, kn = query_norm[None, :], key_norm[None, :]
    total = qw + 2 * kw
    peers = max(members - 1, 1)
    dma = pltpu.SemaphoreType.DMA

    def sems(kinds):
        return [
            dma((5, others)),
            dma((5, others)),
            dma((2, others)),
            dma((2, others)),
            dma((kinds, beside)) if kinds > 1 else dma((beside,)),
            dma((kinds, beside)) if kinds > 1 else dma((beside,)),
        ]

    saved = call(
        partial(forward_kernel, rows_of, cols_of, members),
        (
            ((tokens, depth), low),
            ((tokens, lanes), wide),
            ((tokens, qw + kw), wide),
            ((tokens, total), low),
            ((heads, tokens, tokens), wide),
            ((2, tokens, size), wide),
            ((rows_of, tokens, qw), low),
            ((tokens, depth), wide),
            ((tokens, lanes), wide),
            ((tokens, depth), low),
            ((tokens, fw), low),
            ((tokens, 2 * fw), low),
            ((members, tokens, depth), low),
        ),
        [
            vmem((tokens, lanes), wide),
            vmem((tokens, depth), low),
            vmem((tokens, total), wide),
            vmem((others, tokens, total), low),
            vmem((others, tokens, total), low),
            vmem((2, tokens // 2, total), low),
            vmem((tokens, fw), wide),
            vmem((others, tokens, fw), low),
            vmem((others, tokens, fw), low),
            vmem((2, tokens // 2, fw), low),
            vmem((tokens, 2 * fw), wide),
            vmem((others, tokens, 2 * fw), low),
            vmem((others, tokens, 2 * fw), low),
            vmem((2, tokens // 2, 2 * fw), low),
            vmem((others, tokens, qw), low),
            vmem((2, tokens, lanes), wide),
            vmem((2, rows_of, tokens, lanes), wide),
            vmem((tokens, depth), wide),
            vmem((beside, tokens, depth), wide),
        ]
        + sems(1)
        + [dma((peers,)), dma((peers,)), dma((1,))]
        + [dma((3, max(6, others)))] * 2,
        0,
        dict(
            x=block_input,
            seg_row=seg_row,
            inverse=inverse,
            gain1=gain1,
            wq=query_weight,
            wk=key_weight,
            wv=value_weight,
            qn=qn,
            kn=kn,
            wo=output_weight,
            gain2=gain2,
            wg=gate_weight,
            wu=up_weight,
            ct=cotangent,
            wd=down_weight,
        ),
        late=("wo", "wg", "wu", "ct", "wd"),
        outside=(12,),
    )
    *saved, ct_all = saved
    saved = dict(
        zip(("n1", "fs", "raw", "lows", "shares", "trig", "mixed", "mid", "ss", "n2", "hid", "gub"), saved)
    )
    weights = (query_weight, key_weight, value_weight, output_weight, gate_weight, up_weight)
    shapes = [weight.shape for weight in weights]
    pieces = {
        (depth, fw): 2 * rows_of,
        (qw, depth): rows_of,
        (depth, qw * rows_of): 1,
        (depth, kw * rows_of): 2,
    }
    slots = sum(split(*shape) * times for shape, times in pieces.items())
    spares = {(shape[0] // split(*shape), shape[1]) for shape in pieces}
    done = call(
        partial(backward_kernel, rows_of, cols_of, members),
        (
            ((tokens, depth), low),
            ((tokens, depth), wide),
            ((16, depth), wide),
            ((members, rows_of, tokens, fw), low),
            *((shape, low) for shape in shapes * 2),
        ),
        [vmem(shape, low) for shape in shapes]
        + [
            vmem((others, tokens, fw), low),
            vmem((others, tokens, 2 * fw), low),
            vmem((depth, tokens), low),
            vmem((tokens, depth), wide),
            vmem((tokens, depth), low),
            vmem((tokens, qw), wide),
            vmem((others, tokens, qw), low),
            vmem((others, tokens, qw), low),
            vmem((heads, tokens, tokens), low),
            vmem((heads, tokens, tokens), low),
            vmem((tokens, total), low),
            vmem((others, tokens, total), low),
            vmem((8, lanes), wide),
            vmem((2, tokens + 8, lanes), wide),
            vmem((2, rows_of, tokens + 8, lanes), wide),
            vmem((3, tokens + 8, depth), wide),
            vmem((3, beside, tokens + 8, depth), wide),
        ]
        + sems(3)
        + [vmem((members, 16, depth), wide), dma((peers,)), dma((peers,))]
        + [dma((slots,))] * 5
        + [dma((2,))]
        + [dma((2, peers))] * 2
        + [dma((2, peers, others))] * 2
        + [dma((rows_of,))]
        + [vmem((2, *shape), low) for shape in sorted(spares)],
        1,
        dict(
            x=block_input,
            ct=cotangent,
            **saved,
            gain1=gain1,
            gain2=gain2,
            qn=qn,
            kn=kn,
            wq=query_weight,
            wk=key_weight,
            wv=value_weight,
            wo=output_weight,
            wg=gate_weight,
            wu=up_weight,
            wd=down_weight,
        ),
        late=("x", "n1", "fs", "raw", "lows", "shares", "trig", "mixed", "mid", "ss", "ct", "wd", "wq", "wk", "wv", "wo", "wg", "wu"),
        outside=range(3, 16),
    )
    block_output, input_gradient, small, hid_all, *partials = done[:10]
    block_output, input_gradient, gq, gk, gv, go, gg, gu, gd, *sums = widen(
        (block_output, input_gradient, *partials),
        [low] + [wide] * 12,
        hid_all,
        ct_all,
        small,
        down_weight.shape,
        size,
    )
    sum1, sum2, sum_q, sum_k = (vector[0] for vector in sums)
    return (
        block_output,
        input_gradient,
        sum1,
        gq,
        gk,
        gv,
        sum_q,
        sum_k,
        go,
        sum2,
        gg,
        gu,
        gd,
    )


def solution(mesh):
    return jax.shard_map(
        per_device,
        mesh=mesh,
        in_specs=(
            P("dp", "row"),
            P("dp", None),
            P("row"),
            P("row", "col"),
            P("row", "col"),
            P("row", "col"),
            P(),
            P(),
            P("col", "row"),
            P("row"),
            P("row", "col"),
            P("row", "col"),
            P("col", "row"),
            P("dp", "row"),
        ),
        out_specs=(
            P("dp", "row"),
            P("dp", "row"),
            P("row"),
            P("row", "col"),
            P("row", "col"),
            P("row", "col"),
            P(),
            P(),
            P("col", "row"),
            P("row"),
            P("row", "col"),
            P("row", "col"),
            P("col", "row"),
        ),
        check_vma=False,
    )
```
